32 devices in a mesh: row: 4 (over z), col: 4 (over x, core), ch: 2 (over y).
Axes of the slice: x: 2, y: 2, z: 4, core: 2. Of those that a mesh axis runs over, the one named last changes fastest.
Arguments:
- image_tokens: bfloat16 [64, 1024, 128], P(('row', 'ch'), 'col'), may hold values from -61 to 61
- labels: int32 [64, 1024], P(('row', 'ch'), 'col'), may hold values from 0 to 2
- rel_index: int32 [64, 64], replicated, may hold values from 0 to 224
- norm_gain: float32 [2, 2, 128], replicated, may hold values from 0.25 to 1.75
- norm_shift: float32 [2, 2, 128], replicated, may hold values from -1.5 to 1.5
- qkv_weight: bfloat16 [2, 3, 128, 128], P(None, None, None, 'ch'), may hold values from -5 to 5
- qkv_bias: float32 [2, 3, 128], P(None, None, 'ch'), may hold values from -1.5 to 1.5
- bias_table: float32 [2, 225, 4], P(None, None, 'ch'), may hold values from -4 to 4
- proj_weight: bfloat16 [2, 128, 128], P(None, 'ch'), may hold values from -0.5 to 0.5
- proj_bias: float32 [2, 128], replicated, may hold values from -1.5 to 1.5
- fc1_weight: bfloat16 [2, 128, 512], P(None, None, 'ch'), may hold values from -0.5 to 0.5
- fc1_bias: float32 [2, 512], P(None, 'ch'), may hold values from -2.5 to 2.5
- fc2_weight: bfloat16 [2, 512, 128], P(None, 'ch'), may hold values from -0.25 to 0.25
- fc2_bias: float32 [2, 128], replicated, may hold values from -1.5 to 1.5
Outputs:
- encoded: bfloat16 [64, 1024, 128], P(('row', 'ch'), 'col')
The draws below stay inside these ranges and needn't reach their ends.
All inputs are finite; a program needn't handle non-finite values.
Results may differ from the reference program's by a relative error of at most 0.014.
Values may be sent and summed in bfloat16 or wider, within the bound.
No kernel may reach another device: no remote copies, remote signals or barrier semaphores. Data moves between devices by JAX's collectives and lax.ppermute only.
A program may use at most 128 MiB of HBM per device.

```python
import jax
import jax.numpy as jnp
from jax import lax

C = 128
HEADS = 4
MLP_WIDTH = 512
WIN = 8
SHIFT = 4
TABLE = 225
BLOCKS = 2
KINDS = 3
IMG_ROWS = 64
IMG_COLS = 1024


def draw_image_tokens(key, part):
    base_key = jax.random.fold_in(key, 11)
    values = jnp.clip(jax.random.normal(base_key, (IMG_ROWS, IMG_COLS, C), jnp.float32), -6.0, 6.0)
    return values.astype(jnp.bfloat16)


def draw_qkv_weight(key, part):
    noise_key = jax.random.fold_in(key, 21)
    noise = jnp.clip(jax.random.normal(noise_key, (BLOCKS, 3, C, C), jnp.float32), -4.0, 4.0) * C ** (-0.5)
    return noise.astype(jnp.bfloat16)


def place_ends(values, rng, smallest, high):
    dims = values.shape
    spot = [jax.random.randint(jax.random.fold_in(rng, axis), (), 0, dims[axis]) for axis in range(len(dims))]
    values = values.at[tuple(spot)].set(smallest)
    longest = dims.index(max(dims))
    spot[longest] = (spot[longest] + 1) % dims[longest]
    return values.at[tuple(spot)].set(high)


def steps_of(own_key, extent, shards, low, top_value):
    loudness = 1.0
    for dim, shards_of in shards:
        draws = jax.random.uniform(jax.random.fold_in(jax.random.fold_in(own_key, 6), dim), (shards_of,), jnp.float32, low / len(shards), top_value / len(shards))
        loudness = loudness * jnp.repeat(jnp.exp(draws), extent[dim] // shards_of).reshape((-1,) + (1,) * (len(extent) - 1 - dim))
    return loudness


def scatter_about(rng, extent, scale, bound, shards=(), held_as=jnp.bfloat16):
    drawn = scale * jax.random.normal(rng, extent, jnp.float32)
    if shards:
        drawn = drawn * steps_of(rng, extent, shards, -0.22, 0.18)
    return jnp.clip(drawn, -bound, bound).astype(held_as)


def setup_inputs(seed: int = 0) -> dict:
    arg_keys = jax.random.split(jax.random.key(seed), 15)
    image_tokens = draw_image_tokens(jax.random.fold_in(arg_keys[14], 71), 0)
    labels = place_ends(jax.random.randint(arg_keys[1], (IMG_ROWS, IMG_COLS), 0, KINDS), jax.random.fold_in(arg_keys[1], 1), 0, KINDS - 1).astype(jnp.int32)
    rel_index = place_ends(jax.random.randint(arg_keys[2], (WIN * WIN, WIN * WIN), 0, TABLE), jax.random.fold_in(arg_keys[2], 1), 0, TABLE - 1).astype(jnp.int32)
    norm_gain = jnp.clip(1.0 + 0.15 * jax.random.normal(arg_keys[3], (BLOCKS, 2, C), jnp.float32), 0.25, 1.75)
    norm_shift = scatter_about(arg_keys[4], (BLOCKS, 2, C), 0.3, 1.5, (), jnp.float32)
    qkv_weight = draw_qkv_weight(jax.random.fold_in(arg_keys[14], 71), 0)
    qkv_bias = scatter_about(arg_keys[6], (BLOCKS, 3, C), 0.3, 1.5, ((2, 2),), jnp.float32)
    bias_table = scatter_about(arg_keys[7], (BLOCKS, TABLE, HEADS), 1.0, 4.0, ((2, 2),), jnp.float32)
    proj_weight = scatter_about(arg_keys[8], (BLOCKS, C, C), C ** -0.5, 0.5, ((1, 2),))
    proj_bias = scatter_about(arg_keys[9], (BLOCKS, C), 0.3, 1.5, (), jnp.float32)
    fc1_weight = scatter_about(arg_keys[10], (BLOCKS, C, MLP_WIDTH), C ** -0.5, 0.5, ((2, 2),))
    fc1_bias = scatter_about(arg_keys[11], (BLOCKS, MLP_WIDTH), 0.5, 2.5, ((1, 2),), jnp.float32)
    fc2_weight = scatter_about(arg_keys[12], (BLOCKS, MLP_WIDTH, C), MLP_WIDTH ** -0.5, 0.25, ((1, 2),))
    fc2_bias = scatter_about(arg_keys[13], (BLOCKS, C), 0.3, 1.5, (), jnp.float32)
    return {"image_tokens": image_tokens, "labels": labels, "rel_index": rel_index, "norm_gain": norm_gain, "norm_shift": norm_shift, "qkv_weight": qkv_weight, "qkv_bias": qkv_bias, "bias_table": bias_table, "proj_weight": proj_weight, "proj_bias": proj_bias, "fc1_weight": fc1_weight, "fc1_bias": fc1_bias, "fc2_weight": fc2_weight, "fc2_bias": fc2_bias}


EPS = 1e-05

def layer_norm(values, gain, offset):
    widened = values.astype(jnp.float32)
    center = widened - lax.optimization_barrier(jnp.mean(widened, axis=-1, keepdims=True))
    spread = lax.optimization_barrier(jnp.mean(center * center, axis=-1, keepdims=True))
    return (center * lax.rsqrt(spread + EPS) * gain + offset).astype(jnp.bfloat16)

def position_bias(rel_index, table):
    entries = table.shape[0]
    onehot = (rel_index.reshape(-1, 1) == jnp.arange(entries, dtype=jnp.int32)[None, :]).astype(jnp.float32)
    picked = jnp.dot(onehot, table, precision=lax.Precision.HIGHEST, preferred_element_type=jnp.float32)
    length = rel_index.shape[0]
    return picked.T.reshape(table.shape[1], length, length)

def window_attention(triple, region, bias):
    rows, cols = (triple.shape[0], triple.shape[1])
    width = triple.shape[3]
    heads = bias.shape[0]
    depth = width // heads
    across = rows // WIN
    along = cols // WIN
    grid = triple.reshape(across, WIN, along, WIN, 3, heads, depth)
    grid = grid.transpose(0, 2, 4, 5, 1, 3, 6).reshape(across, along, 3, heads, WIN * WIN, depth)
    grid = grid.astype(jnp.float32)
    scores = jnp.einsum('abhpd,abhqd->abhpq', grid[:, :, 0], grid[:, :, 1])
    scores = scores * depth ** (-0.5) + bias
    if region is not None:
        window_ids = region.reshape(across, WIN, along, WIN).transpose(0, 2, 1, 3).reshape(across, along, WIN * WIN)
        allowed = window_ids[:, :, :, None] == window_ids[:, :, None, :]
        scores = jnp.where(allowed[:, :, None], scores, -jnp.inf)
    highest = lax.optimization_barrier(jnp.max(scores, axis=-1, keepdims=True))
    raised = jnp.exp(scores - highest)
    weights = (raised / lax.optimization_barrier(jnp.sum(raised, axis=-1, keepdims=True))).astype(jnp.bfloat16)
    mixed = jnp.einsum('abhpq,abhqd->abhpd', weights.astype(jnp.float32), grid[:, :, 2])
    mixed = mixed.astype(jnp.bfloat16).reshape(across, along, heads, WIN, WIN, depth)
    return mixed.transpose(0, 3, 1, 4, 2, 5).reshape(rows, cols, width)

def attend_image(triple, region, bias, offset):
    rolled = jnp.roll(triple, (-offset, -offset), axis=(0, 1))
    bands = rolled.reshape(IMG_ROWS // WIN, WIN, IMG_COLS, 3, C)
    if region is None:
        result = lax.map(lambda band: window_attention(band, None, bias), bands)
    else:
        region_bands = jnp.roll(region, (-offset, -offset), axis=(0, 1)).reshape(IMG_ROWS // WIN, WIN, IMG_COLS)
        result = lax.map(lambda pair: window_attention(pair[0], pair[1], bias), (bands, region_bands))
    result = result.reshape(IMG_ROWS, IMG_COLS, C)
    return jnp.roll(result, (offset, offset), axis=(0, 1))

def swin_block(tokens, block, region, offset, norm_gain, norm_shift, qkv_weight, qkv_bias, bias_table, proj_weight, proj_bias, fc1_weight, fc1_bias, fc2_weight, fc2_bias, rel_index):
    normed = layer_norm(tokens, norm_gain[block, 0], norm_shift[block, 0])
    stacked = qkv_weight[block].transpose(1, 0, 2).reshape(C, 3 * C)
    triple = jnp.dot(normed.reshape(-1, C), stacked, preferred_element_type=jnp.float32)
    triple = (triple.reshape(IMG_ROWS, IMG_COLS, 3, C) + qkv_bias[block]).astype(jnp.bfloat16)
    bias = position_bias(rel_index, bias_table[block])
    attended = attend_image(triple, region, bias, offset)
    mixed = jnp.dot(attended.reshape(-1, C), proj_weight[block], preferred_element_type=jnp.float32)
    middle = (tokens.astype(jnp.float32) + mixed.reshape(IMG_ROWS, IMG_COLS, C) + proj_bias[block]).astype(jnp.bfloat16)

    def feed(band):
        normed_two = layer_norm(band, norm_gain[block, 1], norm_shift[block, 1])
        inner = jnp.dot(normed_two.reshape(-1, C), fc1_weight[block], preferred_element_type=jnp.float32)
        hidden = jax.nn.gelu(inner + fc1_bias[block], approximate=False).astype(jnp.bfloat16)
        outer = jnp.dot(hidden, fc2_weight[block], preferred_element_type=jnp.float32).reshape(band.shape)
        return (band.astype(jnp.float32) + outer + fc2_bias[block]).astype(jnp.bfloat16)
    result = lax.map(feed, middle.reshape(IMG_ROWS // WIN, WIN, IMG_COLS, C))
    return result.reshape(IMG_ROWS, IMG_COLS, C)

def reference(image_tokens, labels, rel_index, norm_gain, norm_shift, qkv_weight, qkv_bias, bias_table, proj_weight, proj_bias, fc1_weight, fc1_bias, fc2_weight, fc2_bias):
    grid_rows = jnp.arange(IMG_ROWS, dtype=jnp.int32)
    grid_cols = jnp.arange(IMG_COLS, dtype=jnp.int32)
    region = labels * 4 + (grid_rows < SHIFT).astype(jnp.int32)[:, None] * 2 + (grid_cols < SHIFT).astype(jnp.int32)[None, :]
    current = image_tokens
    for block in range(BLOCKS):
        if block % 2 == 1:
            current = swin_block(current, block, region, SHIFT, norm_gain, norm_shift, qkv_weight, qkv_bias, bias_table, proj_weight, proj_bias, fc1_weight, fc1_bias, fc2_weight, fc2_bias, rel_index)
        else:
            current = swin_block(current, block, None, 0, norm_gain, norm_shift, qkv_weight, qkv_bias, bias_table, proj_weight, proj_bias, fc1_weight, fc1_bias, fc2_weight, fc2_bias, rel_index)
    return current
```

```python
import math

import jax
import jax.numpy as jnp
from jax import lax
from jax.experimental import pallas as pl
from jax.experimental.pallas import tpu as pltpu
from jax.sharding import PartitionSpec as P

WIN = 8
SHIFT = 4
EPS = 1e-05
NEG = -1e30
LOG2E = math.log2(math.e)
BF = jnp.bfloat16
F32 = jnp.float32


def dot_nt(a, b):
    return lax.dot_general(a, b, (((1,), (1,)), ((), ())), preferred_element_type=F32)


def dot_nn(a, b):
    return lax.dot_general(a, b, (((1,), (0,)), ((), ())), preferred_element_type=F32)


def layer_norm(x, gain, shift):
    center = x - jnp.mean(x, axis=-1, keepdims=True)
    spread = jnp.mean(center * center, axis=-1, keepdims=True)
    return (center * lax.rsqrt(spread + EPS) * gain + shift).astype(BF)


def gelu(v):
    half = 0.5 * v
    return half + half * lax.erf(v * math.sqrt(0.5))


def head_masks(heads, depth, width):
    lane = lax.broadcasted_iota(jnp.int32, (WIN * WIN, width), 1)
    return [(lane // depth == h).astype(F32).astype(BF) for h in range(heads)]


def stack_heads(rows, masks):
    return jnp.concatenate([rows * mask for mask in masks], axis=0)


def attend(q, k, v, bias, allowed, masks, ones):
    scores = dot_nt(q, stack_heads(k, masks)) + bias
    if allowed is not None:
        scores = jnp.where(allowed, scores, NEG)
    lanes = 128
    first = lax.broadcasted_iota(jnp.int32, (q.shape[0], lanes), 1) < WIN * WIN
    parts = []
    for start in range(0, scores.shape[1], lanes):
        s = scores[:, start : start + lanes]
        low = jnp.max(jnp.where(first, s, NEG), axis=-1, keepdims=True)
        high = jnp.max(jnp.where(first, NEG, s), axis=-1, keepdims=True)
        parts.append(jnp.exp2(s - jnp.where(first, low, high)).astype(BF))
    weights = jnp.concatenate(parts, axis=1)
    rhs = jnp.concatenate([stack_heads(v, masks), ones], axis=1)
    summed = dot_nn(weights, rhs)
    width = v.shape[1]
    return summed[:, :width] / summed[:, width:]


def pick(table, index):
    rows = index.shape[0]
    wide = jnp.concatenate([index, index], axis=1)
    low_index = jnp.minimum(wide, 127)
    high_index = jnp.maximum(wide - 128, 0)
    in_low = wide < 128
    first = lax.broadcasted_iota(jnp.int32, wide.shape, 1) < index.shape[1]

    def of_head(h):
        low = jnp.broadcast_to(table[h : h + 1, :128], (rows, 128))
        high = jnp.broadcast_to(table[h : h + 1, 128:], (rows, 128))
        return jnp.where(
            in_low,
            jnp.take_along_axis(low, low_index, axis=1),
            jnp.take_along_axis(high, high_index, axis=1),
        )

    return jnp.concatenate(
        [jnp.where(first, of_head(h), of_head(h + 1)) for h in range(0, table.shape[0], 2)], axis=1
    )


def mlp(middle, gain, shift, fc1, fc1_bias, fc2, fc2_bias):
    normed = layer_norm(middle, gain, shift)
    hidden = gelu(dot_nt(normed, fc1) + fc1_bias).astype(BF)
    return middle + dot_nn(hidden, fc2) + fc2_bias


def split_qkv(normed, wqkv, qkv_bias, scale):
    c = normed.shape[1]
    product = dot_nt(normed, wqkv) + qkv_bias
    if product.shape[1] == 3 * c:
        return (
            (product[:, :c] * scale).astype(BF),
            product[:, c : 2 * c].astype(BF),
            product[:, 2 * c :].astype(BF),
        )
    return product[:, :c].astype(BF), product[:, c:].astype(BF)


def regular_kernel(
    x_ref, left_ref, right_ref, rel_ref, table_ref, wqkv_ref, proj_ref, fc1_ref, fc2_ref,
    gain_ref, shift_ref, qkvb_ref, projb_ref, fc1b_ref, fc2b_ref, top_ref, bottom_ref, bias_ref,
):
    c = x_ref.shape[2]
    heads = table_ref.shape[0]
    depth = c // heads
    tokens = WIN * WIN
    scale = depth ** (-0.5) * LOG2E
    masks = head_masks(heads, depth, c)
    ones = jnp.concatenate(masks, axis=0)
    bias_ref[...] = pick(table_ref[...] * LOG2E, rel_ref[...])

    def run(x):
        q, k, v = split_qkv(
            layer_norm(x, gain_ref[0:1], shift_ref[0:1]), wqkv_ref[...], qkvb_ref[...], scale
        )
        outs = []
        for w in range(x.shape[0] // tokens):
            at = slice(w * tokens, (w + 1) * tokens)
            outs.append(attend(q[at], k[at], v[at], bias_ref[...], None, masks, ones))
        attended = jnp.concatenate(outs, axis=0).astype(BF)
        middle = x + dot_nn(attended, proj_ref[...]) + projb_ref[...]
        middle = middle.astype(BF).astype(F32)
        return mlp(
            middle, gain_ref[1:2], shift_ref[1:2], fc1_ref[...], fc1b_ref[...], fc2_ref[...], fc2b_ref[...]
        )

    group = 4

    def step(i, carry):
        start = pl.multiple_of(i * group * WIN, group * WIN)
        block = x_ref[:, pl.ds(start, group * WIN), :].astype(F32)
        x = jnp.concatenate(
            [block[r, w * WIN : (w + 1) * WIN] for w in range(group) for r in range(WIN)], axis=0
        )
        out = run(x)
        for r in range(WIN):
            row = jnp.concatenate(
                [out[w * tokens + r * WIN : w * tokens + (r + 1) * WIN] for w in range(group)], axis=0
            ).astype(BF)
            target = top_ref if r < SHIFT else bottom_ref
            target[r % SHIFT, pl.ds(start, group * WIN), :] = row
        return carry

    lax.fori_loop(0, x_ref.shape[1] // (group * WIN), step, 0)
    left = left_ref[...].astype(F32).reshape(tokens, c)
    right = right_ref[...].astype(F32).reshape(tokens, c)
    out = run(jnp.concatenate([left, right], axis=0))
    first = lax.broadcasted_iota(jnp.int32, (tokens, c), 0) % WIN < SHIFT
    edge = jnp.where(first, out[tokens:], out[:tokens])
    cols = x_ref.shape[1]
    for r in range(WIN):
        target = top_ref if r < SHIFT else bottom_ref
        target[r % SHIFT, cols : cols + WIN, :] = edge[r * WIN : (r + 1) * WIN].astype(BF)


def shifted_kernel(
    top_ref, bottom_ref, above_ref, below_ref, region_ref, rel_ref, table_ref, wqkv_ref, proj_ref,
    fc1_ref, fc2_ref, gain_ref, shift_ref, qkvb_ref, projb_ref, fc1b_ref, fc2b_ref, out_ref,
    bias_ref, own_ref, halo_ref, res_ref, *, group,
):
    c = top_ref.shape[2]
    cols = out_ref.shape[1]
    heads = table_ref.shape[0]
    depth = c // heads
    half = SHIFT * WIN
    tokens = WIN * WIN
    scale = depth ** (-0.5) * LOG2E
    masks = head_masks(heads, depth, c)
    ones = jnp.concatenate(masks, axis=0)
    bias_ref[...] = pick(table_ref[...] * LOG2E, rel_ref[...])
    for dst, srcs in ((own_ref, (top_ref, bottom_ref)), (halo_ref, (above_ref, below_ref))):
        for s, src in enumerate(srcs):
            value = src[...].astype(F32)
            edge = value[:, cols:]
            dst[s * SHIFT : (s + 1) * SHIFT, 0:WIN, :] = edge
            dst[s * SHIFT : (s + 1) * SHIFT, WIN : WIN + cols, :] = value[:, :cols]
            dst[s * SHIFT : (s + 1) * SHIFT, WIN + cols :, :] = edge
    first = lax.broadcasted_iota(jnp.int32, (WIN, group * WIN, c), 1) % WIN < SHIFT

    def step(i, carry):
        start = pl.multiple_of(i * group * WIN, WIN)

        def gather(ref):
            before = ref[:, pl.ds(start, group * WIN), :]
            after = ref[:, pl.ds(start + WIN, group * WIN), :]
            both = jnp.where(first, after, before)
            return jnp.concatenate(
                [
                    both[s * SHIFT + r, w * WIN : (w + 1) * WIN]
                    for w in range(group) for s in range(2) for r in range(SHIFT)
                ],
                axis=0,
            )

        x = gather(own_ref)
        gain, shift = gain_ref[0:1], shift_ref[0:1]
        q, k_own, v_own = split_qkv(layer_norm(x, gain, shift), wqkv_ref[...], qkvb_ref[...], scale)
        k_halo, v_halo = split_qkv(
            layer_norm(gather(halo_ref), gain, shift), wqkv_ref[c:], qkvb_ref[:, c:], scale
        )
        outs = []
        for w in range(group):
            ids = region_ref[i * group + w]
            key_ids = ids[:, :tokens * 2]
            for s in range(2):
                at = slice((w * 2 + s) * half, (w * 2 + s + 1) * half)
                k = jnp.concatenate([k_own[at], k_halo[at]], axis=0)
                v = jnp.concatenate([v_own[at], v_halo[at]], axis=0)
                row = ids[s : s + 1, :]
                keys = jnp.concatenate([row, row], axis=1)
                square = jnp.broadcast_to(row, (2 * tokens, 2 * tokens)).T[:half]
                allowed = jnp.concatenate([square, square], axis=1) == keys
                outs.append(
                    attend(q[at], k, v, bias_ref[s * half : (s + 1) * half], allowed, masks, ones)
                )
        attended = jnp.concatenate(outs, axis=0).astype(BF)
        middle = x + dot_nn(attended, proj_ref[...]) + projb_ref[...]
        middle = middle.astype(BF).astype(F32)
        out = mlp(
            middle, gain_ref[1:2], shift_ref[1:2], fc1_ref[...], fc1b_ref[...], fc2_ref[...], fc2b_ref[...]
        )
        for r in range(WIN):
            s, a = r // SHIFT, r % SHIFT
            res_ref[r, pl.ds(start, group * WIN), :] = jnp.concatenate(
                [
                    out[(w * 2 + s) * half + a * WIN : (w * 2 + s) * half + (a + 1) * WIN]
                    for w in range(group)
                ],
                axis=0,
            )
        return carry

    lax.fori_loop(0, (cols + WIN) // (group * WIN), step, 0)
    low = lax.broadcasted_iota(jnp.int32, (WIN, cols, c), 1) % WIN < SHIFT
    out_ref[...] = jnp.where(low, res_ref[:, 0:cols, :], res_ref[:, WIN : WIN + cols, :]).astype(BF)


def call(kernel, out_shapes, scratch, *args):
    return pl.pallas_call(
        kernel,
        out_shape=out_shapes,
        scratch_shapes=scratch,
        compiler_params=pltpu.CompilerParams(vmem_limit_bytes=48 * 1024 * 1024),
    )(*args)


def neighbours(axis, by):
    size = lax.axis_size(axis)
    return [(i, i + by) for i in range(size) if 0 <= i + by < size]


def padded(shard, sides, width):
    for axis, dim in sides:
        length = shard.shape[dim]
        last = lax.slice_in_dim(shard, length - width, length, axis=dim)
        leading = lax.slice_in_dim(shard, 0, width, axis=dim)
        before = lax.ppermute(last, axis, neighbours(axis, 1))
        after = lax.ppermute(leading, axis, neighbours(axis, -1))
        shard = jnp.concatenate([before, shard, after], axis=dim)
    return shard


def on_device(
    image_tokens, labels, rel_index, norm_gain, norm_shift, qkv_weight, qkv_bias, bias_table,
    proj_weight, proj_bias, fc1_weight, fc1_bias, fc2_weight, fc2_bias,
):
    own_rows, tile_cols, c = image_tokens.shape
    groups = lax.axis_size("ch")
    swap = [(i, (i + 1) % groups) for i in range(groups)]
    blocks, _, _, part = qkv_weight.shape
    hidden = fc1_weight.shape[2]
    entries = bias_table.shape[1]
    own_heads = bias_table.shape[2]

    def others(value):
        found = [value]
        for _ in range(groups - 1):
            found.append(lax.ppermute(found[-1], "ch", swap))
        return found

    weights = []
    for b in range(blocks):
        packed = jnp.concatenate(
            [
                qkv_weight[b].transpose(0, 2, 1).reshape(3 * part, c),
                proj_weight[b],
                fc1_weight[b].T,
                fc2_weight[b],
            ],
            axis=0,
        )
        weights.append(others(packed))
    tables = jnp.pad(bias_table.transpose(0, 2, 1), ((0, 0), (0, 0), (0, 256 - entries)))
    flat = jnp.concatenate([qkv_bias.reshape(-1), fc1_bias.reshape(-1), tables.reshape(-1)])
    small = [v.reshape(-1) for v in others(flat.reshape(-1, 128))]

    def full(b):
        got = weights[b]
        at = 0

        def take(rows):
            nonlocal at
            out = [g[at : at + rows] for g in got]
            at += rows
            return out

        qkv = jnp.concatenate([g.reshape(3, part, c) for g in take(3 * part)], axis=1).reshape(-1, c)
        proj = jnp.concatenate(take(part), axis=0)
        fc1 = jnp.concatenate(take(hidden), axis=0)
        fc2 = jnp.concatenate(take(hidden), axis=0)
        nq, nf = qkv_bias.size, fc1_bias.size
        qkvb = jnp.concatenate([s[:nq].reshape(blocks, 3, part)[b] for s in small], axis=1)
        fc1b = jnp.concatenate([s[nq : nq + nf].reshape(blocks, hidden)[b] for s in small], axis=0)
        table = jnp.concatenate(
            [s[nq + nf :].reshape(blocks, own_heads, 256)[b] for s in small], axis=0
        )
        return (
            table, qkv, proj, fc1, fc2, norm_gain[b], norm_shift[b], qkvb.reshape(1, -1),
            proj_bias[b][None], fc1b[None], fc2_bias[b][None],
        )

    left = lax.ppermute(image_tokens[:, tile_cols - WIN :], "col", neighbours("col", 1))
    right = lax.ppermute(image_tokens[:, :WIN], "col", neighbours("col", -1))

    margin = padded(labels, (("col", 1), (("row", "ch"), 0)), SHIFT)
    first_row = (lax.axis_index("row") * groups + lax.axis_index("ch")) * own_rows
    image_rows = own_rows * groups * lax.axis_size("row")
    image_cols = tile_cols * lax.axis_size("col")
    grid_rows = jnp.mod(first_row - SHIFT + jnp.arange(own_rows + 2 * SHIFT), image_rows)
    grid_cols = jnp.mod(
        lax.axis_index("col") * tile_cols - SHIFT + jnp.arange(tile_cols + 2 * SHIFT), image_cols
    )
    region = margin * 4 + (grid_rows < SHIFT)[:, None] * 2 + (grid_cols < SHIFT)[None, :]
    wins = tile_cols // WIN + 1
    half = SHIFT * WIN
    cells = region.reshape(4, SHIFT, wins, 2, SHIFT)[:, :, :, ::-1, :]
    cells = cells.transpose(2, 0, 1, 3, 4).reshape(wins, 4, half)
    order = jnp.stack(
        [
            jnp.concatenate([cells[:, 1], cells[:, 0]], axis=1),
            jnp.concatenate([cells[:, 2], cells[:, 3]], axis=1),
        ],
        axis=1,
    )
    order = jnp.concatenate([order, order], axis=2).astype(F32)

    rel = rel_index.reshape(2, SHIFT, 2, SHIFT, 2, SHIFT, 2, SHIFT)[:, :, ::-1, :, :, :, ::-1, :]
    rel = rel.reshape(2, half, 2, half)
    rel_shifted = jnp.concatenate(
        [
            jnp.concatenate([rel[1, :, 1], rel[1, :, 0]], axis=1),
            jnp.concatenate([rel[0, :, 0], rel[0, :, 1]], axis=1),
        ],
        axis=0,
    )

    strip = jax.ShapeDtypeStruct((SHIFT, tile_cols + WIN, c), BF)
    tokens = WIN * WIN
    heads = own_heads * groups
    bias_scratch = pltpu.VMEM((tokens, heads * tokens), F32)
    top, bottom = call(
        regular_kernel, (strip, strip), [bias_scratch], image_tokens, left, right, rel_index, *full(0)
    )
    above = lax.ppermute(bottom, ("row", "ch"), neighbours(("row", "ch"), 1))
    below = lax.ppermute(top, ("row", "ch"), neighbours(("row", "ch"), -1))
    group = max(g for g in range(1, 5) if wins % g == 0)
    wide = pltpu.VMEM((WIN, tile_cols + 2 * WIN, c), F32)
    return call(
        lambda *refs: shifted_kernel(*refs, group=group),
        jax.ShapeDtypeStruct(image_tokens.shape, BF),
        [bias_scratch, wide, wide, pltpu.VMEM((WIN, tile_cols + WIN, c), F32)],
        top, bottom, above, below, order, rel_shifted, *full(1),
    )


def solution(mesh):
    in_specs = (
        P(("row", "ch"), "col", None),
        P(("row", "ch"), "col"),
        P(),
        P(),
        P(),
        P(None, None, None, "ch"),
        P(None, None, "ch"),
        P(None, None, "ch"),
        P(None, "ch", None),
        P(),
        P(None, None, "ch"),
        P(None, "ch"),
        P(None, "ch", None),
        P(),
    )
    out_specs = P(("row", "ch"), "col", None)
    return jax.shard_map(
        on_device, mesh=mesh, in_specs=in_specs, out_specs=out_specs, check_vma=False
    )
```

```python
import math

import jax
import jax.numpy as jnp
from jax import lax
from jax.experimental import pallas as pl
from jax.experimental.pallas import tpu as pltpu
from jax.sharding import PartitionSpec as P

WIN = 8
SHIFT = 4
EPS = 1e-05
NEG = -1e30
LOG2E = math.log2(math.e)
BF = jnp.bfloat16
F32 = jnp.float32


def dot_nt(a, b):
    return lax.dot_general(a, b, (((1,), (1,)), ((), ())), preferred_element_type=F32)


def dot_nn(a, b):
    return lax.dot_general(a, b, (((1,), (0,)), ((), ())), preferred_element_type=F32)


def layer_norm(x, gain, shift):
    center = x - jnp.mean(x, axis=-1, keepdims=True)
    spread = jnp.mean(center * center, axis=-1, keepdims=True)
    return (center * lax.rsqrt(spread + EPS) * gain + shift).astype(BF)


def gelu(v):
    half = 0.5 * v
    return half + half * lax.erf(v * math.sqrt(0.5))


def head_masks(heads, depth, width):
    lane = lax.broadcasted_iota(jnp.int32, (WIN * WIN, width), 1)
    return [(lane // depth == h).astype(F32).astype(BF) for h in range(heads)]


def stack_heads(rows, masks):
    return jnp.concatenate([rows * mask for mask in masks], axis=0)


def attend(q, k, v, bias, allowed, masks, ones):
    scores = dot_nt(q, stack_heads(k, masks)) + bias
    if allowed is not None:
        scores = jnp.where(allowed, scores, NEG)
    lanes = 128
    first = lax.broadcasted_iota(jnp.int32, (q.shape[0], lanes), 1) < WIN * WIN
    parts = []
    for start in range(0, scores.shape[1], lanes):
        s = scores[:, start : start + lanes]
        low = jnp.max(jnp.where(first, s, NEG), axis=-1, keepdims=True)
        high = jnp.max(jnp.where(first, NEG, s), axis=-1, keepdims=True)
        parts.append(jnp.exp2(s - jnp.where(first, low, high)).astype(BF))
    weights = jnp.concatenate(parts, axis=1)
    rhs = jnp.concatenate([stack_heads(v, masks), ones], axis=1)
    summed = dot_nn(weights, rhs)
    width = v.shape[1]
    return summed[:, :width] / summed[:, width:]


def pick(low_rows, high_rows, skip, wide):
    rows = wide.shape[0]
    in_low = wide < 128
    low_index = jnp.minimum(wide, 127)
    high_index = jnp.maximum(wide - skip, 0)
    first = lax.broadcasted_iota(jnp.int32, wide.shape, 1) < WIN * WIN

    def of_head(h):
        low = jnp.broadcast_to(low_rows[h] * LOG2E, (rows, 128))
        high = jnp.broadcast_to(high_rows[h] * LOG2E, (rows, 128))
        return jnp.where(
            in_low,
            jnp.take_along_axis(low, low_index, axis=1),
            jnp.take_along_axis(high, high_index, axis=1),
        )

    return jnp.concatenate(
        [jnp.where(first, of_head(h), of_head(h + 1)) for h in range(0, len(low_rows), 2)], axis=1
    )


def split3(value):
    high = value.astype(BF)
    rest = value - high.astype(F32)
    middle = rest.astype(BF)
    return [high, middle, (rest - middle.astype(F32)).astype(BF)]


QKVB, FC1B, TABLE = 0, 3, 5
GAIN, SHIFTS, PROJB, FC2B = 9, 11, 13, 14
SMALL = 16


def pack_kernel(*refs, count):
    hbm, refs = refs[:count], refs[count:]
    (w0_ref, w1_ref, left_ref, right_ref, rel2_ref), refs = refs[:5], refs[5:]
    staged, small_ref, sems = refs[:count], refs[count], refs[count + 1]
    cols = hbm[0].shape[1]
    edge = 2 * WIN
    copies = [
        pltpu.make_async_copy(hbm[0].at[:, 0:edge], staged[0].at[0], sems.at[0]),
        pltpu.make_async_copy(hbm[0].at[:, cols - edge : cols], staged[0].at[1], sems.at[count]),
    ]
    copies += [pltpu.make_async_copy(hbm[k], staged[k], sems.at[k]) for k in range(1, count)]
    for copy in copies:
        copy.start()
    for copy in copies:
        copy.wait()
    (x, labels, rel, gain, shift, qkv, qkvb, table, proj, projb, fc1, fc1b, fc2, fc2b) = staged
    c = x.shape[3]
    part = qkv.shape[3]
    hidden = fc1.shape[2]
    entries = table.shape[1]
    for b, out in enumerate((w0_ref, w1_ref)):
        at = 0
        for m in range(3):
            out[at : at + part, :] = qkv[b, m].astype(F32).T.astype(BF)
            at += part
        out[at : at + part, :] = proj[b]
        at += part
        for start in range(0, hidden, 128):
            out[at : at + c, :] = fc1[b, :, start : start + 128]
            at += c
        out[at : at + hidden, :] = fc2[b]
        at += hidden
        small_ref[...] = jnp.zeros_like(small_ref)
        small_ref[QKVB : QKVB + 3, 0:part] = qkvb[b]
        for k in range(hidden // 128):
            small_ref[FC1B + k : FC1B + k + 1, :] = fc1b[b : b + 1, k * 128 : (k + 1) * 128]
        k = TABLE
        for h in range(table.shape[2]):
            for first in (0, entries - 128):
                column = table[b, first : first + 128, h : h + 1]
                small_ref[k : k + 1, :] = jnp.broadcast_to(column, (128, 128)).T[0:1]
                k += 1
        small_ref[GAIN : GAIN + 2, :] = gain[b]
        small_ref[SHIFTS : SHIFTS + 2, :] = shift[b]
        small_ref[PROJB : PROJB + 1, :] = projb[b : b + 1, :]
        small_ref[FC2B : FC2B + 1, :] = fc2b[b : b + 1, :]
        for piece in split3(small_ref[...]):
            out[at : at + SMALL, :] = piece
            at += SMALL
    ids = (labels[...] + 1).astype(F32).astype(BF)
    for r in range(WIN):
        left_ref[r] = x[0, r, 0:WIN]
        right_ref[r] = x[1, r, WIN:]
    left_ref[WIN] = ids[:, 0:128]
    right_ref[WIN] = ids[:, cols - 128 : cols]
    rel2_ref[...] = jnp.concatenate([rel[...], rel[...]], axis=1)


class Weights:

    def __init__(self, packs, scratch, c, part, hidden):
        self.qkv, self.proj, self.fc1, self.fc2 = scratch
        self.c = c
        self.packs = packs
        self.part, self.hidden = part, hidden
        self.start_small = 4 * part + (hidden // 128) * c + hidden

    def small(self, row, rows=1, width=128):
        out = []
        for p in self.packs:
            at = self.start_small
            value = sum(
                p[at + k * SMALL : at + (k + 1) * SMALL, :].astype(F32) for k in range(3)
            )
            out.append(value[row : row + rows, :width])
        return out

    def load(self):
        c, part, hidden = self.c, self.part, self.hidden
        for m in range(3):
            rows = jnp.concatenate([p[m * part : (m + 1) * part, :] for p in self.packs], axis=0)
            self.qkv[:, m * c : (m + 1) * c] = rows.astype(F32).T.astype(BF)
        for g, p in enumerate(self.packs):
            at = 3 * part
            self.proj[g * part : (g + 1) * part, :] = p[at : at + part, :]
            at += part
            for k in range(hidden // 128):
                lane = g * hidden + k * 128
                self.fc1[:, lane : lane + 128] = p[at : at + c, :]
                at += c
            self.fc2[g * hidden : (g + 1) * hidden, :] = p[at : at + hidden, :]
        self.gain = [self.small(GAIN + k)[0] for k in range(2)]
        self.shift = [self.small(SHIFTS + k)[0] for k in range(2)]
        self.proj_bias = self.small(PROJB)[0]
        self.fc2_bias = self.small(FC2B)[0]
        self.qkv_bias = jnp.concatenate(
            [v for m in range(3) for v in self.small(QKVB + m, width=part)], axis=1
        )
        rows = [self.small(FC1B + k) for k in range(hidden // 128)]
        self.fc1_bias = jnp.concatenate(
            [row[g] for g in range(len(self.packs)) for row in rows], axis=1
        )

    def bias(self, own_heads, skip, wide):
        rows = [self.small(TABLE + k) for k in range(2 * own_heads)]
        low = [rows[2 * h][g] for g in range(len(self.packs)) for h in range(own_heads)]
        high = [rows[2 * h + 1][g] for g in range(len(self.packs)) for h in range(own_heads)]
        return pick(low, high, skip, wide)

    def queries(self, x, scale):
        c = self.c
        product = dot_nn(layer_norm(x, self.gain[0], self.shift[0]), self.qkv[...]) + self.qkv_bias
        return (
            (product[:, :c] * scale).astype(BF),
            product[:, c : 2 * c].astype(BF),
            product[:, 2 * c :].astype(BF),
        )

    def keys(self, x):
        c = self.c
        normed = layer_norm(x, self.gain[0], self.shift[0])
        product = dot_nn(normed, self.qkv[:, c:]) + self.qkv_bias[:, c:]
        return product[:, :c].astype(BF), product[:, c:].astype(BF)

    def finish(self, x, attended):
        middle = x + dot_nn(attended, self.proj[...]) + self.proj_bias
        middle = middle.astype(BF).astype(F32)
        normed = layer_norm(middle, self.gain[1], self.shift[1])
        hidden = gelu(dot_nn(normed, self.fc1[...]) + self.fc1_bias).astype(BF)
        return middle + dot_nn(hidden, self.fc2[...]) + self.fc2_bias


def regular_kernel(
    x_ref, left_ref, right_ref, labels_ref, rel_ref, *refs, groups, own_heads, entries, part, hidden
):
    packs, refs = refs[:groups], refs[groups:]
    (top_ref, bottom_ref, bias_ref), scratch = refs[:3], refs[3:]
    c = x_ref.shape[2]
    cols = x_ref.shape[1]
    heads = own_heads * groups
    depth = c // heads
    tokens = WIN * WIN
    scale = depth ** (-0.5) * LOG2E
    w = Weights(packs, scratch, c, part, hidden)
    w.load()
    masks = head_masks(heads, depth, c)
    ones = jnp.concatenate(masks, axis=0)
    bias_ref[...] = w.bias(own_heads, entries - 128, rel_ref[...])

    lanes = jnp.concatenate(
        [
            left_ref[WIN].astype(F32),
            (labels_ref[...] + 1).astype(F32),
            right_ref[WIN].astype(F32),
        ],
        axis=1,
    )
    span = lanes.shape[1]
    lane = lax.broadcasted_iota(jnp.int32, (WIN, span), 1)
    match = lane % WIN == lax.broadcasted_iota(jnp.int32, (WIN, span), 0)
    spread = jnp.concatenate(
        [jnp.where(match, lanes[r : r + 1], 0.0) for r in range(WIN)], axis=0
    ).astype(BF)
    source = lax.broadcasted_iota(jnp.int32, (span, 128), 0)
    window = lax.broadcasted_iota(jnp.int32, (span, 128), 1)
    chosen = ((source - 128 + SHIFT) // WIN == window) & (source >= 128 - SHIFT)
    ids = dot_nn(spread, chosen.astype(F32).astype(BF))
    for r in range(WIN):
        target = top_ref if r < SHIFT else bottom_ref
        target[r % SHIFT, cols + WIN :, :] = ids[r * WIN : (r + 1) * WIN].astype(BF)

    def run(x):
        q, k, v = w.queries(x, scale)
        outs = []
        for n in range(x.shape[0] // tokens):
            at = slice(n * tokens, (n + 1) * tokens)
            outs.append(attend(q[at], k[at], v[at], bias_ref[...], None, masks, ones))
        return w.finish(x, jnp.concatenate(outs, axis=0).astype(BF))

    group = 4

    def step(i, carry):
        start = pl.multiple_of(i * group * WIN, group * WIN)
        block = x_ref[:, pl.ds(start, group * WIN), :].astype(F32)
        x = jnp.concatenate(
            [block[r, n * WIN : (n + 1) * WIN] for n in range(group) for r in range(WIN)], axis=0
        )
        out = run(x)
        for r in range(WIN):
            row = jnp.concatenate(
                [out[n * tokens + r * WIN : n * tokens + (r + 1) * WIN] for n in range(group)], axis=0
            ).astype(BF)
            target = top_ref if r < SHIFT else bottom_ref
            target[r % SHIFT, pl.ds(start, group * WIN), :] = row
        return carry

    lax.fori_loop(0, cols // (group * WIN), step, 0)
    left = left_ref[0:WIN].astype(F32).reshape(tokens, c)
    right = right_ref[0:WIN].astype(F32).reshape(tokens, c)
    out = run(jnp.concatenate([left, right], axis=0))
    first = lax.broadcasted_iota(jnp.int32, (tokens, c), 0) % WIN < SHIFT
    edge = jnp.where(first, out[tokens:], out[:tokens])
    for r in range(WIN):
        target = top_ref if r < SHIFT else bottom_ref
        target[r % SHIFT, cols : cols + WIN, :] = edge[r * WIN : (r + 1) * WIN].astype(BF)


def shifted_kernel(
    top_ref, bottom_ref, above_ref, below_ref, rel_ref, *refs,
    group, groups, own_heads, entries, part, hidden,
):
    packs, refs = refs[:groups], refs[groups:]
    (out_ref, bias_ref, own_ref, halo_ref, res_ref, qid_ref, kid_ref), scratch = refs[:7], refs[7:]
    c = top_ref.shape[2]
    cols = out_ref.shape[1]
    heads = own_heads * groups
    depth = c // heads
    half = SHIFT * WIN
    tokens = WIN * WIN
    scale = depth ** (-0.5) * LOG2E
    w = Weights(packs, scratch, c, part, hidden)
    w.load()
    masks = head_masks(heads, depth, c)
    ones = jnp.concatenate(masks, axis=0)

    rel = rel_ref[...]
    rel = jnp.concatenate(
        [
            jnp.concatenate([rel[a + SHIFT : a + WIN], rel[a : a + SHIFT]], axis=0)
            for a in range(0, tokens, WIN)
        ],
        axis=0,
    )
    lane = lax.broadcasted_iota(jnp.int32, rel.shape, 1)
    rel = jnp.where(lane % WIN < SHIFT, pltpu.roll(rel, 128 - SHIFT, 1), pltpu.roll(rel, SHIFT, 1))
    rel = jnp.concatenate([pltpu.roll(rel[half:], half, 1), rel[:half]], axis=0)
    bias_ref[...] = w.bias(own_heads, entries - 128, rel)

    for s, (own, halo) in enumerate(((top_ref, above_ref), (bottom_ref, below_ref))):
        parts = []
        for dst, src in ((own_ref, own), (halo_ref, halo)):
            value = src[...].astype(F32)
            edge = value[:, cols : cols + WIN]
            dst[s * SHIFT : (s + 1) * SHIFT, 0:WIN, :] = edge
            dst[s * SHIFT : (s + 1) * SHIFT, WIN : WIN + cols, :] = value[:, :cols]
            dst[s * SHIFT : (s + 1) * SHIFT, WIN + cols :, :] = edge
            parts.append(value[:, cols + WIN :].reshape(half, 128))
        qid_ref[s] = parts[0]
        both = jnp.concatenate(parts + parts, axis=0)
        kid_ref[s] = both.T
    first = lax.broadcasted_iota(jnp.int32, (WIN, group * WIN, c), 1) % WIN < SHIFT

    def step(i, carry):
        start = pl.multiple_of(i * group * WIN, WIN)

        def gather(ref):
            before = ref[:, pl.ds(start, group * WIN), :]
            after = ref[:, pl.ds(start + WIN, group * WIN), :]
            both = jnp.where(first, after, before)
            return jnp.concatenate(
                [
                    both[s * SHIFT + r, n * WIN : (n + 1) * WIN]
                    for n in range(group) for s in range(2) for r in range(SHIFT)
                ],
                axis=0,
            )

        x = gather(own_ref)
        q, k_own, v_own = w.queries(x, scale)
        k_halo, v_halo = w.keys(gather(halo_ref))
        outs = []
        for n in range(group):
            j = i * group + n
            for s in range(2):
                at = slice((n * 2 + s) * half, (n * 2 + s + 1) * half)
                k = jnp.concatenate([k_own[at], k_halo[at]], axis=0)
                v = jnp.concatenate([v_own[at], v_halo[at]], axis=0)
                keys = kid_ref[s, pl.ds(j, 1), :]
                queries = jnp.take_along_axis(qid_ref[s], jnp.full((half, 128), j, jnp.int32), axis=1)
                allowed = jnp.concatenate([queries, queries], axis=1) == jnp.concatenate(
                    [keys, keys], axis=1
                )
                outs.append(
                    attend(q[at], k, v, bias_ref[s * half : (s + 1) * half], allowed, masks, ones)
                )
        out = w.finish(x, jnp.concatenate(outs, axis=0).astype(BF))
        for r in range(WIN):
            s, a = r // SHIFT, r % SHIFT
            res_ref[r, pl.ds(start, group * WIN), :] = jnp.concatenate(
                [
                    out[(n * 2 + s) * half + a * WIN : (n * 2 + s) * half + (a + 1) * WIN]
                    for n in range(group)
                ],
                axis=0,
            )
        return carry

    lax.fori_loop(0, (cols + WIN) // (group * WIN), step, 0)
    low = lax.broadcasted_iota(jnp.int32, (WIN, cols, c), 1) % WIN < SHIFT
    out_ref[...] = jnp.where(low, res_ref[:, 0:cols, :], res_ref[:, WIN : WIN + cols, :]).astype(BF)


def call(kernel, out_shapes, scratch, *args, in_specs=None):
    specs = {} if in_specs is None else {"in_specs": in_specs}
    return pl.pallas_call(
        kernel,
        out_shape=out_shapes,
        scratch_shapes=scratch,
        compiler_params=pltpu.CompilerParams(vmem_limit_bytes=48 * 1024 * 1024),
        **specs,
    )(*args)


def neighbours(axis, by):
    size = lax.axis_size(axis)
    return [(i, i + by) for i in range(size) if 0 <= i + by < size]


def on_device(*args):
    image_tokens, labels, rel_index = args[:3]
    qkv_weight, bias_table, fc1_weight = args[5], args[7], args[10]
    tile_cols, c = image_tokens.shape[1:]
    groups = lax.axis_size("ch")
    swap = [(i, (i + 1) % groups) for i in range(groups)]
    part = qkv_weight.shape[3]
    hidden = fc1_weight.shape[2]
    entries = bias_table.shape[1]
    own_heads = bias_table.shape[2]
    tokens = WIN * WIN

    def others(value):
        found = [value]
        for _ in range(groups - 1):
            found.append(lax.ppermute(found[-1], "ch", swap))
        return found

    rows = 4 * part + (hidden // 128) * c + hidden + 3 * SMALL
    pack = jax.ShapeDtypeStruct((rows, 128), BF)
    edge = jax.ShapeDtypeStruct((WIN + 1, WIN, c), BF)
    staged = [pltpu.VMEM((2, WIN, 2 * WIN, c), BF)] + [pltpu.VMEM(a.shape, a.dtype) for a in args[1:]]
    own0, own1, left_edge, right_edge, rel2 = call(
        lambda *refs: pack_kernel(*refs, count=len(args)),
        (pack, pack, edge, edge, jax.ShapeDtypeStruct((tokens, 2 * tokens), jnp.int32)),
        staged + [pltpu.VMEM((SMALL, 128), F32), pltpu.SemaphoreType.DMA((len(args) + 1,))],
        *args,
        in_specs=[pl.BlockSpec(memory_space=pl.ANY)] * len(args),
    )
    packs0 = others(own0)
    left = lax.ppermute(right_edge, "col", neighbours("col", 1))
    right = lax.ppermute(left_edge, "col", neighbours("col", -1))
    packs1 = others(own1)

    sizes = dict(groups=groups, own_heads=own_heads, entries=entries, part=part, hidden=hidden)
    weights_scratch = [
        pltpu.VMEM((c, 3 * c), BF),
        pltpu.VMEM((c, c), BF),
        pltpu.VMEM((c, groups * hidden), BF),
        pltpu.VMEM((groups * hidden, c), BF),
    ]
    strip = jax.ShapeDtypeStruct((SHIFT, tile_cols + 2 * WIN, c), BF)
    bias_scratch = pltpu.VMEM((tokens, own_heads * groups * tokens), F32)
    top, bottom = call(
        lambda *refs: regular_kernel(*refs, **sizes),
        (strip, strip),
        [bias_scratch] + weights_scratch,
        image_tokens, left, right, labels, rel2, *packs0,
    )
    above = lax.ppermute(bottom, ("row", "ch"), neighbours(("row", "ch"), 1))
    below = lax.ppermute(top, ("row", "ch"), neighbours(("row", "ch"), -1))
    wins = tile_cols // WIN + 1
    group = max(g for g in range(1, 5) if wins % g == 0)
    wide = pltpu.VMEM((WIN, tile_cols + 2 * WIN, c), F32)
    return call(
        lambda *refs: shifted_kernel(*refs, group=group, **sizes),
        jax.ShapeDtypeStruct(image_tokens.shape, BF),
        [
            bias_scratch, wide, wide, pltpu.VMEM((WIN, tile_cols + WIN, c), F32),
            pltpu.VMEM((2, SHIFT * WIN, 128), F32), pltpu.VMEM((2, 128, 128), F32),
        ] + weights_scratch,
        top, bottom, above, below, rel2, *packs1,
    )


def solution(mesh):
    in_specs = (
        P(("row", "ch"), "col", None),
        P(("row", "ch"), "col"),
        P(),
        P(),
        P(),
        P(None, None, None, "ch"),
        P(None, None, "ch"),
        P(None, None, "ch"),
        P(None, "ch", None),
        P(),
        P(None, None, "ch"),
        P(None, "ch"),
        P(None, "ch", None),
        P(),
    )
    out_specs = P(("row", "ch"), "col", None)
    return jax.shard_map(
        on_device, mesh=mesh, in_specs=in_specs, out_specs=out_specs, check_vma=False
    )
```

```python
import math

import jax
import jax.numpy as jnp
from jax import lax
from jax.experimental import pallas as pl
from jax.experimental.pallas import tpu as pltpu
from jax.sharding import PartitionSpec as P


WIN = 8
SHIFT = 4
EPS = 1e-05
NEG = -1e30
LOG2E = math.log2(math.e)
BF = jnp.bfloat16
F32 = jnp.float32


def dot_nt(a, b):
    return lax.dot_general(a, b, (((1,), (1,)), ((), ())), preferred_element_type=F32)


def dot_nn(a, b):
    return lax.dot_general(a, b, (((1,), (0,)), ((), ())), preferred_element_type=F32)


def layer_norm(x, gain, shift):
    center = x - jnp.mean(x, axis=-1, keepdims=True)
    spread = jnp.mean(center * center, axis=-1, keepdims=True)
    return (center * lax.rsqrt(spread + EPS) * gain + shift).astype(BF)


def gelu(v):
    half = 0.5 * v
    return half + half * lax.erf(v * math.sqrt(0.5))


def head_masks(heads, depth, width):
    lane = lax.broadcasted_iota(jnp.int32, (WIN * WIN, width), 1)
    return [(lane // depth == h).astype(F32).astype(BF) for h in range(heads)]


def stack_heads(rows, masks):
    return jnp.concatenate([rows * mask for mask in masks], axis=0)


def attend(q, k, v, bias, allowed, masks, ones):
    scores = dot_nt(q, stack_heads(k, masks)) + bias
    if allowed is not None:
        scores = jnp.where(allowed, scores, NEG)
    lanes = 128
    first = lax.broadcasted_iota(jnp.int32, (q.shape[0], lanes), 1) < WIN * WIN
    parts = []
    for start in range(0, scores.shape[1], lanes):
        s = scores[:, start : start + lanes]
        low = jnp.max(jnp.where(first, s, NEG), axis=-1, keepdims=True)
        high = jnp.max(jnp.where(first, NEG, s), axis=-1, keepdims=True)
        parts.append(jnp.exp2(s - jnp.where(first, low, high)).astype(BF))
    weights = jnp.concatenate(parts, axis=1)
    rhs = jnp.concatenate([stack_heads(v, masks), ones], axis=1)
    summed = dot_nn(weights, rhs)
    width = v.shape[1]
    return summed[:, :width] / summed[:, width:]


def pick(low_rows, high_rows, skip, wide):
    rows = wide.shape[0]
    in_low = wide < 128
    low_index = jnp.minimum(wide, 127)
    high_index = jnp.maximum(wide - skip, 0)
    first = lax.broadcasted_iota(jnp.int32, wide.shape, 1) < WIN * WIN

    def of_head(h):
        low = jnp.broadcast_to(low_rows[h] * LOG2E, (rows, 128))
        high = jnp.broadcast_to(high_rows[h] * LOG2E, (rows, 128))
        return jnp.where(
            in_low,
            jnp.take_along_axis(low, low_index, axis=1),
            jnp.take_along_axis(high, high_index, axis=1),
        )

    return jnp.concatenate(
        [jnp.where(first, of_head(h), of_head(h + 1)) for h in range(0, len(low_rows), 2)], axis=1
    )


def split3(value):
    high = value.astype(BF)
    rest = value - high.astype(F32)
    middle = rest.astype(BF)
    return [high, middle, (rest - middle.astype(F32)).astype(BF)]


QKVB, FC1B, TABLE = 0, 3, 5
GAIN, SHIFTS, PROJB, FC2B = 9, 11, 13, 14
SMALL = 16


def pack_kernel(*refs, count):
    hbm, refs = refs[:count], refs[count:]
    (w0_ref, w1_ref, left_ref, right_ref, rel2_ref), refs = refs[:5], refs[5:]
    staged, small_ref, sems = refs[:count], refs[count], refs[count + 1]
    cols = hbm[0].shape[1]
    edge = 2 * WIN
    copies = [
        pltpu.make_async_copy(hbm[0].at[:, 0:edge], staged[0].at[0], sems.at[0]),
        pltpu.make_async_copy(hbm[0].at[:, cols - edge : cols], staged[0].at[1], sems.at[count]),
    ]
    copies += [pltpu.make_async_copy(hbm[k], staged[k], sems.at[k]) for k in range(1, count)]
    for copy in copies:
        copy.start()
    for copy in copies:
        copy.wait()
    (x, labels, rel, gain, shift, qkv, qkvb, table, proj, projb, fc1, fc1b, fc2, fc2b) = staged
    c = x.shape[3]
    part = qkv.shape[2]
    hidden = fc1.shape[2]
    entries = table.shape[2]
    for b, out in enumerate((w0_ref, w1_ref)):
        at = 0
        for m in range(3):
            out[at : at + part, :] = qkv[b, m]
            at += part
        out[at : at + part, :] = proj[b]
        at += part
        for start in range(0, hidden, 128):
            out[at : at + c, :] = fc1[b, :, start : start + 128]
            at += c
        out[at : at + hidden, :] = fc2[b]
        at += hidden
        small_ref[...] = jnp.zeros_like(small_ref)
        for m in range(3):
            small_ref[QKVB + m : QKVB + m + 1, 0:part] = qkvb[m, b : b + 1]
        for k in range(hidden // 128):
            small_ref[FC1B + k : FC1B + k + 1, :] = fc1b[b : b + 1, k * 128 : (k + 1) * 128]
        k = TABLE
        for h in range(table.shape[1]):
            for first in (0, entries - 128):
                small_ref[k : k + 1, :] = table[b, h : h + 1, first : first + 128]
                k += 1
        small_ref[GAIN : GAIN + 2, :] = gain[b]
        small_ref[SHIFTS : SHIFTS + 2, :] = shift[b]
        small_ref[PROJB : PROJB + 1, :] = projb[b : b + 1, :]
        small_ref[FC2B : FC2B + 1, :] = fc2b[b : b + 1, :]
        for piece in split3(small_ref[...]):
            out[at : at + SMALL, :] = piece
            at += SMALL
    ids = (labels[...] + 1).astype(F32).astype(BF)
    for r in range(WIN):
        left_ref[r] = x[0, r, 0:WIN]
        right_ref[r] = x[1, r, WIN:]
    left_ref[WIN] = ids[:, 0:128]
    right_ref[WIN] = ids[:, cols - 128 : cols]
    rel2_ref[...] = jnp.concatenate([rel[...], rel[...]], axis=1)


class Weights:

    def __init__(self, packs, scratch, c, part, hidden):
        self.qkv, self.proj, self.fc1, self.fc2 = scratch
        self.c = c
        self.packs = packs
        self.part, self.hidden = part, hidden
        self.start_small = 4 * part + (hidden // 128) * c + hidden

    def small(self, row, rows=1, width=128):
        out = []
        for p in self.packs:
            at = self.start_small
            value = sum(
                p[at + k * SMALL : at + (k + 1) * SMALL, :].astype(F32) for k in range(3)
            )
            out.append(value[row : row + rows, :width])
        return out

    def load(self):
        c, part, hidden = self.c, self.part, self.hidden
        for m in range(3):
            rows = jnp.concatenate([p[m * part : (m + 1) * part, :] for p in self.packs], axis=0)
            self.qkv[:, m * c : (m + 1) * c] = rows.astype(F32).T.astype(BF)
        for g, p in enumerate(self.packs):
            at = 3 * part
            self.proj[g * part : (g + 1) * part, :] = p[at : at + part, :]
            at += part
            for k in range(hidden // 128):
                lane = g * hidden + k * 128
                self.fc1[:, lane : lane + 128] = p[at : at + c, :]
                at += c
            self.fc2[g * hidden : (g + 1) * hidden, :] = p[at : at + hidden, :]
        self.gain = [self.small(GAIN + k)[0] for k in range(2)]
        self.shift = [self.small(SHIFTS + k)[0] for k in range(2)]
        self.proj_bias = self.small(PROJB)[0]
        self.fc2_bias = self.small(FC2B)[0]
        self.qkv_bias = jnp.concatenate(
            [v for m in range(3) for v in self.small(QKVB + m, width=part)], axis=1
        )
        rows = [self.small(FC1B + k) for k in range(hidden // 128)]
        self.fc1_bias = jnp.concatenate(
            [row[g] for g in range(len(self.packs)) for row in rows], axis=1
        )

    def bias(self, own_heads, skip, wide):
        rows = [self.small(TABLE + k) for k in range(2 * own_heads)]
        low = [rows[2 * h][g] for g in range(len(self.packs)) for h in range(own_heads)]
        high = [rows[2 * h + 1][g] for g in range(len(self.packs)) for h in range(own_heads)]
        return pick(low, high, skip, wide)

    def queries(self, x, scale):
        c = self.c
        product = dot_nn(layer_norm(x, self.gain[0], self.shift[0]), self.qkv[...]) + self.qkv_bias
        return (
            (product[:, :c] * scale).astype(BF),
            product[:, c : 2 * c].astype(BF),
            product[:, 2 * c :].astype(BF),
        )

    def keys(self, x):
        c = self.c
        normed = layer_norm(x, self.gain[0], self.shift[0])
        product = dot_nn(normed, self.qkv[:, c:]) + self.qkv_bias[:, c:]
        return product[:, :c].astype(BF), product[:, c:].astype(BF)

    def finish(self, x, attended):
        middle = x + dot_nn(attended, self.proj[...]) + self.proj_bias
        middle = middle.astype(BF).astype(F32)
        normed = layer_norm(middle, self.gain[1], self.shift[1])
        hidden = gelu(dot_nn(normed, self.fc1[...]) + self.fc1_bias).astype(BF)
        return middle + dot_nn(hidden, self.fc2[...]) + self.fc2_bias


def regular_kernel(
    x_hbm, labels_hbm, left_ref, right_ref, rel_ref, *refs, groups, own_heads, entries, part, hidden
):
    packs, refs = refs[:groups], refs[groups:]
    (top_ref, bottom_ref, bias_ref, x_ref, labels_ref, sems), scratch = refs[:6], refs[6:]
    x_copy = pltpu.make_async_copy(x_hbm, x_ref, sems.at[0])
    labels_copy = pltpu.make_async_copy(labels_hbm, labels_ref, sems.at[1])
    x_copy.start()
    labels_copy.start()
    c = x_ref.shape[2]
    cols = x_ref.shape[1]
    heads = own_heads * groups
    depth = c // heads
    tokens = WIN * WIN
    scale = depth ** (-0.5) * LOG2E
    w = Weights(packs, scratch, c, part, hidden)
    w.load()
    masks = head_masks(heads, depth, c)
    ones = jnp.concatenate(masks, axis=0)
    bias_ref[...] = w.bias(own_heads, entries - 128, rel_ref[...])

    labels_copy.wait()
    lanes = jnp.concatenate(
        [
            left_ref[WIN].astype(F32),
            (labels_ref[...] + 1).astype(F32),
            right_ref[WIN].astype(F32),
        ],
        axis=1,
    )
    span = lanes.shape[1]
    lane = lax.broadcasted_iota(jnp.int32, (WIN, span), 1)
    match = lane % WIN == lax.broadcasted_iota(jnp.int32, (WIN, span), 0)
    spread = jnp.concatenate(
        [jnp.where(match, lanes[r : r + 1], 0.0) for r in range(WIN)], axis=0
    ).astype(BF)
    source = lax.broadcasted_iota(jnp.int32, (span, 128), 0)
    window = lax.broadcasted_iota(jnp.int32, (span, 128), 1)
    chosen = ((source - 128 + SHIFT) // WIN == window) & (source >= 128 - SHIFT)
    ids = dot_nn(spread, chosen.astype(F32).astype(BF))
    for r in range(WIN):
        target = top_ref if r < SHIFT else bottom_ref
        target[r % SHIFT, cols + WIN :, :] = ids[r * WIN : (r + 1) * WIN].astype(BF)

    def run(x):
        q, k, v = w.queries(x, scale)
        outs = []
        for n in range(x.shape[0] // tokens):
            at = slice(n * tokens, (n + 1) * tokens)
            outs.append(attend(q[at], k[at], v[at], bias_ref[...], None, masks, ones))
        return w.finish(x, jnp.concatenate(outs, axis=0).astype(BF))

    group = 4

    def step(i, carry):
        start = pl.multiple_of(i * group * WIN, group * WIN)
        block = x_ref[:, pl.ds(start, group * WIN), :].astype(F32)
        x = jnp.concatenate(
            [block[r, n * WIN : (n + 1) * WIN] for n in range(group) for r in range(WIN)], axis=0
        )
        out = run(x)
        for r in range(WIN):
            row = jnp.concatenate(
                [out[n * tokens + r * WIN : n * tokens + (r + 1) * WIN] for n in range(group)], axis=0
            ).astype(BF)
            target = top_ref if r < SHIFT else bottom_ref
            target[r % SHIFT, pl.ds(start, group * WIN), :] = row
        return carry

    x_copy.wait()
    lax.fori_loop(0, cols // (group * WIN), step, 0)
    left = left_ref[0:WIN].astype(F32).reshape(tokens, c)
    right = right_ref[0:WIN].astype(F32).reshape(tokens, c)
    out = run(jnp.concatenate([left, right], axis=0))
    first = lax.broadcasted_iota(jnp.int32, (tokens, c), 0) % WIN < SHIFT
    edge = jnp.where(first, out[tokens:], out[:tokens])
    for r in range(WIN):
        target = top_ref if r < SHIFT else bottom_ref
        target[r % SHIFT, cols : cols + WIN, :] = edge[r * WIN : (r + 1) * WIN].astype(BF)


def shifted_kernel(
    top_ref, bottom_ref, above_ref, below_ref, rel_ref, *refs,
    group, groups, own_heads, entries, part, hidden,
):
    packs, refs = refs[:groups], refs[groups:]
    (out_ref, bias_ref, own_ref, halo_ref, res_ref, qid_ref, kid_ref), scratch = refs[:7], refs[7:]
    c = top_ref.shape[2]
    cols = out_ref.shape[1]
    heads = own_heads * groups
    depth = c // heads
    half = SHIFT * WIN
    tokens = WIN * WIN
    scale = depth ** (-0.5) * LOG2E
    w = Weights(packs, scratch, c, part, hidden)
    w.load()
    masks = head_masks(heads, depth, c)
    ones = jnp.concatenate(masks, axis=0)

    rel = rel_ref[...]
    rel = jnp.concatenate(
        [
            jnp.concatenate([rel[a + SHIFT : a + WIN], rel[a : a + SHIFT]], axis=0)
            for a in range(0, tokens, WIN)
        ],
        axis=0,
    )
    lane = lax.broadcasted_iota(jnp.int32, rel.shape, 1)
    rel = jnp.where(lane % WIN < SHIFT, pltpu.roll(rel, 128 - SHIFT, 1), pltpu.roll(rel, SHIFT, 1))
    rel = jnp.concatenate([pltpu.roll(rel[half:], half, 1), rel[:half]], axis=0)
    bias_ref[...] = w.bias(own_heads, entries - 128, rel)

    for s, (own, halo) in enumerate(((top_ref, above_ref), (bottom_ref, below_ref))):
        parts = []
        for dst, src in ((own_ref, own), (halo_ref, halo)):
            value = src[...].astype(F32)
            edge = value[:, cols : cols + WIN]
            dst[s * SHIFT : (s + 1) * SHIFT, 0:WIN, :] = edge
            dst[s * SHIFT : (s + 1) * SHIFT, WIN : WIN + cols, :] = value[:, :cols]
            dst[s * SHIFT : (s + 1) * SHIFT, WIN + cols :, :] = edge
            parts.append(value[:, cols + WIN :].reshape(half, 128))
        qid_ref[s] = parts[0]
        both = jnp.concatenate(parts + parts, axis=0)
        kid_ref[s] = both.T
    first = lax.broadcasted_iota(jnp.int32, (WIN, group * WIN, c), 1) % WIN < SHIFT

    def step(i, carry):
        start = pl.multiple_of(i * group * WIN, WIN)

        def gather(ref):
            before = ref[:, pl.ds(start, group * WIN), :]
            after = ref[:, pl.ds(start + WIN, group * WIN), :]
            both = jnp.where(first, after, before)
            return jnp.concatenate(
                [
                    both[s * SHIFT + r, n * WIN : (n + 1) * WIN]
                    for n in range(group) for s in range(2) for r in range(SHIFT)
                ],
                axis=0,
            )

        x = gather(own_ref)
        q, k_own, v_own = w.queries(x, scale)
        k_halo, v_halo = w.keys(gather(halo_ref))
        outs = []
        for n in range(group):
            j = i * group + n
            for s in range(2):
                at = slice((n * 2 + s) * half, (n * 2 + s + 1) * half)
                k = jnp.concatenate([k_own[at], k_halo[at]], axis=0)
                v = jnp.concatenate([v_own[at], v_halo[at]], axis=0)
                keys = kid_ref[s, pl.ds(j, 1), :]
                queries = jnp.take_along_axis(qid_ref[s], jnp.full((half, 128), j, jnp.int32), axis=1)
                allowed = jnp.concatenate([queries, queries], axis=1) == jnp.concatenate(
                    [keys, keys], axis=1
                )
                outs.append(
                    attend(q[at], k, v, bias_ref[s * half : (s + 1) * half], allowed, masks, ones)
                )
        out = w.finish(x, jnp.concatenate(outs, axis=0).astype(BF))
        for r in range(WIN):
            s, a = r // SHIFT, r % SHIFT
            res_ref[r, pl.ds(start, group * WIN), :] = jnp.concatenate(
                [
                    out[(n * 2 + s) * half + a * WIN : (n * 2 + s) * half + (a + 1) * WIN]
                    for n in range(group)
                ],
                axis=0,
            )
        return carry

    lax.fori_loop(0, (cols + WIN) // (group * WIN), step, 0)
    low = lax.broadcasted_iota(jnp.int32, (WIN, cols, c), 1) % WIN < SHIFT
    out_ref[...] = jnp.where(low, res_ref[:, 0:cols, :], res_ref[:, WIN : WIN + cols, :]).astype(BF)


def call(kernel, out_shapes, scratch, *args, in_specs=None):
    specs = {} if in_specs is None else {"in_specs": in_specs}
    return pl.pallas_call(
        kernel,
        out_shape=out_shapes,
        scratch_shapes=scratch,
        compiler_params=pltpu.CompilerParams(vmem_limit_bytes=48 * 1024 * 1024),
        **specs,
    )(*args)


def in_hbm(value):
    return pltpu.with_memory_space_constraint(value, pltpu.HBM)


def neighbours(axis, by):
    size = lax.axis_size(axis)
    return [(i, i + by) for i in range(size) if 0 <= i + by < size]


def both_blocks(*args):
    image_tokens, labels, _ = args[:3]
    qkv_weight, bias_table, fc1_weight = args[5], args[7], args[10]
    tile_cols, c = image_tokens.shape[1:]
    groups = lax.axis_size("ch")
    swap = [(i, (i + 1) % groups) for i in range(groups)]
    part = qkv_weight.shape[3]
    hidden = fc1_weight.shape[2]
    entries = bias_table.shape[1]
    own_heads = bias_table.shape[2]
    tokens = WIN * WIN

    def others(value):
        found = [value]
        for _ in range(groups - 1):
            found.append(lax.ppermute(found[-1], "ch", swap))
        return found

    rows = 4 * part + (hidden // 128) * c + hidden + 3 * SMALL
    pack = jax.ShapeDtypeStruct((rows, 128), BF)
    edge = jax.ShapeDtypeStruct((WIN + 1, WIN, c), BF)
    args = list(args)
    args[5] = qkv_weight.transpose(0, 1, 3, 2)
    args[6] = args[6].transpose(1, 0, 2)
    args[7] = bias_table.transpose(0, 2, 1)
    staged = [pltpu.VMEM((2, WIN, 2 * WIN, c), BF)] + [pltpu.VMEM(a.shape, a.dtype) for a in args[1:]]
    own0, own1, left_edge, right_edge, rel2 = call(
        lambda *refs: pack_kernel(*refs, count=len(args)),
        (pack, pack, edge, edge, jax.ShapeDtypeStruct((tokens, 2 * tokens), jnp.int32)),
        staged + [pltpu.VMEM((SMALL, 128), F32), pltpu.SemaphoreType.DMA((len(args) + 1,))],
        *(in_hbm(a) for a in args),
        in_specs=[pl.BlockSpec(memory_space=pltpu.HBM)] * len(args),
    )
    packs0 = others(own0)
    left = lax.ppermute(right_edge, "col", neighbours("col", 1))
    right = lax.ppermute(left_edge, "col", neighbours("col", -1))
    packs1 = others(own1)

    sizes = dict(groups=groups, own_heads=own_heads, entries=entries, part=part, hidden=hidden)
    weights_scratch = [
        pltpu.VMEM((c, 3 * c), BF),
        pltpu.VMEM((c, c), BF),
        pltpu.VMEM((c, groups * hidden), BF),
        pltpu.VMEM((groups * hidden, c), BF),
    ]
    strip = jax.ShapeDtypeStruct((SHIFT, tile_cols + 2 * WIN, c), BF)
    bias_scratch = pltpu.VMEM((tokens, own_heads * groups * tokens), F32)
    top, bottom = call(
        lambda *refs: regular_kernel(*refs, **sizes),
        (strip, strip),
        [
            bias_scratch, pltpu.VMEM(image_tokens.shape, BF), pltpu.VMEM(labels.shape, jnp.int32),
            pltpu.SemaphoreType.DMA((2,)),
        ] + weights_scratch,
        in_hbm(image_tokens), in_hbm(labels), left, right, rel2, *packs0,
        in_specs=[pl.BlockSpec(memory_space=pltpu.HBM)] * 2
        + [pl.BlockSpec(memory_space=pltpu.VMEM)] * (3 + groups),
    )
    above = lax.ppermute(bottom, ("row", "ch"), neighbours(("row", "ch"), 1))
    below = lax.ppermute(top, ("row", "ch"), neighbours(("row", "ch"), -1))
    wins = tile_cols // WIN + 1
    group = max(g for g in range(1, 5) if wins % g == 0)
    wide = pltpu.VMEM((WIN, tile_cols + 2 * WIN, c), F32)
    return call(
        lambda *refs: shifted_kernel(*refs, group=group, **sizes),
        jax.ShapeDtypeStruct(image_tokens.shape, BF),
        [
            bias_scratch, wide, wide, pltpu.VMEM((WIN, tile_cols + WIN, c), F32),
            pltpu.VMEM((2, SHIFT * WIN, 128), F32), pltpu.VMEM((2, 128, 128), F32),
        ] + weights_scratch,
        top, bottom, above, below, rel2, *packs1,
    )


def solution(mesh):
    in_specs = (
        P(("row", "ch"), "col", None),
        P(("row", "ch"), "col"),
        P(),
        P(),
        P(),
        P(None, None, None, "ch"),
        P(None, None, "ch"),
        P(None, None, "ch"),
        P(None, "ch", None),
        P(),
        P(None, None, "ch"),
        P(None, "ch"),
        P(None, "ch", None),
        P(),
    )
    out_specs = P(("row", "ch"), "col", None)
    return jax.shard_map(
        both_blocks, mesh=mesh, in_specs=in_specs, out_specs=out_specs, check_vma=False
    )
```

```python
import math

import jax
import jax.numpy as jnp
from jax import lax
from jax.experimental import pallas as pl
from jax.experimental.pallas import tpu as pltpu
from jax.sharding import PartitionSpec as P


WIN = 8
SHIFT = 4
EPS = 1e-05
NEG = -1e30
LOG2E = math.log2(math.e)
BF = jnp.bfloat16
F32 = jnp.float32


def dot_nt(a, b):
    return lax.dot_general(a, b, (((1,), (1,)), ((), ())), preferred_element_type=F32)


def dot_nn(a, b):
    return lax.dot_general(a, b, (((1,), (0,)), ((), ())), preferred_element_type=F32)


def layer_norm(x, gain, shift):
    center = x - jnp.mean(x, axis=-1, keepdims=True)
    spread = jnp.mean(center * center, axis=-1, keepdims=True)
    return (center * lax.rsqrt(spread + EPS) * gain + shift).astype(BF)


def gelu(v):
    half = 0.5 * v
    return half + half * lax.erf(v * math.sqrt(0.5))


def head_masks(heads, depth, width):
    lane = lax.broadcasted_iota(jnp.int32, (WIN * WIN, width), 1)
    return [(lane // depth == h).astype(F32).astype(BF) for h in range(heads)]


def stack_heads(rows, masks):
    return jnp.concatenate([rows * mask for mask in masks], axis=0)


def attend(q, k, v, bias, allowed, masks, ones):
    scores = dot_nt(q, stack_heads(k, masks)) + bias
    if allowed is not None:
        scores = jnp.where(allowed, scores, NEG)
    lanes = 128
    first = lax.broadcasted_iota(jnp.int32, (q.shape[0], lanes), 1) < WIN * WIN
    parts = []
    for start in range(0, scores.shape[1], lanes):
        s = scores[:, start : start + lanes]
        low = jnp.max(jnp.where(first, s, NEG), axis=-1, keepdims=True)
        high = jnp.max(jnp.where(first, NEG, s), axis=-1, keepdims=True)
        parts.append(jnp.exp2(s - jnp.where(first, low, high)).astype(BF))
    weights = jnp.concatenate(parts, axis=1)
    rhs = jnp.concatenate([stack_heads(v, masks), ones], axis=1)
    summed = dot_nn(weights, rhs)
    width = v.shape[1]
    return summed[:, :width] / summed[:, width:]


def pick(low_rows, high_rows, skip, wide):
    rows = wide.shape[0]
    in_low = wide < 128
    low_index = jnp.minimum(wide, 127)
    high_index = jnp.maximum(wide - skip, 0)
    first = lax.broadcasted_iota(jnp.int32, wide.shape, 1) < WIN * WIN

    def of_head(h):
        low = jnp.broadcast_to(low_rows[h] * LOG2E, (rows, 128))
        high = jnp.broadcast_to(high_rows[h] * LOG2E, (rows, 128))
        return jnp.where(
            in_low,
            jnp.take_along_axis(low, low_index, axis=1),
            jnp.take_along_axis(high, high_index, axis=1),
        )

    return jnp.concatenate(
        [jnp.where(first, of_head(h), of_head(h + 1)) for h in range(0, len(low_rows), 2)], axis=1
    )


def split3(value):
    high = value.astype(BF)
    rest = value - high.astype(F32)
    middle = rest.astype(BF)
    return [high, middle, (rest - middle.astype(F32)).astype(BF)]


QKVB, FC1B, TABLE = 0, 3, 5
GAIN, SHIFTS, PROJB, FC2B = 9, 11, 13, 14
SMALL = 16


def pack_kernel(*refs, count):
    hbm, refs = refs[:count], refs[count:]
    (w0_ref, w1_ref, left_ref, right_ref, rel2_ref), refs = refs[:5], refs[5:]
    staged, small_ref, sems = refs[:count], refs[count], refs[count + 1]
    cols = hbm[0].shape[1]
    edge = 2 * WIN
    copies = [
        pltpu.make_async_copy(hbm[0].at[:, 0:edge], staged[0].at[0], sems.at[0]),
        pltpu.make_async_copy(hbm[0].at[:, cols - edge : cols], staged[0].at[1], sems.at[count]),
    ]
    copies += [pltpu.make_async_copy(hbm[k], staged[k], sems.at[k]) for k in range(1, count)]
    for copy in copies:
        copy.start()
    for copy in copies:
        copy.wait()
    (x, labels, rel, gain, shift, qkv, qkvb, table, proj, projb, fc1, fc1b, fc2, fc2b) = staged
    c = x.shape[3]
    part = qkv.shape[2]
    hidden = fc1.shape[2]
    entries = table.shape[2]
    for b, out in enumerate((w0_ref, w1_ref)):
        at = 0
        for m in range(3):
            out[at : at + part, :] = qkv[b, m]
            at += part
        out[at : at + part, :] = proj[b]
        at += part
        for start in range(0, hidden, 128):
            out[at : at + c, :] = fc1[b, :, start : start + 128]
            at += c
        out[at : at + hidden, :] = fc2[b]
        at += hidden
        small_ref[...] = jnp.zeros_like(small_ref)
        for m in range(3):
            small_ref[QKVB + m : QKVB + m + 1, 0:part] = qkvb[m, b : b + 1]
        for k in range(hidden // 128):
            small_ref[FC1B + k : FC1B + k + 1, :] = fc1b[b : b + 1, k * 128 : (k + 1) * 128]
        k = TABLE
        for h in range(table.shape[1]):
            for first in (0, entries - 128):
                small_ref[k : k + 1, :] = table[b, h : h + 1, first : first + 128]
                k += 1
        small_ref[GAIN : GAIN + 2, :] = gain[b]
        small_ref[SHIFTS : SHIFTS + 2, :] = shift[b]
        small_ref[PROJB : PROJB + 1, :] = projb[b : b + 1, :]
        small_ref[FC2B : FC2B + 1, :] = fc2b[b : b + 1, :]
        for piece in split3(small_ref[...]):
            out[at : at + SMALL, :] = piece
            at += SMALL
    ids = (labels[...] + 1).astype(F32).astype(BF)
    for r in range(WIN):
        left_ref[r] = x[0, r, 0:WIN]
        right_ref[r] = x[1, r, WIN:]
    left_ref[WIN] = ids[:, 0:128]
    right_ref[WIN] = ids[:, cols - 128 : cols]
    rel2_ref[...] = jnp.concatenate([rel[...], rel[...]], axis=1)


class Weights:

    def __init__(self, packs, scratch, c, part, hidden):
        self.qkv, self.proj, self.fc1, self.fc2, self.rows = scratch
        self.c = c
        self.packs = packs
        self.part, self.hidden = part, hidden
        self.start_small = 4 * part + (hidden // 128) * c + hidden

    def small(self, row, rows=1, width=128):
        out = []
        for p in self.packs:
            at = self.start_small
            value = sum(
                p[at + k * SMALL : at + (k + 1) * SMALL, :].astype(F32) for k in range(3)
            )
            out.append(value[row : row + rows, :width])
        return out

    def load(self):
        c, part, hidden = self.c, self.part, self.hidden
        for m in range(3):
            rows = jnp.concatenate([p[m * part : (m + 1) * part, :] for p in self.packs], axis=0)
            self.qkv[:, m * c : (m + 1) * c] = rows.astype(F32).T.astype(BF)
        for g, p in enumerate(self.packs):
            at = 3 * part
            self.proj[g * part : (g + 1) * part, :] = p[at : at + part, :]
            at += part
            for k in range(hidden // 128):
                lane = g * hidden + k * 128
                self.fc1[:, lane : lane + 128] = p[at : at + c, :]
                at += c
            self.fc2[g * hidden : (g + 1) * hidden, :] = p[at : at + hidden, :]
        vectors = [self.small(GAIN + k)[0] for k in range(2)]
        vectors += [self.small(SHIFTS + k)[0] for k in range(2)]
        vectors += [self.small(PROJB)[0], self.small(FC2B)[0]]
        for k, row in enumerate(vectors):
            self.rows[k : k + 1, 0:c] = row
        self.rows[6:7, 0 : 3 * c] = jnp.concatenate(
            [v for m in range(3) for v in self.small(QKVB + m, width=part)], axis=1
        )
        rows = [self.small(FC1B + k) for k in range(hidden // 128)]
        self.rows[7:8, :] = jnp.concatenate(
            [row[g] for g in range(len(self.packs)) for row in rows], axis=1
        )

    def row(self, k):
        return self.rows[k : k + 1, 0 : self.c]

    def bias(self, own_heads, skip, wide):
        rows = [self.small(TABLE + k) for k in range(2 * own_heads)]
        low = [rows[2 * h][g] for g in range(len(self.packs)) for h in range(own_heads)]
        high = [rows[2 * h + 1][g] for g in range(len(self.packs)) for h in range(own_heads)]
        return pick(low, high, skip, wide)

    def queries(self, x, scale):
        c = self.c
        product = dot_nn(layer_norm(x, self.row(0), self.row(2)), self.qkv[...]) + self.rows[6:7, 0 : 3 * c]
        return (
            (product[:, :c] * scale).astype(BF),
            product[:, c : 2 * c].astype(BF),
            product[:, 2 * c :].astype(BF),
        )

    def keys(self, x):
        c = self.c
        normed = layer_norm(x, self.row(0), self.row(2))
        product = dot_nn(normed, self.qkv[:, c:]) + self.rows[6:7, c : 3 * c]
        return product[:, :c].astype(BF), product[:, c:].astype(BF)

    def finish(self, x, attended):
        middle = x + dot_nn(attended, self.proj[...]) + self.row(4)
        middle = middle.astype(BF).astype(F32)
        normed = layer_norm(middle, self.row(1), self.row(3))
        hidden = gelu(dot_nn(normed, self.fc1[...]) + self.rows[7:8, :]).astype(BF)
        return middle + dot_nn(hidden, self.fc2[...]) + self.row(5)


def pipeline(chunks, first, second, third):
    def trip(i, carry):
        for u in range(2):
            t = 2 * i + u
            third(jnp.clip(t - 2, 0, chunks - 1), u)
            second(jnp.clip(t - 1, 0, chunks - 1), 1 - u)
            first(jnp.minimum(t, chunks - 1), u)
        return carry

    lax.fori_loop(0, (chunks + 3) // 2, trip, 0)


def regular_kernel(
    x_hbm, labels_hbm, left_ref, right_ref, rel_ref, *refs, groups, own_heads, entries, part, hidden
):
    packs, refs = refs[:groups], refs[groups:]
    (top_ref, bottom_ref, bias_ref, x_ref, labels_ref, sems, out_ref, qkv_ref, att_ref), scratch = refs[:9], refs[9:]
    cols = x_hbm.shape[1]
    x_copy = pltpu.make_async_copy(x_hbm, x_ref.at[:, 0:cols], sems.at[0])
    labels_copy = pltpu.make_async_copy(labels_hbm, labels_ref, sems.at[1])
    x_copy.start()
    labels_copy.start()
    c = x_ref.shape[2]
    heads = own_heads * groups
    depth = c // heads
    tokens = WIN * WIN
    scale = depth ** (-0.5) * LOG2E
    w = Weights(packs, scratch, c, part, hidden)
    w.load()
    masks = head_masks(heads, depth, c)
    ones = jnp.concatenate(masks, axis=0)
    bias_ref[...] = w.bias(own_heads, entries - 128, rel_ref[...])

    labels_copy.wait()
    lanes = jnp.concatenate(
        [
            left_ref[WIN].astype(F32),
            (labels_ref[...] + 1).astype(F32),
            right_ref[WIN].astype(F32),
        ],
        axis=1,
    )
    span = lanes.shape[1]
    lane = lax.broadcasted_iota(jnp.int32, (WIN, span), 1)
    match = lane % WIN == lax.broadcasted_iota(jnp.int32, (WIN, span), 0)
    spread = jnp.concatenate(
        [jnp.where(match, lanes[r : r + 1], 0.0) for r in range(WIN)], axis=0
    ).astype(BF)
    source = lax.broadcasted_iota(jnp.int32, (span, 128), 0)
    window = lax.broadcasted_iota(jnp.int32, (span, 128), 1)
    chosen = ((source - 128 + SHIFT) // WIN == window) & (source >= 128 - SHIFT)
    ids = dot_nn(spread, chosen.astype(F32).astype(BF))
    for r in range(WIN):
        target = top_ref if r < SHIFT else bottom_ref
        target[r % SHIFT, cols + WIN :, :] = ids[r * WIN : (r + 1) * WIN].astype(BF)

    group = 4
    span = group * WIN

    def load(i):
        block = x_ref[:, pl.ds(pl.multiple_of(i * span, span), span), :].astype(F32)
        return jnp.concatenate(
            [block[r, n * WIN : (n + 1) * WIN] for n in range(group) for r in range(WIN)], axis=0
        )

    def first(i, slot):
        for m, value in enumerate(w.queries(load(i), scale)):
            qkv_ref[slot, m] = value

    def second(i, slot):
        for n in range(group):
            at = slice(n * tokens, (n + 1) * tokens)
            q, k, v = (qkv_ref[slot, m, at] for m in range(3))
            att_ref[slot, at] = attend(q, k, v, bias_ref[...], None, masks, ones).astype(BF)

    def third(i, slot):
        out = w.finish(load(i), att_ref[slot])
        for r in range(WIN):
            out_ref[r, pl.ds(pl.multiple_of(i * span, span), span), :] = jnp.concatenate(
                [out[n * tokens + r * WIN : n * tokens + (r + 1) * WIN] for n in range(group)], axis=0
            ).astype(BF)

    for r in range(WIN):
        x_ref[r, cols : cols + 2 * WIN, :] = jnp.concatenate([left_ref[r], right_ref[r]], axis=0)
    x_ref[:, cols + 2 * WIN :, :] = jnp.zeros((WIN, x_ref.shape[1] - cols - 2 * WIN, c), BF)
    x_copy.wait()
    pipeline(x_ref.shape[1] // span, first, second, third)
    before = lax.broadcasted_iota(jnp.int32, (WIN, c), 0) < SHIFT
    for r in range(WIN):
        target = top_ref if r < SHIFT else bottom_ref
        target[r % SHIFT, 0:cols, :] = out_ref[r, 0:cols, :]
        edges = out_ref[r, cols : cols + 2 * WIN, :].astype(F32)
        edge = jnp.where(before, edges[WIN:], edges[:WIN])
        target[r % SHIFT, cols : cols + WIN, :] = edge.astype(BF)


def shifted_kernel(
    top_ref, bottom_ref, above_ref, below_ref, rel_ref, *refs,
    group, groups, own_heads, entries, part, hidden,
):
    packs, refs = refs[:groups], refs[groups:]
    (out_ref, bias_ref, own_ref, halo_ref, res_ref, qid_ref, kid_ref), refs = refs[:7], refs[7:]
    (q_ref, kv_ref, att_ref), scratch = refs[:3], refs[3:]
    c = top_ref.shape[2]
    cols = out_ref.shape[1]
    heads = own_heads * groups
    depth = c // heads
    half = SHIFT * WIN
    tokens = WIN * WIN
    scale = depth ** (-0.5) * LOG2E
    w = Weights(packs, scratch, c, part, hidden)
    w.load()
    masks = head_masks(heads, depth, c)
    ones = jnp.concatenate(masks, axis=0)

    rel = rel_ref[...]
    rel = jnp.concatenate(
        [
            jnp.concatenate([rel[a + SHIFT : a + WIN], rel[a : a + SHIFT]], axis=0)
            for a in range(0, tokens, WIN)
        ],
        axis=0,
    )
    lane = lax.broadcasted_iota(jnp.int32, rel.shape, 1)
    rel = jnp.where(lane % WIN < SHIFT, pltpu.roll(rel, 128 - SHIFT, 1), pltpu.roll(rel, SHIFT, 1))
    rel = jnp.concatenate([pltpu.roll(rel[half:], half, 1), rel[:half]], axis=0)
    bias_ref[...] = w.bias(own_heads, entries - 128, rel)

    for s, (own, halo) in enumerate(((top_ref, above_ref), (bottom_ref, below_ref))):
        parts = []
        for dst, src in ((own_ref, own), (halo_ref, halo)):
            value = src[...].astype(F32)
            edge = value[:, cols : cols + WIN]
            dst[s * SHIFT : (s + 1) * SHIFT, 0:WIN, :] = edge
            dst[s * SHIFT : (s + 1) * SHIFT, WIN : WIN + cols, :] = value[:, :cols]
            dst[s * SHIFT : (s + 1) * SHIFT, WIN + cols :, :] = edge
            parts.append(value[:, cols + WIN :].reshape(half, 128))
        qid_ref[s] = parts[0]
        both = jnp.concatenate(parts + parts, axis=0)
        kid_ref[s] = both.T
    earlier = lax.broadcasted_iota(jnp.int32, (WIN, group * WIN, c), 1) % WIN < SHIFT

    def gather(ref, i):
        start = pl.multiple_of(i * group * WIN, WIN)
        before = ref[:, pl.ds(start, group * WIN), :]
        after = ref[:, pl.ds(start + WIN, group * WIN), :]
        both = jnp.where(earlier, after, before)
        return jnp.concatenate(
            [
                both[s * SHIFT + r, n * WIN : (n + 1) * WIN]
                for n in range(group) for s in range(2) for r in range(SHIFT)
            ],
            axis=0,
        )

    def first(i, slot):
        q, *own = w.queries(gather(own_ref, i), scale)
        q_ref[slot] = q
        for m, value in enumerate(own):
            kv_ref[slot, m, 0] = value
        for m, value in enumerate(w.keys(gather(halo_ref, i))):
            kv_ref[slot, m, 1] = value

    def second(i, slot):
        for n in range(group):
            j = i * group + n
            for s in range(2):
                at = slice((n * 2 + s) * half, (n * 2 + s + 1) * half)
                k, v = (
                    jnp.concatenate([kv_ref[slot, m, 0, at], kv_ref[slot, m, 1, at]], axis=0)
                    for m in range(2)
                )
                keys = kid_ref[s, pl.ds(j, 1), :]
                queries = jnp.take_along_axis(qid_ref[s], jnp.full((half, 128), j, jnp.int32), axis=1)
                allowed = jnp.concatenate([queries, queries], axis=1) == jnp.concatenate(
                    [keys, keys], axis=1
                )
                att_ref[slot, at] = attend(
                    q_ref[slot, at], k, v, bias_ref[s * half : (s + 1) * half], allowed, masks, ones
                ).astype(BF)

    def third(i, slot):
        out = w.finish(gather(own_ref, i), att_ref[slot])
        start = pl.multiple_of(i * group * WIN, WIN)
        for r in range(WIN):
            s, a = r // SHIFT, r % SHIFT
            res_ref[r, pl.ds(start, group * WIN), :] = jnp.concatenate(
                [
                    out[(n * 2 + s) * half + a * WIN : (n * 2 + s) * half + (a + 1) * WIN]
                    for n in range(group)
                ],
                axis=0,
            )

    pipeline((cols + WIN) // (group * WIN), first, second, third)
    low = lax.broadcasted_iota(jnp.int32, (WIN, cols, c), 1) % WIN < SHIFT
    out_ref[...] = jnp.where(low, res_ref[:, 0:cols, :], res_ref[:, WIN : WIN + cols, :]).astype(BF)


def call(kernel, out_shapes, scratch, *args, in_specs=None):
    specs = {} if in_specs is None else {"in_specs": in_specs}
    return pl.pallas_call(
        kernel,
        out_shape=out_shapes,
        scratch_shapes=scratch,
        compiler_params=pltpu.CompilerParams(vmem_limit_bytes=48 * 1024 * 1024),
        **specs,
    )(*args)


def in_hbm(value):
    return pltpu.with_memory_space_constraint(value, pltpu.HBM)


def neighbours(axis, by):
    size = lax.axis_size(axis)
    return [(i, i + by) for i in range(size) if 0 <= i + by < size]


def both_blocks(*args):
    image_tokens, labels, _ = args[:3]
    qkv_weight, bias_table, fc1_weight = args[5], args[7], args[10]
    tile_cols, c = image_tokens.shape[1:]
    groups = lax.axis_size("ch")
    swap = [(i, (i + 1) % groups) for i in range(groups)]
    part = qkv_weight.shape[3]
    hidden = fc1_weight.shape[2]
    entries = bias_table.shape[1]
    own_heads = bias_table.shape[2]
    tokens = WIN * WIN

    def others(value):
        found = [value]
        for _ in range(groups - 1):
            found.append(lax.ppermute(found[-1], "ch", swap))
        return found

    rows = 4 * part + (hidden // 128) * c + hidden + 3 * SMALL
    pack = jax.ShapeDtypeStruct((rows, 128), BF)
    edge = jax.ShapeDtypeStruct((WIN + 1, WIN, c), BF)
    args = list(args)
    args[5] = qkv_weight.transpose(0, 1, 3, 2)
    args[6] = args[6].transpose(1, 0, 2)
    args[7] = bias_table.transpose(0, 2, 1)
    staged = [pltpu.VMEM((2, WIN, 2 * WIN, c), BF)] + [pltpu.VMEM(a.shape, a.dtype) for a in args[1:]]
    own0, own1, left_edge, right_edge, rel2 = call(
        lambda *refs: pack_kernel(*refs, count=len(args)),
        (pack, pack, edge, edge, jax.ShapeDtypeStruct((tokens, 2 * tokens), jnp.int32)),
        staged + [pltpu.VMEM((SMALL, 128), F32), pltpu.SemaphoreType.DMA((len(args) + 1,))],
        *(in_hbm(a) for a in args),
        in_specs=[pl.BlockSpec(memory_space=pltpu.HBM)] * len(args),
    )
    packs0 = others(own0)
    left = lax.ppermute(right_edge, "col", neighbours("col", 1))
    right = lax.ppermute(left_edge, "col", neighbours("col", -1))
    packs1 = others(own1)

    sizes = dict(groups=groups, own_heads=own_heads, entries=entries, part=part, hidden=hidden)
    weights_scratch = [
        pltpu.VMEM((c, 3 * c), BF),
        pltpu.VMEM((c, c), BF),
        pltpu.VMEM((c, groups * hidden), BF),
        pltpu.VMEM((groups * hidden, c), BF),
        pltpu.VMEM((8, groups * hidden), F32),
    ]
    strip = jax.ShapeDtypeStruct((SHIFT, tile_cols + 2 * WIN, c), BF)
    bias_scratch = pltpu.VMEM((tokens, own_heads * groups * tokens), F32)
    wide = pltpu.VMEM((WIN, tile_cols + 4 * WIN, c), BF)
    top, bottom = call(
        lambda *refs: regular_kernel(*refs, **sizes),
        (strip, strip),
        [
            bias_scratch, wide, pltpu.VMEM(labels.shape, jnp.int32), pltpu.SemaphoreType.DMA((2,)),
            wide, pltpu.VMEM((2, 3, 4 * tokens, c), BF), pltpu.VMEM((2, 4 * tokens, c), BF),
        ] + weights_scratch,
        in_hbm(image_tokens), in_hbm(labels), left, right, rel2, *packs0,
        in_specs=[pl.BlockSpec(memory_space=pltpu.HBM)] * 2
        + [pl.BlockSpec(memory_space=pltpu.VMEM)] * (3 + groups),
    )
    above = lax.ppermute(bottom, ("row", "ch"), neighbours(("row", "ch"), 1))
    below = lax.ppermute(top, ("row", "ch"), neighbours(("row", "ch"), -1))
    wins = tile_cols // WIN + 1
    group = max(g for g in range(1, 5) if wins % g == 0)
    wide = pltpu.VMEM((WIN, tile_cols + 2 * WIN, c), F32)
    return call(
        lambda *refs: shifted_kernel(*refs, group=group, **sizes),
        jax.ShapeDtypeStruct(image_tokens.shape, BF),
        [
            bias_scratch, wide, wide, pltpu.VMEM((WIN, tile_cols + WIN, c), F32),
            pltpu.VMEM((2, SHIFT * WIN, 128), F32), pltpu.VMEM((2, 128, 128), F32),
            pltpu.VMEM((2, group * tokens, c), BF), pltpu.VMEM((2, 2, 2, group * tokens, c), BF),
            pltpu.VMEM((2, group * tokens, c), BF),
        ] + weights_scratch,
        top, bottom, above, below, rel2, *packs1,
    )


def solution(mesh):
    in_specs = (
        P(("row", "ch"), "col", None),
        P(("row", "ch"), "col"),
        P(),
        P(),
        P(),
        P(None, None, None, "ch"),
        P(None, None, "ch"),
        P(None, None, "ch"),
        P(None, "ch", None),
        P(),
        P(None, None, "ch"),
        P(None, "ch"),
        P(None, "ch", None),
        P(),
    )
    out_specs = P(("row", "ch"), "col", None)
    return jax.shard_map(
        both_blocks, mesh=mesh, in_specs=in_specs, out_specs=out_specs, check_vma=False
    )
```

```python
import math

import jax
import jax.numpy as jnp
from jax import lax
from jax.experimental import pallas as pl
from jax.experimental.pallas import tpu as pltpu
from jax.sharding import PartitionSpec as P


WIN = 8
SHIFT = 4
EPS = 1e-05
NEG = -1e30
LOG2E = math.log2(math.e)
BF = jnp.bfloat16
F32 = jnp.float32


def dot_nt(a, b):
    return lax.dot_general(a, b, (((1,), (1,)), ((), ())), preferred_element_type=F32)


def dot_nn(a, b):
    return lax.dot_general(a, b, (((1,), (0,)), ((), ())), preferred_element_type=F32)


def gelu(v):
    half = 0.5 * v
    return half + half * lax.erf(v * math.sqrt(0.5))


def head_masks(heads, depth, width):
    lane = lax.broadcasted_iota(jnp.int32, (WIN * WIN, width), 1)
    return [(lane // depth == h).astype(F32).astype(BF) for h in range(heads)]


def stack_heads(rows, masks):
    return jnp.concatenate([rows * mask for mask in masks], axis=0)


def window_pieces(read, bias, allowed, write, masks, ones):
    at = {}

    def score():
        q, k, at["v"] = read()
        at["s"] = dot_nt(q, stack_heads(k, masks))

    def reduce():
        scores = at["s"] + bias()
        if allowed is not None:
            scores = jnp.where(allowed(), scores, NEG)
        first = lax.broadcasted_iota(jnp.int32, (scores.shape[0], 128), 1) < WIN * WIN
        parts = []
        for start in range(0, scores.shape[1], 128):
            s = scores[:, start : start + 128]
            low = jnp.max(jnp.where(first, s, NEG), axis=-1, keepdims=True)
            high = jnp.max(jnp.where(first, NEG, s), axis=-1, keepdims=True)
            parts.append((s, jnp.where(first, low, high)))
        at["s"] = parts

    def mix():
        weights = jnp.concatenate([jnp.exp2(s - m).astype(BF) for s, m in at["s"]], axis=1)
        rhs = jnp.concatenate([stack_heads(at["v"], masks), ones], axis=1)
        at["o"] = dot_nn(weights, rhs)

    def store():
        width = at["o"].shape[1] // 2
        write((at["o"][:, :width] / at["o"][:, width:]).astype(BF))

    return [score, reduce, mix, store]


def skewed(pipelines):
    depth = max(len(p) for p in pipelines)
    return [
        pipelines[n][t - n]
        for t in range(len(pipelines) + depth - 1)
        for n in range(len(pipelines))
        if 0 <= t - n < len(pipelines[n])
    ]


def weave(*threads):
    order = sorted(
        ((k + 0.5) / len(thread), n, k) for n, thread in enumerate(threads) for k in range(len(thread))
    )
    for _, n, k in order:
        threads[n][k]()


def pick(low_rows, high_rows, skip, wide):
    rows = wide.shape[0]
    in_low = wide < 128
    low_index = jnp.minimum(wide, 127)
    high_index = jnp.maximum(wide - skip, 0)
    first = lax.broadcasted_iota(jnp.int32, wide.shape, 1) < WIN * WIN

    def of_head(h):
        low = jnp.broadcast_to(low_rows[h] * LOG2E, (rows, 128))
        high = jnp.broadcast_to(high_rows[h] * LOG2E, (rows, 128))
        return jnp.where(
            in_low,
            jnp.take_along_axis(low, low_index, axis=1),
            jnp.take_along_axis(high, high_index, axis=1),
        )

    return jnp.concatenate(
        [jnp.where(first, of_head(h), of_head(h + 1)) for h in range(0, len(low_rows), 2)], axis=1
    )


def split3(value):
    high = value.astype(BF)
    rest = value - high.astype(F32)
    middle = rest.astype(BF)
    return [high, middle, (rest - middle.astype(F32)).astype(BF)]


QKVB, FC1B, TABLE = 0, 3, 5
GAIN, SHIFTS, PROJB, FC2B = 9, 11, 13, 14
SMALL = 16


def pack_kernel(*refs, count):
    hbm, refs = refs[:count], refs[count:]
    (w0_ref, w1_ref, left_ref, right_ref, rel2_ref), refs = refs[:5], refs[5:]
    staged, small_ref, sems = refs[:count], refs[count], refs[count + 1]
    cols = hbm[0].shape[1]
    edge = 2 * WIN
    copies = [
        pltpu.make_async_copy(hbm[0].at[:, 0:edge], staged[0].at[0], sems.at[0]),
        pltpu.make_async_copy(hbm[0].at[:, cols - edge : cols], staged[0].at[1], sems.at[count]),
    ]
    copies += [pltpu.make_async_copy(hbm[k], staged[k], sems.at[k]) for k in range(1, count)]
    for copy in copies:
        copy.start()
    for copy in copies:
        copy.wait()
    (x, labels, rel, gain, shift, qkv, qkvb, table, proj, projb, fc1, fc1b, fc2, fc2b) = staged
    c = x.shape[3]
    part = qkv.shape[2]
    hidden = fc1.shape[2]
    entries = table.shape[2]
    for b, out in enumerate((w0_ref, w1_ref)):
        at = 0
        for m in range(3):
            out[at : at + part, :] = qkv[b, m]
            at += part
        out[at : at + part, :] = proj[b]
        at += part
        for start in range(0, hidden, 128):
            out[at : at + c, :] = fc1[b, :, start : start + 128]
            at += c
        out[at : at + hidden, :] = fc2[b]
        at += hidden
        small_ref[...] = jnp.zeros_like(small_ref)
        for m in range(3):
            small_ref[QKVB + m : QKVB + m + 1, 0:part] = qkvb[m, b : b + 1]
        for k in range(hidden // 128):
            small_ref[FC1B + k : FC1B + k + 1, :] = fc1b[b : b + 1, k * 128 : (k + 1) * 128]
        k = TABLE
        for h in range(table.shape[1]):
            for first in (0, entries - 128):
                small_ref[k : k + 1, :] = table[b, h : h + 1, first : first + 128]
                k += 1
        small_ref[GAIN : GAIN + 2, :] = gain[b]
        small_ref[SHIFTS : SHIFTS + 2, :] = shift[b]
        small_ref[PROJB : PROJB + 1, :] = projb[b : b + 1, :]
        small_ref[FC2B : FC2B + 1, :] = fc2b[b : b + 1, :]
        for piece in split3(small_ref[...]):
            out[at : at + SMALL, :] = piece
            at += SMALL
    ids = (labels[...] + 1).astype(F32).astype(BF)
    for r in range(WIN):
        left_ref[r] = x[0, r, 0:WIN]
        right_ref[r] = x[1, r, WIN:]
    left_ref[WIN] = ids[:, 0:128]
    right_ref[WIN] = ids[:, cols - 128 : cols]
    rel2_ref[...] = jnp.concatenate([rel[...], rel[...]], axis=1)


class Weights:

    def __init__(self, packs, scratch, c, part, hidden):
        self.qkv, self.proj, self.fc1, self.fc2, self.rows = scratch
        self.c = c
        self.packs = packs
        self.part, self.hidden = part, hidden
        self.start_small = 4 * part + (hidden // 128) * c + hidden

    def small(self, row, rows=1, width=128):
        out = []
        for p in self.packs:
            at = self.start_small
            value = sum(
                p[at + k * SMALL : at + (k + 1) * SMALL, :].astype(F32) for k in range(3)
            )
            out.append(value[row : row + rows, :width])
        return out

    def load(self):
        c, part, hidden = self.c, self.part, self.hidden
        for m in range(3):
            rows = jnp.concatenate([p[m * part : (m + 1) * part, :] for p in self.packs], axis=0)
            self.qkv[:, m * c : (m + 1) * c] = rows.astype(F32).T.astype(BF)
        for g, p in enumerate(self.packs):
            at = 3 * part
            self.proj[g * part : (g + 1) * part, :] = p[at : at + part, :]
            at += part
            for k in range(hidden // 128):
                lane = g * hidden + k * 128
                self.fc1[:, lane : lane + 128] = p[at : at + c, :]
                at += c
            self.fc2[g * hidden : (g + 1) * hidden, :] = p[at : at + hidden, :]
        vectors = [self.small(GAIN + k)[0] for k in range(2)]
        vectors += [self.small(SHIFTS + k)[0] for k in range(2)]
        vectors += [self.small(PROJB)[0], self.small(FC2B)[0]]
        for k, row in enumerate(vectors):
            self.rows[k : k + 1, 0:c] = row
        self.rows[6:7, 0 : 3 * c] = jnp.concatenate(
            [v for m in range(3) for v in self.small(QKVB + m, width=part)], axis=1
        )
        rows = [self.small(FC1B + k) for k in range(hidden // 128)]
        self.rows[7:8, :] = jnp.concatenate(
            [row[g] for g in range(len(self.packs)) for row in rows], axis=1
        )

    def row(self, k):
        return self.rows[k : k + 1, 0 : self.c]

    def bias(self, own_heads, skip, wide):
        rows = [self.small(TABLE + k) for k in range(2 * own_heads)]
        low = [rows[2 * h][g] for g in range(len(self.packs)) for h in range(own_heads)]
        high = [rows[2 * h + 1][g] for g in range(len(self.packs)) for h in range(own_heads)]
        return pick(low, high, skip, wide)

    def norm_pieces(self, at, k):
        def mean():
            x = at["x"]
            at["center"] = x - jnp.mean(x, axis=-1, keepdims=True)

        def spread():
            center = at["center"]
            at["spread"] = jnp.mean(center * center, axis=-1, keepdims=True)

        def normed():
            scaled = at["center"] * lax.rsqrt(at["spread"] + EPS)
            at["normed"] = (scaled * self.row(k) + self.row(2 + k)).astype(BF)

        return [mean, spread, normed]

    def project_pieces(self, load, stores):
        at = {}
        c = self.c

        def begin():
            at["x"] = load()

        def product(m, scale, store):
            def dot():
                at[m] = dot_nn(at["normed"], self.qkv[:, m * c : (m + 1) * c])

            def keep():
                value = at.pop(m) + self.rows[6:7, m * c : (m + 1) * c]
                store((value if scale is None else value * scale).astype(BF))

            return dot, keep

        mean, spread, normed = self.norm_pieces(at, 0)
        made = [product(*entry) for entry in stores]

        def start():
            begin()
            mean()

        return [start, spread, normed] + [dot for dot, _ in made] + [keep for _, keep in made]

    def finish_pieces(self, load, attended, store):
        at = {}
        width = 256

        def project():
            at["p"] = dot_nn(attended(), self.proj[...])

        def begin():
            middle = (load() + at.pop("p") + self.row(4)).astype(BF).astype(F32)
            at["x"] = middle
            at["middle"] = middle

        mean, spread, normed = self.norm_pieces(at, 1)

        def start():
            begin()
            mean()

        def up(k):
            def dot():
                at["up", k] = dot_nn(at["normed"], self.fc1[:, k : k + width])

            return dot

        def act(k):
            def gate():
                at["act", k] = gelu(at.pop(("up", k)) + self.rows[7:8, k : k + width]).astype(BF)

            return gate

        def down(k):
            def dot():
                at["down", k] = dot_nn(at.pop(("act", k)), self.fc2[k : k + width, :])

            return dot

        def end():
            total = at["middle"] + self.row(5)
            for k in starts:
                total = total + at["down", k]
            store(total)

        starts = range(0, self.fc2.shape[0], width)
        pieces = [project, start, spread, normed]
        chains = [[up(k), act(k), down(k)] for k in starts]
        return pieces + skewed(chains) + [end]


def pipeline(chunks, first, second, third):
    for t in range(chunks + 2):
        threads = []
        if t >= 2:
            threads.append(third(t - 2))
        if 1 <= t <= chunks:
            threads.append(second(t - 1))
        if t < chunks:
            threads.append(first(t))
        weave(*threads)


def regular_kernel(
    x_hbm, labels_hbm, left_ref, right_ref, rel_ref, *refs, groups, own_heads, entries, part, hidden
):
    packs, refs = refs[:groups], refs[groups:]
    (top_ref, bottom_ref, bias_ref, x_ref, labels_ref, sems, out_ref, qkv_ref, att_ref), scratch = refs[:9], refs[9:]
    cols = x_hbm.shape[1]
    x_copy = pltpu.make_async_copy(x_hbm, x_ref.at[:, 0:cols], sems.at[0])
    labels_copy = pltpu.make_async_copy(labels_hbm, labels_ref, sems.at[1])
    x_copy.start()
    labels_copy.start()
    c = x_ref.shape[2]
    heads = own_heads * groups
    depth = c // heads
    tokens = WIN * WIN
    scale = depth ** (-0.5) * LOG2E
    w = Weights(packs, scratch, c, part, hidden)
    w.load()
    masks = head_masks(heads, depth, c)
    ones = jnp.concatenate(masks, axis=0)
    bias_ref[...] = w.bias(own_heads, entries - 128, rel_ref[...])

    labels_copy.wait()
    lanes = jnp.concatenate(
        [
            left_ref[WIN].astype(F32),
            (labels_ref[...] + 1).astype(F32),
            right_ref[WIN].astype(F32),
        ],
        axis=1,
    )
    span = lanes.shape[1]
    lane = lax.broadcasted_iota(jnp.int32, (WIN, span), 1)
    match = lane % WIN == lax.broadcasted_iota(jnp.int32, (WIN, span), 0)
    spread = jnp.concatenate(
        [jnp.where(match, lanes[r : r + 1], 0.0) for r in range(WIN)], axis=0
    ).astype(BF)
    source = lax.broadcasted_iota(jnp.int32, (span, 128), 0)
    window = lax.broadcasted_iota(jnp.int32, (span, 128), 1)
    chosen = ((source - 128 + SHIFT) // WIN == window) & (source >= 128 - SHIFT)
    ids = dot_nn(spread, chosen.astype(F32).astype(BF))
    for r in range(WIN):
        target = top_ref if r < SHIFT else bottom_ref
        target[r % SHIFT, cols + WIN :, :] = ids[r * WIN : (r + 1) * WIN].astype(BF)

    group = 4
    span = group * WIN

    def load(i):
        block = x_ref[:, i * span : (i + 1) * span, :].astype(F32)
        return jnp.concatenate(
            [block[r, n * WIN : (n + 1) * WIN] for n in range(group) for r in range(WIN)], axis=0
        )

    def first(i):
        def keep(m):
            def store(value):
                qkv_ref[i % 2, m] = value

            return store

        return w.project_pieces(
            lambda: load(i), [(0, scale, keep(0)), (1, None, keep(1)), (2, None, keep(2))]
        )

    def second(i):
        def window(n):
            rows = slice(n * tokens, (n + 1) * tokens)

            def write(value):
                att_ref[i % 2, rows] = value

            return window_pieces(
                lambda: [qkv_ref[i % 2, m, rows] for m in range(3)],
                lambda: bias_ref[...], None, write, masks, ones,
            )

        return skewed([window(n) for n in range(group)])

    def third(i):
        def store(out):
            for r in range(WIN):
                out_ref[r, i * span : (i + 1) * span, :] = jnp.concatenate(
                    [out[n * tokens + r * WIN : n * tokens + (r + 1) * WIN] for n in range(group)],
                    axis=0,
                ).astype(BF)

        return w.finish_pieces(lambda: load(i), lambda: att_ref[i % 2], store)

    for r in range(WIN):
        x_ref[r, cols : cols + 2 * WIN, :] = jnp.concatenate([left_ref[r], right_ref[r]], axis=0)
    x_ref[:, cols + 2 * WIN :, :] = jnp.zeros((WIN, x_ref.shape[1] - cols - 2 * WIN, c), BF)
    x_copy.wait()
    pipeline(x_ref.shape[1] // span, first, second, third)
    before = lax.broadcasted_iota(jnp.int32, (WIN, c), 0) < SHIFT
    for r in range(WIN):
        target = top_ref if r < SHIFT else bottom_ref
        target[r % SHIFT, 0:cols, :] = out_ref[r, 0:cols, :]
        edges = out_ref[r, cols : cols + 2 * WIN, :].astype(F32)
        edge = jnp.where(before, edges[WIN:], edges[:WIN])
        target[r % SHIFT, cols : cols + WIN, :] = edge.astype(BF)


def shifted_kernel(
    top_ref, bottom_ref, above_ref, below_ref, rel_ref, *refs,
    group, groups, own_heads, entries, part, hidden,
):
    packs, refs = refs[:groups], refs[groups:]
    (out_ref, bias_ref, own_ref, halo_ref, res_ref, qid_ref, kid_ref), refs = refs[:7], refs[7:]
    (q_ref, kv_ref, att_ref), scratch = refs[:3], refs[3:]
    c = top_ref.shape[2]
    cols = out_ref.shape[1]
    heads = own_heads * groups
    depth = c // heads
    half = SHIFT * WIN
    tokens = WIN * WIN
    scale = depth ** (-0.5) * LOG2E
    w = Weights(packs, scratch, c, part, hidden)
    w.load()
    masks = head_masks(heads, depth, c)
    ones = jnp.concatenate(masks, axis=0)

    rel = rel_ref[...]
    rel = jnp.concatenate(
        [
            jnp.concatenate([rel[a + SHIFT : a + WIN], rel[a : a + SHIFT]], axis=0)
            for a in range(0, tokens, WIN)
        ],
        axis=0,
    )
    lane = lax.broadcasted_iota(jnp.int32, rel.shape, 1)
    rel = jnp.where(lane % WIN < SHIFT, pltpu.roll(rel, 128 - SHIFT, 1), pltpu.roll(rel, SHIFT, 1))
    rel = jnp.concatenate([pltpu.roll(rel[half:], half, 1), rel[:half]], axis=0)
    bias_ref[...] = w.bias(own_heads, entries - 128, rel)

    for s, (own, halo) in enumerate(((top_ref, above_ref), (bottom_ref, below_ref))):
        parts = []
        for dst, src in ((own_ref, own), (halo_ref, halo)):
            value = src[...].astype(F32)
            edge = value[:, cols : cols + WIN]
            dst[s * SHIFT : (s + 1) * SHIFT, 0:WIN, :] = edge
            dst[s * SHIFT : (s + 1) * SHIFT, WIN : WIN + cols, :] = value[:, :cols]
            dst[s * SHIFT : (s + 1) * SHIFT, WIN + cols :, :] = edge
            parts.append(value[:, cols + WIN :].reshape(half, 128))
        qid_ref[s] = parts[0]
        both = jnp.concatenate(parts + parts, axis=0)
        kid_ref[s] = both.T
    earlier = lax.broadcasted_iota(jnp.int32, (WIN, c), 0) < SHIFT

    def gather(ref, i):
        pieces = []
        for n in range(group):
            start = (i * group + n) * WIN
            for r in range(WIN):
                before = ref[r, start : start + WIN, :]
                after = ref[r, start + WIN : start + 2 * WIN, :]
                pieces.append(jnp.where(earlier, after, before))
        return jnp.concatenate(pieces, axis=0)

    def first(i):
        def keep(target):
            def store(value):
                target[...] = value

            return store

        slot = i % 2
        own = w.project_pieces(
            lambda: gather(own_ref, i),
            [(0, scale, keep(q_ref.at[slot]))]
            + [(1 + m, None, keep(kv_ref.at[slot, m, 0])) for m in range(2)],
        )
        halo = w.project_pieces(
            lambda: gather(halo_ref, i), [(1 + m, None, keep(kv_ref.at[slot, m, 1])) for m in range(2)]
        )
        return skewed([own, halo])

    def second(i):
        slot = i % 2

        def window(n, s):
            j = i * group + n
            rows = slice((n * 2 + s) * half, (n * 2 + s + 1) * half)

            def read():
                k, v = (
                    jnp.concatenate([kv_ref[slot, m, 0, rows], kv_ref[slot, m, 1, rows]], axis=0)
                    for m in range(2)
                )
                return q_ref[slot, rows], k, v

            def allowed():
                keys = kid_ref[s, j : j + 1, :]
                queries = jnp.broadcast_to(qid_ref[s, :, j : j + 1], (half, 128))
                same = queries == keys
                return jnp.concatenate([same, same], axis=1)

            def write(value):
                att_ref[slot, rows] = value

            return window_pieces(
                read, lambda: bias_ref[s * half : (s + 1) * half], allowed, write, masks, ones
            )

        return skewed([window(n, s) for n in range(group) for s in range(2)])

    def third(i):
        start = i * group * WIN

        def store(out):
            for r in range(WIN):
                s, a = r // SHIFT, r % SHIFT
                res_ref[r, start : start + group * WIN, :] = jnp.concatenate(
                    [
                        out[(n * 2 + s) * half + a * WIN : (n * 2 + s) * half + (a + 1) * WIN]
                        for n in range(group)
                    ],
                    axis=0,
                )

        return w.finish_pieces(lambda: gather(own_ref, i), lambda: att_ref[i % 2], store)

    pipeline((cols + WIN) // (group * WIN), first, second, third)
    low = lax.broadcasted_iota(jnp.int32, (WIN, cols, c), 1) % WIN < SHIFT
    out_ref[...] = jnp.where(low, res_ref[:, 0:cols, :], res_ref[:, WIN : WIN + cols, :]).astype(BF)


def call(kernel, out_shapes, scratch, *args, in_specs=None):
    specs = {} if in_specs is None else {"in_specs": in_specs}
    return pl.pallas_call(
        kernel,
        out_shape=out_shapes,
        scratch_shapes=scratch,
        compiler_params=pltpu.CompilerParams(vmem_limit_bytes=48 * 1024 * 1024),
        **specs,
    )(*args)


def in_hbm(value):
    return pltpu.with_memory_space_constraint(value, pltpu.HBM)


def neighbours(axis, by):
    size = lax.axis_size(axis)
    return [(i, i + by) for i in range(size) if 0 <= i + by < size]


def both_blocks(*args):
    image_tokens, labels, _ = args[:3]
    qkv_weight, bias_table, fc1_weight = args[5], args[7], args[10]
    tile_cols, c = image_tokens.shape[1:]
    groups = lax.axis_size("ch")
    swap = [(i, (i + 1) % groups) for i in range(groups)]
    part = qkv_weight.shape[3]
    hidden = fc1_weight.shape[2]
    entries = bias_table.shape[1]
    own_heads = bias_table.shape[2]
    tokens = WIN * WIN

    def others(value):
        found = [value]
        for _ in range(groups - 1):
            found.append(lax.ppermute(found[-1], "ch", swap))
        return found

    rows = 4 * part + (hidden // 128) * c + hidden + 3 * SMALL
    pack = jax.ShapeDtypeStruct((rows, 128), BF)
    edge = jax.ShapeDtypeStruct((WIN + 1, WIN, c), BF)
    args = list(args)
    args[5] = qkv_weight.transpose(0, 1, 3, 2)
    args[6] = args[6].transpose(1, 0, 2)
    args[7] = bias_table.transpose(0, 2, 1)
    staged = [pltpu.VMEM((2, WIN, 2 * WIN, c), BF)] + [pltpu.VMEM(a.shape, a.dtype) for a in args[1:]]
    own0, own1, left_edge, right_edge, rel2 = call(
        lambda *refs: pack_kernel(*refs, count=len(args)),
        (pack, pack, edge, edge, jax.ShapeDtypeStruct((tokens, 2 * tokens), jnp.int32)),
        staged + [pltpu.VMEM((SMALL, 128), F32), pltpu.SemaphoreType.DMA((len(args) + 1,))],
        *(in_hbm(a) for a in args),
        in_specs=[pl.BlockSpec(memory_space=pltpu.HBM)] * len(args),
    )
    packs0 = others(own0)
    left = lax.ppermute(right_edge, "col", neighbours("col", 1))
    right = lax.ppermute(left_edge, "col", neighbours("col", -1))
    packs1 = others(own1)

    sizes = dict(groups=groups, own_heads=own_heads, entries=entries, part=part, hidden=hidden)
    weights_scratch = [
        pltpu.VMEM((c, 3 * c), BF),
        pltpu.VMEM((c, c), BF),
        pltpu.VMEM((c, groups * hidden), BF),
        pltpu.VMEM((groups * hidden, c), BF),
        pltpu.VMEM((8, groups * hidden), F32),
    ]
    strip = jax.ShapeDtypeStruct((SHIFT, tile_cols + 2 * WIN, c), BF)
    bias_scratch = pltpu.VMEM((tokens, own_heads * groups * tokens), F32)
    wide = pltpu.VMEM((WIN, tile_cols + 4 * WIN, c), BF)
    top, bottom = call(
        lambda *refs: regular_kernel(*refs, **sizes),
        (strip, strip),
        [
            bias_scratch, wide, pltpu.VMEM(labels.shape, jnp.int32), pltpu.SemaphoreType.DMA((2,)),
            wide, pltpu.VMEM((2, 3, 4 * tokens, c), BF), pltpu.VMEM((2, 4 * tokens, c), BF),
        ] + weights_scratch,
        in_hbm(image_tokens), in_hbm(labels), left, right, rel2, *packs0,
        in_specs=[pl.BlockSpec(memory_space=pltpu.HBM)] * 2
        + [pl.BlockSpec(memory_space=pltpu.VMEM)] * (3 + groups),
    )
    above = lax.ppermute(bottom, ("row", "ch"), neighbours(("row", "ch"), 1))
    below = lax.ppermute(top, ("row", "ch"), neighbours(("row", "ch"), -1))
    wins = tile_cols // WIN + 1
    group = max(g for g in range(1, 5) if wins % g == 0)
    wide = pltpu.VMEM((WIN, tile_cols + 2 * WIN, c), F32)
    return call(
        lambda *refs: shifted_kernel(*refs, group=group, **sizes),
        jax.ShapeDtypeStruct(image_tokens.shape, BF),
        [
            bias_scratch, wide, wide, pltpu.VMEM((WIN, tile_cols + WIN, c), F32),
            pltpu.VMEM((2, SHIFT * WIN, 128), F32), pltpu.VMEM((2, 128, 128), F32),
            pltpu.VMEM((2, group * tokens, c), BF), pltpu.VMEM((2, 2, 2, group * tokens, c), BF),
            pltpu.VMEM((2, group * tokens, c), BF),
        ] + weights_scratch,
        top, bottom, above, below, rel2, *packs1,
    )


def solution(mesh):
    in_specs = (
        P(("row", "ch"), "col", None),
        P(("row", "ch"), "col"),
        P(),
        P(),
        P(),
        P(None, None, None, "ch"),
        P(None, None, "ch"),
        P(None, None, "ch"),
        P(None, "ch", None),
        P(),
        P(None, None, "ch"),
        P(None, "ch"),
        P(None, "ch", None),
        P(),
    )
    out_specs = P(("row", "ch"), "col", None)
    return jax.shard_map(
        both_blocks, mesh=mesh, in_specs=in_specs, out_specs=out_specs, check_vma=False
    )
```

```python
import math

import jax
import jax.numpy as jnp
from jax import lax
from jax.experimental import pallas as pl
from jax.experimental.pallas import tpu as pltpu
from jax.sharding import PartitionSpec as P


WIN = 8
SHIFT = 4
EPS = 1e-05
NEG = -1e30
LOG2E = math.log2(math.e)
BF = jnp.bfloat16
F32 = jnp.float32


def dot_nt(a, b):
    return lax.dot_general(a, b, (((1,), (1,)), ((), ())), preferred_element_type=F32)


def dot_nn(a, b):
    return lax.dot_general(a, b, (((1,), (0,)), ((), ())), preferred_element_type=F32)


def gelu(v):
    half = 0.5 * v
    return half + half * lax.erf(v * math.sqrt(0.5))


def head_masks(heads, depth, width):
    lane = lax.broadcasted_iota(jnp.int32, (WIN * WIN, width), 1)
    return [(lane // depth == h).astype(F32).astype(BF) for h in range(heads)]


def stack_heads(rows, masks):
    return jnp.concatenate([rows * mask for mask in masks], axis=0)


def window_pieces(read, bias, allowed, write, masks, ones):
    at = {}

    def score():
        q, k, at["v"] = read()
        at["s"] = dot_nt(q, stack_heads(k, masks))

    def reduce():
        scores = at["s"] + bias()
        if allowed is not None:
            scores = jnp.where(allowed(), scores, NEG)
        first = lax.broadcasted_iota(jnp.int32, (scores.shape[0], 128), 1) < WIN * WIN
        parts = []
        for start in range(0, scores.shape[1], 128):
            s = scores[:, start : start + 128]
            low = jnp.max(jnp.where(first, s, NEG), axis=-1, keepdims=True)
            high = jnp.max(jnp.where(first, NEG, s), axis=-1, keepdims=True)
            parts.append((s, jnp.where(first, low, high)))
        at["s"] = parts

    def mix():
        weights = jnp.concatenate([jnp.exp2(s - m).astype(BF) for s, m in at["s"]], axis=1)
        rhs = jnp.concatenate([stack_heads(at["v"], masks), ones], axis=1)
        at["o"] = dot_nn(weights, rhs)

    def store():
        width = at["o"].shape[1] // 2
        write((at["o"][:, :width] / at["o"][:, width:]).astype(BF))

    return [score, reduce, mix, store]


def skewed(pipelines):
    depth = max(len(p) for p in pipelines)
    return [
        pipelines[n][t - n]
        for t in range(len(pipelines) + depth - 1)
        for n in range(len(pipelines))
        if 0 <= t - n < len(pipelines[n])
    ]


def weave(*threads):
    order = sorted(
        ((k + 0.5) / len(thread), n, k) for n, thread in enumerate(threads) for k in range(len(thread))
    )
    for _, n, k in order:
        threads[n][k]()


def pick(low_rows, high_rows, skip, wide):
    rows = wide.shape[0]
    in_low = wide < 128
    low_index = jnp.minimum(wide, 127)
    high_index = jnp.maximum(wide - skip, 0)
    first = lax.broadcasted_iota(jnp.int32, wide.shape, 1) < WIN * WIN

    def of_head(h):
        low = jnp.broadcast_to(low_rows[h] * LOG2E, (rows, 128))
        high = jnp.broadcast_to(high_rows[h] * LOG2E, (rows, 128))
        return jnp.where(
            in_low,
            jnp.take_along_axis(low, low_index, axis=1),
            jnp.take_along_axis(high, high_index, axis=1),
        )

    return jnp.concatenate(
        [jnp.where(first, of_head(h), of_head(h + 1)) for h in range(0, len(low_rows), 2)], axis=1
    )


def split3(value):
    high = value.astype(BF)
    rest = value - high.astype(F32)
    middle = rest.astype(BF)
    return [high, middle, (rest - middle.astype(F32)).astype(BF)]


QKVB, FC1B, TABLE = 0, 3, 5
GAIN, SHIFTS, PROJB, FC2B = 9, 11, 13, 14
SMALL = 16


def pack_kernel(*refs, count):
    hbm, refs = refs[:count], refs[count:]
    (w0_ref, w1_ref, left_ref, right_ref, rel2_ref), refs = refs[:5], refs[5:]
    staged, small_ref, sems = refs[:count], refs[count], refs[count + 1]
    cols = hbm[0].shape[1]
    edge = 2 * WIN
    copies = [
        pltpu.make_async_copy(hbm[0].at[:, 0:edge], staged[0].at[0], sems.at[0]),
        pltpu.make_async_copy(hbm[0].at[:, cols - edge : cols], staged[0].at[1], sems.at[count]),
    ]
    copies += [pltpu.make_async_copy(hbm[k], staged[k], sems.at[k]) for k in range(1, count)]
    for copy in copies:
        copy.start()
    for copy in copies:
        copy.wait()
    (x, labels, rel, gain, shift, qkv, qkvb, table, proj, projb, fc1, fc1b, fc2, fc2b) = staged
    c = x.shape[3]
    part = qkv.shape[2]
    hidden = fc1.shape[2]
    entries = table.shape[2]
    for b, out in enumerate((w0_ref, w1_ref)):
        at = 0
        for m in range(3):
            out[at : at + part, :] = qkv[b, m]
            at += part
        out[at : at + part, :] = proj[b]
        at += part
        for start in range(0, hidden, 128):
            out[at : at + c, :] = fc1[b, :, start : start + 128]
            at += c
        out[at : at + hidden, :] = fc2[b]
        at += hidden
        small_ref[...] = jnp.zeros_like(small_ref)
        for m in range(3):
            small_ref[QKVB + m : QKVB + m + 1, 0:part] = qkvb[m, b : b + 1]
        for k in range(hidden // 128):
            small_ref[FC1B + k : FC1B + k + 1, :] = fc1b[b : b + 1, k * 128 : (k + 1) * 128]
        k = TABLE
        for h in range(table.shape[1]):
            for first in (0, entries - 128):
                small_ref[k : k + 1, :] = table[b, h : h + 1, first : first + 128]
                k += 1
        small_ref[GAIN : GAIN + 2, :] = gain[b]
        small_ref[SHIFTS : SHIFTS + 2, :] = shift[b]
        small_ref[PROJB : PROJB + 1, :] = projb[b : b + 1, :]
        small_ref[FC2B : FC2B + 1, :] = fc2b[b : b + 1, :]
        for piece in split3(small_ref[...]):
            out[at : at + SMALL, :] = piece
            at += SMALL
    ids = (labels[...] + 1).astype(F32).astype(BF)
    for r in range(WIN):
        left_ref[r] = x[0, r, 0:WIN]
        right_ref[r] = x[1, r, WIN:]
    left_ref[WIN] = ids[:, 0:128]
    right_ref[WIN] = ids[:, cols - 128 : cols]
    rel2_ref[...] = jnp.concatenate([rel[...], rel[...]], axis=1)


class Weights:

    def __init__(self, packs, scratch, c, part, hidden):
        self.qkv, self.proj, self.fc1, self.fc2, self.rows = scratch
        self.c = c
        self.packs = packs
        self.part, self.hidden = part, hidden
        self.start_small = 4 * part + (hidden // 128) * c + hidden

    def small(self, row, rows=1, width=128):
        out = []
        for p in self.packs:
            at = self.start_small
            value = sum(
                p[at + k * SMALL : at + (k + 1) * SMALL, :].astype(F32) for k in range(3)
            )
            out.append(value[row : row + rows, :width])
        return out

    def load(self):
        c, part, hidden = self.c, self.part, self.hidden
        for m in range(3):
            rows = jnp.concatenate([p[m * part : (m + 1) * part, :] for p in self.packs], axis=0)
            self.qkv[:, m * c : (m + 1) * c] = rows.astype(F32).T.astype(BF)
        for g, p in enumerate(self.packs):
            at = 3 * part
            self.proj[g * part : (g + 1) * part, :] = p[at : at + part, :]
            at += part
            for k in range(hidden // 128):
                lane = g * hidden + k * 128
                self.fc1[:, lane : lane + 128] = p[at : at + c, :]
                at += c
            self.fc2[g * hidden : (g + 1) * hidden, :] = p[at : at + hidden, :]
        vectors = [self.small(GAIN + k)[0] for k in range(2)]
        vectors += [self.small(SHIFTS + k)[0] for k in range(2)]
        vectors += [self.small(PROJB)[0], self.small(FC2B)[0]]
        for k, row in enumerate(vectors):
            self.rows[k : k + 1, 0:c] = row
        self.rows[6:7, 0 : 3 * c] = jnp.concatenate(
            [v for m in range(3) for v in self.small(QKVB + m, width=part)], axis=1
        )
        rows = [self.small(FC1B + k) for k in range(hidden // 128)]
        self.rows[7:8, :] = jnp.concatenate(
            [row[g] for g in range(len(self.packs)) for row in rows], axis=1
        )

    def row(self, k):
        return self.rows[k : k + 1, 0 : self.c]

    def bias(self, own_heads, skip, wide):
        rows = [self.small(TABLE + k) for k in range(2 * own_heads)]
        low = [rows[2 * h][g] for g in range(len(self.packs)) for h in range(own_heads)]
        high = [rows[2 * h + 1][g] for g in range(len(self.packs)) for h in range(own_heads)]
        return pick(low, high, skip, wide)

    def norm_pieces(self, at, k):
        def mean():
            x = at["x"]
            at["center"] = x - jnp.mean(x, axis=-1, keepdims=True)

        def spread():
            center = at["center"]
            at["spread"] = jnp.mean(center * center, axis=-1, keepdims=True)

        def normed():
            scaled = at["center"] * lax.rsqrt(at["spread"] + EPS)
            at["normed"] = (scaled * self.row(k) + self.row(2 + k)).astype(BF)

        return [mean, spread, normed]

    def project_pieces(self, load, stores):
        at = {}
        c = self.c

        def begin():
            at["x"] = load()

        def product(m, scale, store):
            def dot():
                at[m] = dot_nn(at["normed"], self.qkv[:, m * c : (m + 1) * c])

            def keep():
                value = at.pop(m) + self.rows[6:7, m * c : (m + 1) * c]
                store((value if scale is None else value * scale).astype(BF))

            return dot, keep

        mean, spread, normed = self.norm_pieces(at, 0)
        made = [product(*entry) for entry in stores]

        def start():
            begin()
            mean()

        return [start, spread, normed] + [dot for dot, _ in made] + [keep for _, keep in made]

    def finish_pieces(self, load, attended, store):
        at = {}
        width = 256

        def project():
            at["p"] = dot_nn(attended(), self.proj[...])

        def begin():
            middle = (load() + at.pop("p") + self.row(4)).astype(BF).astype(F32)
            at["x"] = middle
            at["middle"] = middle

        mean, spread, normed = self.norm_pieces(at, 1)

        def start():
            begin()
            mean()

        def up(k):
            def dot():
                at["up", k] = dot_nn(at["normed"], self.fc1[:, k : k + width])

            return dot

        def act(k):
            def gate():
                at["act", k] = gelu(at.pop(("up", k)) + self.rows[7:8, k : k + width]).astype(BF)

            return gate

        def down(k):
            def dot():
                at["down", k] = dot_nn(at.pop(("act", k)), self.fc2[k : k + width, :])

            return dot

        def end():
            total = at["middle"] + self.row(5)
            for k in starts:
                total = total + at["down", k]
            store(total)

        starts = range(0, self.fc2.shape[0], width)
        pieces = [project, start, spread, normed]
        chains = [[up(k), act(k), down(k)] for k in starts]
        return pieces + skewed(chains) + [end]


def pipeline(chunks, first, second, third):
    for t in range(chunks + 2):
        threads = []
        if t >= 2:
            threads.append(third(t - 2))
        if 1 <= t <= chunks:
            threads.append(second(t - 1))
        if t < chunks:
            threads.append(first(t))
        weave(*threads)


def parity():
    return (lax.axis_index("row") * lax.axis_size("ch") + lax.axis_index("ch")) % 2


def regular_kernel(
    x_hbm, labels_hbm, left_ref, right_ref, rel_ref, *refs, groups, own_heads, entries, part, hidden
):
    packs, refs = refs[:groups], refs[groups:]
    (near_ref, far_ref, bias_ref, x_ref, labels_ref, sems, out_ref, qkv_ref, att_ref, id_ref), scratch = refs[:10], refs[10:]
    cols = x_hbm.shape[1]
    x_copy = pltpu.make_async_copy(x_hbm, x_ref.at[:, 0:cols], sems.at[0])
    labels_copy = pltpu.make_async_copy(labels_hbm, labels_ref, sems.at[1])
    x_copy.start()
    labels_copy.start()
    c = x_ref.shape[2]
    heads = own_heads * groups
    depth = c // heads
    tokens = WIN * WIN
    scale = depth ** (-0.5) * LOG2E
    w = Weights(packs, scratch, c, part, hidden)
    w.load()
    masks = head_masks(heads, depth, c)
    ones = jnp.concatenate(masks, axis=0)
    bias_ref[...] = w.bias(own_heads, entries - 128, rel_ref[...])

    labels_copy.wait()
    lanes = jnp.concatenate(
        [
            left_ref[WIN].astype(F32),
            (labels_ref[...] + 1).astype(F32),
            right_ref[WIN].astype(F32),
        ],
        axis=1,
    )
    span = lanes.shape[1]
    lane = lax.broadcasted_iota(jnp.int32, (WIN, span), 1)
    match = lane % WIN == lax.broadcasted_iota(jnp.int32, (WIN, span), 0)
    spread = jnp.concatenate(
        [jnp.where(match, lanes[r : r + 1], 0.0) for r in range(WIN)], axis=0
    ).astype(BF)
    source = lax.broadcasted_iota(jnp.int32, (span, 128), 0)
    window = lax.broadcasted_iota(jnp.int32, (span, 128), 1)
    chosen = ((source - 128 + SHIFT) // WIN == window) & (source >= 128 - SHIFT)
    ids = dot_nn(spread, chosen.astype(F32).astype(BF))
    id_ref[...] = ids.reshape(WIN, WIN, 128).astype(BF)

    group = 4
    span = group * WIN

    def load(i):
        block = x_ref[:, i * span : (i + 1) * span, :].astype(F32)
        return jnp.concatenate(
            [block[r, n * WIN : (n + 1) * WIN] for n in range(group) for r in range(WIN)], axis=0
        )

    def first(i):
        def keep(m):
            def store(value):
                qkv_ref[i % 2, m] = value

            return store

        return w.project_pieces(
            lambda: load(i), [(0, scale, keep(0)), (1, None, keep(1)), (2, None, keep(2))]
        )

    def second(i):
        def window(n):
            rows = slice(n * tokens, (n + 1) * tokens)

            def write(value):
                att_ref[i % 2, rows] = value

            return window_pieces(
                lambda: [qkv_ref[i % 2, m, rows] for m in range(3)],
                lambda: bias_ref[...], None, write, masks, ones,
            )

        return skewed([window(n) for n in range(group)])

    def third(i):
        def store(out):
            for r in range(WIN):
                out_ref[r, i * span : (i + 1) * span, :] = jnp.concatenate(
                    [out[n * tokens + r * WIN : n * tokens + (r + 1) * WIN] for n in range(group)],
                    axis=0,
                ).astype(BF)

        return w.finish_pieces(lambda: load(i), lambda: att_ref[i % 2], store)

    for r in range(WIN):
        x_ref[r, cols : cols + 2 * WIN, :] = jnp.concatenate([left_ref[r], right_ref[r]], axis=0)
    x_ref[:, cols + 2 * WIN :, :] = jnp.zeros((WIN, x_ref.shape[1] - cols - 2 * WIN, c), BF)
    x_copy.wait()
    pipeline(x_ref.shape[1] // span, first, second, third)
    before = lax.broadcasted_iota(jnp.int32, (WIN, c), 0) < SHIFT
    for target, side in ((near_ref, 1 - parity()), (far_ref, parity())):
        for r in range(SHIFT):
            row = side * SHIFT + r
            target[r, 0:cols, :] = out_ref[row, 0:cols, :]
            edges = out_ref[row, cols : cols + 2 * WIN, :].astype(F32)
            edge = jnp.where(before, edges[WIN:], edges[:WIN])
            target[r, cols : cols + WIN, :] = edge.astype(BF)
            target[r, cols + WIN :, :] = id_ref[row]


def even_split(count, most):
    parts = -(-count // most)
    return [(count * k // parts, count * (k + 1) // parts) for k in range(parts)]


def shifted_kernel(own_in, halo_in, rel_ref, *refs, chunks, near, groups, own_heads, entries, part, hidden):
    packs, refs = refs[:groups], refs[groups:]
    if not near:
        done_ref, refs = refs[0], refs[1:]
    (out_ref, bias_ref, own_ref, halo_ref, res_ref), refs = refs[:5], refs[5:]
    (q_ref, kv_ref, att_ref), scratch = refs[:3], refs[3:]
    side = 1 - parity() if near else parity()
    c = own_in.shape[2]
    cols = out_ref.shape[1]
    heads = own_heads * groups
    depth = c // heads
    half = SHIFT * WIN
    tokens = WIN * WIN
    scale = depth ** (-0.5) * LOG2E
    w = Weights(packs, scratch, c, part, hidden)
    w.load()
    masks = head_masks(heads, depth, c)
    ones = jnp.concatenate(masks, axis=0)

    rel = rel_ref[...]
    rel = jnp.concatenate(
        [
            jnp.concatenate([rel[a + SHIFT : a + WIN], rel[a : a + SHIFT]], axis=0)
            for a in range(0, tokens, WIN)
        ],
        axis=0,
    )
    lane = lax.broadcasted_iota(jnp.int32, rel.shape, 1)
    rel = jnp.where(lane % WIN < SHIFT, pltpu.roll(rel, 128 - SHIFT, 1), pltpu.roll(rel, SHIFT, 1))
    rel = jnp.where(side == 0, pltpu.roll(rel[half:], half, 1), rel[:half])
    bias_ref[...] = w.bias(own_heads, entries - 128, rel)

    parts = []
    for dst, src in ((own_ref, own_in), (halo_ref, halo_in)):
        value = src[...].astype(F32)
        edge = value[:, cols : cols + WIN]
        dst[:, 0:WIN, :] = edge
        dst[:, WIN : WIN + cols, :] = value[:, :cols]
        dst[:, WIN + cols :, :] = edge
        parts.append(value[:, cols + WIN :].reshape(half, 128))
    query_ids = parts[0]
    key_ids = jnp.concatenate(parts + parts, axis=0).T
    earlier = lax.broadcasted_iota(jnp.int32, (WIN, c), 0) < SHIFT

    def gather(ref, i):
        pieces = []
        for j in range(*chunks[i]):
            for r in range(SHIFT):
                before = ref[r, j * WIN : (j + 1) * WIN, :]
                after = ref[r, (j + 1) * WIN : (j + 2) * WIN, :]
                pieces.append(jnp.where(earlier, after, before))
        return jnp.concatenate(pieces, axis=0)

    def first(i):
        slot = i % 2
        count = (chunks[i][1] - chunks[i][0]) * half

        def keep(target):
            def store(value):
                target[0:count] = value

            return store

        own = w.project_pieces(
            lambda: gather(own_ref, i),
            [(0, scale, keep(q_ref.at[slot]))]
            + [(1 + m, None, keep(kv_ref.at[slot, m, 0])) for m in range(2)],
        )
        halo = w.project_pieces(
            lambda: gather(halo_ref, i), [(1 + m, None, keep(kv_ref.at[slot, m, 1])) for m in range(2)]
        )
        return skewed([own, halo])

    def second(i):
        slot = i % 2
        base = chunks[i][0]

        def window(j):
            rows = slice((j - base) * half, (j - base + 1) * half)

            def read():
                k, v = (
                    jnp.concatenate([kv_ref[slot, m, 0, rows], kv_ref[slot, m, 1, rows]], axis=0)
                    for m in range(2)
                )
                return q_ref[slot, rows], k, v

            def allowed():
                same = jnp.broadcast_to(query_ids[:, j : j + 1], (half, 128)) == key_ids[j : j + 1, :]
                return jnp.concatenate([same, same], axis=1)

            def write(value):
                att_ref[slot, rows] = value

            return window_pieces(read, lambda: bias_ref[...], allowed, write, masks, ones)

        return skewed([window(j) for j in range(*chunks[i])])

    def third(i):
        base, stop = chunks[i]

        def store(out):
            for r in range(SHIFT):
                res_ref[r, base * WIN : stop * WIN, :] = jnp.concatenate(
                    [
                        out[n * half + r * WIN : n * half + (r + 1) * WIN]
                        for n in range(stop - base)
                    ],
                    axis=0,
                )

        return w.finish_pieces(
            lambda: gather(own_ref, i), lambda: att_ref[i % 2, 0 : (stop - base) * half], store
        )

    pipeline(len(chunks), first, second, third)
    low = lax.broadcasted_iota(jnp.int32, (SHIFT, cols, c), 1) % WIN < SHIFT
    result = jnp.where(low, res_ref[:, 0:cols, :], res_ref[:, WIN : WIN + cols, :]).astype(BF)
    if near:
        out_ref[...] = result
    else:
        out_ref[pl.ds(side * SHIFT, SHIFT)] = result
        out_ref[pl.ds((1 - side) * SHIFT, SHIFT)] = done_ref[...]


def call(kernel, out_shapes, scratch, *args, in_specs=None):
    specs = {} if in_specs is None else {"in_specs": in_specs}
    return pl.pallas_call(
        kernel,
        out_shape=out_shapes,
        scratch_shapes=scratch,
        compiler_params=pltpu.CompilerParams(vmem_limit_bytes=48 * 1024 * 1024),
        **specs,
    )(*args)


def in_hbm(value):
    return pltpu.with_memory_space_constraint(value, pltpu.HBM)


def neighbours(axis, by):
    size = lax.axis_size(axis)
    return [(i, i + by) for i in range(size) if 0 <= i + by < size]


def both_blocks(*args):
    image_tokens, labels, _ = args[:3]
    qkv_weight, bias_table, fc1_weight = args[5], args[7], args[10]
    tile_cols, c = image_tokens.shape[1:]
    groups = lax.axis_size("ch")
    swap = [(i, (i + 1) % groups) for i in range(groups)]
    part = qkv_weight.shape[3]
    hidden = fc1_weight.shape[2]
    entries = bias_table.shape[1]
    own_heads = bias_table.shape[2]
    tokens = WIN * WIN

    def others(value):
        found = [value]
        for _ in range(groups - 1):
            found.append(lax.ppermute(found[-1], "ch", swap))
        return found

    rows = 4 * part + (hidden // 128) * c + hidden + 3 * SMALL
    pack = jax.ShapeDtypeStruct((rows, 128), BF)
    edge = jax.ShapeDtypeStruct((WIN + 1, WIN, c), BF)
    args = list(args)
    args[5] = qkv_weight.transpose(0, 1, 3, 2)
    args[6] = args[6].transpose(1, 0, 2)
    args[7] = bias_table.transpose(0, 2, 1)
    staged = [pltpu.VMEM((2, WIN, 2 * WIN, c), BF)] + [pltpu.VMEM(a.shape, a.dtype) for a in args[1:]]
    own0, own1, left_edge, right_edge, rel2 = call(
        lambda *refs: pack_kernel(*refs, count=len(args)),
        (pack, pack, edge, edge, jax.ShapeDtypeStruct((tokens, 2 * tokens), jnp.int32)),
        staged + [pltpu.VMEM((SMALL, 128), F32), pltpu.SemaphoreType.DMA((len(args) + 1,))],
        *(in_hbm(a) for a in args),
        in_specs=[pl.BlockSpec(memory_space=pltpu.HBM)] * len(args),
    )
    packs0 = others(own0)
    left = lax.ppermute(right_edge, "col", neighbours("col", 1))
    right = lax.ppermute(left_edge, "col", neighbours("col", -1))
    packs1 = others(own1)

    sizes = dict(groups=groups, own_heads=own_heads, entries=entries, part=part, hidden=hidden)
    weights_scratch = [
        pltpu.VMEM((c, 3 * c), BF),
        pltpu.VMEM((c, c), BF),
        pltpu.VMEM((c, groups * hidden), BF),
        pltpu.VMEM((groups * hidden, c), BF),
        pltpu.VMEM((8, groups * hidden), F32),
    ]
    strip = jax.ShapeDtypeStruct((SHIFT, tile_cols + 2 * WIN, c), BF)
    bias_scratch = pltpu.VMEM((tokens, own_heads * groups * tokens), F32)
    wide = pltpu.VMEM((WIN, tile_cols + 4 * WIN, c), BF)
    near, far = call(
        lambda *refs: regular_kernel(*refs, **sizes),
        (strip, strip),
        [
            bias_scratch, wide, pltpu.VMEM(labels.shape, jnp.int32), pltpu.SemaphoreType.DMA((2,)),
            wide, pltpu.VMEM((2, 3, 4 * tokens, c), BF), pltpu.VMEM((2, 4 * tokens, c), BF),
            pltpu.VMEM((WIN, WIN, 128), BF),
        ] + weights_scratch,
        in_hbm(image_tokens), in_hbm(labels), left, right, rel2, *packs0,
        in_specs=[pl.BlockSpec(memory_space=pltpu.HBM)] * 2
        + [pl.BlockSpec(memory_space=pltpu.VMEM)] * (3 + groups),
    )
    bands = lax.axis_size(("row", "ch"))

    def swapped(value, first):
        pairs = [(m, m + 1) for m in range(first, bands - 1, 2)]
        return lax.ppermute(value, ("row", "ch"), pairs + [(j, i) for i, j in pairs])

    near_halo = swapped(near, 0)
    far_halo = swapped(far, 1)
    chunks = even_split(tile_cols // WIN + 1, 7)
    most = max(stop - base for base, stop in chunks) * SHIFT * WIN
    strip_wide = pltpu.VMEM((SHIFT, tile_cols + 2 * WIN, c), F32)
    scratch = [
        pltpu.VMEM((SHIFT * WIN, own_heads * groups * tokens), F32), strip_wide, strip_wide,
        pltpu.VMEM((SHIFT, tile_cols + WIN, c), F32),
        pltpu.VMEM((2, most, c), BF), pltpu.VMEM((2, 2, 2, most, c), BF), pltpu.VMEM((2, most, c), BF),
    ] + weights_scratch
    near_out = call(
        lambda *refs: shifted_kernel(*refs, chunks=chunks, near=True, **sizes),
        jax.ShapeDtypeStruct((SHIFT, tile_cols, c), BF),
        scratch, near, near_halo, rel2, *packs1,
    )
    return call(
        lambda *refs: shifted_kernel(*refs, chunks=chunks, near=False, **sizes),
        jax.ShapeDtypeStruct(image_tokens.shape, BF),
        scratch, far, far_halo, rel2, *packs1, near_out,
    )


def solution(mesh):
    in_specs = (
        P(("row", "ch"), "col", None),
        P(("row", "ch"), "col"),
        P(),
        P(),
        P(),
        P(None, None, None, "ch"),
        P(None, None, "ch"),
        P(None, None, "ch"),
        P(None, "ch", None),
        P(),
        P(None, None, "ch"),
        P(None, "ch"),
        P(None, "ch", None),
        P(),
    )
    out_specs = P(("row", "ch"), "col", None)
    return jax.shard_map(
        both_blocks, mesh=mesh, in_specs=in_specs, out_specs=out_specs, check_vma=False
    )
```

```python
import math

import jax
import jax.numpy as jnp
from jax import lax
from jax.experimental import pallas as pl
from jax.experimental.pallas import tpu as pltpu
from jax.sharding import PartitionSpec as P


WIN = 8
SHIFT = 4
EPS = 1e-05
NEG = -1e30
LOG2E = math.log2(math.e)
BF = jnp.bfloat16
F32 = jnp.float32


def dot_nt(a, b):
    return lax.dot_general(a, b, (((1,), (1,)), ((), ())), preferred_element_type=F32)


def dot_nn(a, b):
    return lax.dot_general(a, b, (((1,), (0,)), ((), ())), preferred_element_type=F32)


def gelu(v):
    half = 0.5 * v
    return half + half * lax.erf(v * math.sqrt(0.5))


def head_masks(heads, depth, width):
    lane = lax.broadcasted_iota(jnp.int32, (WIN * WIN, width), 1)
    return [(lane // depth == h).astype(F32).astype(BF) for h in range(heads)]


def stack_heads(rows, masks):
    return jnp.concatenate([rows * mask for mask in masks], axis=0)


def window_pieces(read, bias, allowed, write, masks, ones):
    at = {}

    def score():
        q, k, at["v"] = read()
        at["s"] = dot_nt(q, stack_heads(k, masks))

    def reduce():
        scores = at["s"] + bias()
        if allowed is not None:
            scores = jnp.where(allowed(), scores, NEG)
        first = lax.broadcasted_iota(jnp.int32, (scores.shape[0], 128), 1) < WIN * WIN
        parts = []
        for start in range(0, scores.shape[1], 128):
            s = scores[:, start : start + 128]
            low = jnp.max(jnp.where(first, s, NEG), axis=-1, keepdims=True)
            high = jnp.max(jnp.where(first, NEG, s), axis=-1, keepdims=True)
            parts.append((s, jnp.where(first, low, high)))
        at["s"] = parts

    def mix():
        weights = jnp.concatenate([jnp.exp2(s - m).astype(BF) for s, m in at["s"]], axis=1)
        rhs = jnp.concatenate([stack_heads(at["v"], masks), ones], axis=1)
        at["o"] = dot_nn(weights, rhs)

    def store():
        width = at["o"].shape[1] // 2
        write(at["o"][:, :width] / at["o"][:, width:])

    return [score, reduce, mix, store]


def skewed(pipelines):
    depth = max(len(p) for p in pipelines)
    return [
        pipelines[n][t - n]
        for t in range(len(pipelines) + depth - 1)
        for n in range(len(pipelines))
        if 0 <= t - n < len(pipelines[n])
    ]


def offset(threads, lag):
    return [
        thread[t - n * lag]
        for t in range(max(len(thread) + n * lag for n, thread in enumerate(threads)))
        for n, thread in enumerate(threads)
        if 0 <= t - n * lag < len(thread)
    ]


def weave(*threads):
    order = sorted(
        ((k + 0.5) / len(thread), n, k) for n, thread in enumerate(threads) for k in range(len(thread))
    )
    for _, n, k in order:
        threads[n][k]()


def pick(low_rows, high_rows, skip, wide):
    rows = wide.shape[0]
    in_low = wide < 128
    low_index = jnp.minimum(wide, 127)
    high_index = jnp.maximum(wide - skip, 0)
    first = lax.broadcasted_iota(jnp.int32, wide.shape, 1) < WIN * WIN

    def of_head(h):
        low = jnp.broadcast_to(low_rows[h] * LOG2E, (rows, 128))
        high = jnp.broadcast_to(high_rows[h] * LOG2E, (rows, 128))
        return jnp.where(
            in_low,
            jnp.take_along_axis(low, low_index, axis=1),
            jnp.take_along_axis(high, high_index, axis=1),
        )

    return jnp.concatenate(
        [jnp.where(first, of_head(h), of_head(h + 1)) for h in range(0, len(low_rows), 2)], axis=1
    )


def split3(value):
    high = value.astype(BF)
    rest = value - high.astype(F32)
    middle = rest.astype(BF)
    return [high, middle, (rest - middle.astype(F32)).astype(BF)]


QKVB, FC1B, TABLE = 0, 3, 5
GAIN, SHIFTS, PROJB, FC2B = 9, 11, 13, 14
SMALL = 16


def pack_kernel(*refs, count):
    hbm, refs = refs[:count], refs[count:]
    (w0_ref, w1_ref, left_ref, right_ref, rel2_ref), refs = refs[:5], refs[5:]
    staged, small_ref, sems = refs[:count], refs[count], refs[count + 1]
    cols = hbm[0].shape[1]
    edge = 2 * WIN
    copies = [
        pltpu.make_async_copy(hbm[0].at[:, 0:edge], staged[0].at[0], sems.at[0]),
        pltpu.make_async_copy(hbm[0].at[:, cols - edge : cols], staged[0].at[1], sems.at[count]),
    ]
    copies += [pltpu.make_async_copy(hbm[k], staged[k], sems.at[k]) for k in range(1, count)]
    for copy in copies:
        copy.start()
    for copy in copies:
        copy.wait()
    (x, labels, rel, gain, shift, qkv, qkvb, table, proj, projb, fc1, fc1b, fc2, fc2b) = staged
    c = x.shape[3]
    part = qkv.shape[2]
    hidden = fc1.shape[2]
    entries = table.shape[2]
    for b, out in enumerate((w0_ref, w1_ref)):
        at = 0
        for m in range(3):
            out[at : at + part, :] = qkv[b, m]
            at += part
        out[at : at + part, :] = proj[b]
        at += part
        for start in range(0, hidden, 128):
            out[at : at + c, :] = fc1[b, :, start : start + 128]
            at += c
        out[at : at + hidden, :] = fc2[b]
        at += hidden
        small_ref[...] = jnp.zeros_like(small_ref)
        for m in range(3):
            small_ref[QKVB + m : QKVB + m + 1, 0:part] = qkvb[m, b : b + 1]
        for k in range(hidden // 128):
            small_ref[FC1B + k : FC1B + k + 1, :] = fc1b[b : b + 1, k * 128 : (k + 1) * 128]
        k = TABLE
        for h in range(table.shape[1]):
            for first in (0, entries - 128):
                small_ref[k : k + 1, :] = table[b, h : h + 1, first : first + 128]
                k += 1
        small_ref[GAIN : GAIN + 2, :] = gain[b]
        small_ref[SHIFTS : SHIFTS + 2, :] = shift[b]
        small_ref[PROJB : PROJB + 1, :] = projb[b : b + 1, :]
        small_ref[FC2B : FC2B + 1, :] = fc2b[b : b + 1, :]
        for piece in split3(small_ref[...]):
            out[at : at + SMALL, :] = piece
            at += SMALL
    ids = (labels[...] + 1).astype(F32).astype(BF)
    for r in range(WIN):
        left_ref[r] = x[0, r, 0:WIN]
        right_ref[r] = x[1, r, WIN:]
    left_ref[WIN] = ids[:, 0:128]
    right_ref[WIN] = ids[:, cols - 128 : cols]
    rel2_ref[...] = jnp.concatenate([rel[...], rel[...]], axis=1)


class Weights:

    def __init__(self, packs, scratch, c, part, hidden):
        self.qkv, self.proj, self.fc1, self.fc2, self.rows = scratch
        self.c = c
        self.packs = packs
        self.part, self.hidden = part, hidden
        self.start_small = 4 * part + (hidden // 128) * c + hidden

    def small(self, row, rows=1, width=128):
        out = []
        for p in self.packs:
            at = self.start_small
            value = sum(
                p[at + k * SMALL : at + (k + 1) * SMALL, :].astype(F32) for k in range(3)
            )
            out.append(value[row : row + rows, :width])
        return out

    def load(self, attention=True):
        c, part, hidden = self.c, self.part, self.hidden
        for m in range(3 if attention else 0):
            rows = jnp.concatenate([p[m * part : (m + 1) * part, :] for p in self.packs], axis=0)
            self.qkv[:, m * c : (m + 1) * c] = rows.astype(F32).T.astype(BF)
        for g, p in enumerate(self.packs):
            at = 3 * part
            self.proj[g * part : (g + 1) * part, :] = p[at : at + part, :]
            at += part
            for k in range(hidden // 128):
                lane = g * hidden + k * 128
                self.fc1[:, lane : lane + 128] = p[at : at + c, :]
                at += c
            self.fc2[g * hidden : (g + 1) * hidden, :] = p[at : at + hidden, :]
        vectors = [self.small(GAIN + k)[0] for k in range(2)]
        vectors += [self.small(SHIFTS + k)[0] for k in range(2)]
        vectors += [self.small(PROJB)[0], self.small(FC2B)[0]]
        for k, row in enumerate(vectors):
            self.rows[k : k + 1, 0:c] = row
        self.rows[6:7, 0 : 3 * c] = jnp.concatenate(
            [v for m in range(3) for v in self.small(QKVB + m, width=part)], axis=1
        )
        rows = [self.small(FC1B + k) for k in range(hidden // 128)]
        self.rows[7:8, :] = jnp.concatenate(
            [row[g] for g in range(len(self.packs)) for row in rows], axis=1
        )

    def row(self, k):
        return self.rows[k : k + 1, 0 : self.c]

    def bias(self, own_heads, skip, wide):
        rows = [self.small(TABLE + k) for k in range(2 * own_heads)]
        low = [rows[2 * h][g] for g in range(len(self.packs)) for h in range(own_heads)]
        high = [rows[2 * h + 1][g] for g in range(len(self.packs)) for h in range(own_heads)]
        return pick(low, high, skip, wide)

    def norm_pieces(self, at, k):
        def mean():
            x = at["x"]
            at["center"] = x - jnp.mean(x, axis=-1, keepdims=True)

        def spread():
            center = at["center"]
            at["spread"] = jnp.mean(center * center, axis=-1, keepdims=True)

        def normed():
            scaled = at["center"] * lax.rsqrt(at["spread"] + EPS)
            at["normed"] = (scaled * self.row(k) + self.row(2 + k)).astype(BF)

        return [mean, spread, normed]

    def project_pieces(self, load, stores):
        at = {}
        c = self.c

        def begin():
            at["x"] = load()

        def product(m, scale, store):
            def dot():
                at[m] = dot_nn(at["normed"], self.qkv[:, m * c : (m + 1) * c])

            def keep():
                value = at.pop(m) + self.rows[6:7, m * c : (m + 1) * c]
                store((value if scale is None else value * scale).astype(BF))

            return dot, keep

        mean, spread, normed = self.norm_pieces(at, 0)
        made = [product(*entry) for entry in stores]

        def start():
            begin()
            mean()

        return [start, spread, normed], [dot for dot, _ in made] + [keep for _, keep in made]

    def finish_pieces(self, load, attended, store):
        at = {}
        width = 256

        def project():
            at["p"] = dot_nn(attended(), self.proj[...])

        def begin():
            middle = (load() + at.pop("p") + self.row(4)).astype(BF).astype(F32)
            at["x"] = middle
            at["middle"] = middle

        mean, spread, normed = self.norm_pieces(at, 1)

        def start():
            begin()
            mean()

        def up(k):
            def dot():
                at["up", k] = dot_nn(at["normed"], self.fc1[:, k : k + width])

            return dot

        def act(k):
            def gate():
                at["act", k] = gelu(at.pop(("up", k)) + self.rows[7:8, k : k + width]).astype(BF)

            return gate

        def down(k):
            def dot():
                at["down", k] = dot_nn(at.pop(("act", k)), self.fc2[k : k + width, :])

            return dot

        def end():
            total = at["middle"] + self.row(5)
            for k in starts:
                total = total + at["down", k]
            store(total)

        starts = range(0, self.fc2.shape[0], width)
        chains = [[up(k), act(k), down(k)] for k in starts]
        return [project, start, spread, normed], skewed(chains) + [end]


def pipeline(chunks, first, second, third):
    stages = []
    for i in range(chunks):
        norm, rest = first(i)
        mlp_start, mlp_rest = third(i)
        stages.append([norm, rest, second(i), mlp_start, mlp_rest])
    depth = len(stages[0])
    for t in range(chunks + depth - 1):
        weave(*[stages[t - d][d] for d in reversed(range(depth)) if 0 <= t - d < chunks])


def parity():
    return (lax.axis_index("row") * lax.axis_size("ch") + lax.axis_index("ch")) % 2


def edge_ids(left_ref, right_ref, labels):
    lanes = jnp.concatenate(
        [left_ref[WIN].astype(F32), (labels + 1).astype(F32), right_ref[WIN].astype(F32)], axis=1
    )
    span = lanes.shape[1]
    lane = lax.broadcasted_iota(jnp.int32, (WIN, span), 1)
    match = lane % WIN == lax.broadcasted_iota(jnp.int32, (WIN, span), 0)
    spread = jnp.concatenate(
        [jnp.where(match, lanes[r : r + 1], 0.0) for r in range(WIN)], axis=0
    ).astype(BF)
    source = lax.broadcasted_iota(jnp.int32, (span, 128), 0)
    window = lax.broadcasted_iota(jnp.int32, (span, 128), 1)
    chosen = ((source - 128 + SHIFT) // WIN == window) & (source >= 128 - SHIFT)
    return dot_nn(spread, chosen.astype(F32).astype(BF)).reshape(WIN, WIN, 128).astype(BF)


class Rows:

    def __init__(self, weights, x_ref, out_ref, cols):
        self.w, self.x, self.out, self.cols = weights, x_ref, out_ref, cols

    def pieces(self, start, count, attended):
        span = slice(start * WIN, (start + count) * WIN)

        def load():
            block = self.x[:, span, :].astype(F32)
            return jnp.concatenate(
                [block[r, n * WIN : (n + 1) * WIN] for n in range(count) for r in range(SHIFT)], axis=0
            )

        def store(out):
            for r in range(SHIFT):
                rows = [
                    out[(n * SHIFT + r) * WIN : (n * SHIFT + r + 1) * WIN] for n in range(count)
                ]
                if start * WIN < self.cols:
                    self.out[r, span, :] = jnp.concatenate(rows, axis=0).astype(BF)
                else:
                    before = lax.broadcasted_iota(jnp.int32, rows[0].shape, 0) < SHIFT
                    self.out[r, span.start : span.start + WIN, :] = jnp.where(
                        before, rows[1], rows[0]
                    ).astype(BF)

        return self.w.finish_pieces(load, attended, store)


def block0_chunks(cols):
    wins = cols // WIN
    return [(n, 4) for n in range(0, wins, 4)] + [(wins, 2)]


def put_edges(x_ref, left_ref, right_ref, cols, base=0):
    for r in range(x_ref.shape[0]):
        x_ref[r, cols : cols + 2 * WIN, :] = jnp.concatenate(
            [left_ref[base + r], right_ref[base + r]], axis=0
        )


def regular_kernel(
    x_hbm, labels_hbm, left_ref, right_ref, rel_ref, *refs, groups, own_heads, entries, part, hidden
):
    packs, refs = refs[:groups], refs[groups:]
    (near_ref, rest_ref, ids_ref, bias_ref, x_ref, side_ref), refs = refs[:6], refs[6:]
    (labels_ref, sems, qkv_ref, att_ref), scratch = refs[:4], refs[4:]
    side = 1 - parity()
    cols = x_hbm.shape[1]
    x_copy = pltpu.make_async_copy(x_hbm, x_ref.at[:, 0:cols], sems.at[0])
    labels_copy = pltpu.make_async_copy(labels_hbm, labels_ref, sems.at[1])
    side_copy = pltpu.make_async_copy(
        x_hbm.at[pl.ds(side * SHIFT, SHIFT)], side_ref.at[:, 0:cols], sems.at[2]
    )
    x_copy.start()
    labels_copy.start()
    side_copy.start()
    c = x_ref.shape[2]
    heads = own_heads * groups
    depth = c // heads
    tokens = WIN * WIN
    half = SHIFT * WIN
    scale = depth ** (-0.5) * LOG2E
    w = Weights(packs, scratch, c, part, hidden)
    w.load()
    masks = head_masks(heads, depth, c)
    ones = jnp.concatenate(masks, axis=0)
    bias_ref[...] = w.bias(own_heads, entries - 128, rel_ref[...])
    labels_copy.wait()
    ids_ref[...] = edge_ids(left_ref, right_ref, labels_ref[...])
    put_edges(x_ref, left_ref, right_ref, cols)
    put_edges(side_ref, left_ref, right_ref, cols, side * SHIFT)
    x_copy.wait()
    side_copy.wait()
    chunks = block0_chunks(cols)
    finish = Rows(w, side_ref, near_ref, cols)

    def first(i):
        start, count = chunks[i]

        def load():
            block = x_ref[:, start * WIN : (start + count) * WIN, :].astype(F32)
            return jnp.concatenate(
                [block[r, n * WIN : (n + 1) * WIN] for n in range(count) for r in range(WIN)], axis=0
            )

        def keep(m):
            def store(value):
                qkv_ref[i % 2, m, 0 : count * tokens] = value

            return store

        return w.project_pieces(load, [(0, scale, keep(0)), (1, None, keep(1)), (2, None, keep(2))])

    def second(i):
        start, count = chunks[i]

        def window(n):
            rows = slice(n * tokens, (n + 1) * tokens)

            def write(value):
                low, high = value[:half], value[half:]
                att_ref[i % 2, n * half : (n + 1) * half] = jnp.where(side == 0, low, high).astype(BF)
                rest_ref[(start + n) * half : (start + n + 1) * half] = jnp.where(
                    side == 0, high, low
                ).astype(BF)

            return window_pieces(
                lambda: [qkv_ref[i % 2, m, rows] for m in range(3)],
                lambda: bias_ref[...], None, write, masks, ones,
            )

        return skewed([window(n) for n in range(count)])

    def third(i):
        start, count = chunks[i]
        return finish.pieces(start, count, lambda: att_ref[i % 2, 0 : count * half])

    pipeline(len(chunks), first, second, third)
    for r in range(SHIFT):
        near_ref[r, cols + WIN :, :] = ids_ref[side * SHIFT + r]


def rest_kernel(x_hbm, left_ref, right_ref, att_ref, ids_ref, *refs, groups, own_heads, entries, part, hidden):
    packs, refs = refs[:groups], refs[groups:]
    (far_ref, x_ref, sems), scratch = refs[:3], refs[3:]
    cols = x_hbm.shape[1]
    side = parity()
    x_copy = pltpu.make_async_copy(
        x_hbm.at[pl.ds(side * SHIFT, SHIFT)], x_ref.at[:, 0:cols], sems.at[0]
    )
    x_copy.start()
    w = Weights(packs, scratch, x_ref.shape[2], part, hidden)
    w.load(attention=False)
    put_edges(x_ref, left_ref, right_ref, cols, side * SHIFT)
    finish = Rows(w, x_ref, far_ref, cols)
    half = SHIFT * WIN
    for r in range(SHIFT):
        far_ref[r, cols + WIN :, :] = ids_ref[side * SHIFT + r]
    x_copy.wait()
    threads = []
    for start, count in block0_chunks(cols):
        rows = slice(start * half, (start + count) * half)
        threads.append(sum(finish.pieces(start, count, lambda rows=rows: att_ref[rows]), []))
    for piece in offset(threads, 4):
        piece()


def even_split(count, most):
    parts = -(-count // most)
    return [(count * k // parts, count * (k + 1) // parts) for k in range(parts)]


def shifted_kernel(own_in, halo_in, rel_ref, *refs, chunks, near, groups, own_heads, entries, part, hidden):
    packs, refs = refs[:groups], refs[groups:]
    if not near:
        done_ref, refs = refs[0], refs[1:]
    (out_ref, bias_ref, own_ref, halo_ref, res_ref), refs = refs[:5], refs[5:]
    (q_ref, kv_ref, att_ref), scratch = refs[:3], refs[3:]
    side = 1 - parity() if near else parity()
    c = own_in.shape[2]
    cols = out_ref.shape[1]
    heads = own_heads * groups
    depth = c // heads
    half = SHIFT * WIN
    tokens = WIN * WIN
    scale = depth ** (-0.5) * LOG2E
    w = Weights(packs, scratch, c, part, hidden)
    w.load()
    masks = head_masks(heads, depth, c)
    ones = jnp.concatenate(masks, axis=0)

    rel = rel_ref[...]
    rel = jnp.concatenate(
        [
            jnp.concatenate([rel[a + SHIFT : a + WIN], rel[a : a + SHIFT]], axis=0)
            for a in range(0, tokens, WIN)
        ],
        axis=0,
    )
    lane = lax.broadcasted_iota(jnp.int32, rel.shape, 1)
    rel = jnp.where(lane % WIN < SHIFT, pltpu.roll(rel, 128 - SHIFT, 1), pltpu.roll(rel, SHIFT, 1))
    rel = jnp.where(side == 0, pltpu.roll(rel[half:], half, 1), rel[:half])
    bias_ref[...] = w.bias(own_heads, entries - 128, rel)

    parts = []
    for dst, src in ((own_ref, own_in), (halo_ref, halo_in)):
        value = src[...].astype(F32)
        edge = value[:, cols : cols + WIN]
        dst[:, 0:WIN, :] = edge
        dst[:, WIN : WIN + cols, :] = value[:, :cols]
        dst[:, WIN + cols :, :] = edge
        parts.append(value[:, cols + WIN :].reshape(half, 128))
    query_ids = parts[0]
    key_ids = jnp.concatenate(parts + parts, axis=0).T
    earlier = lax.broadcasted_iota(jnp.int32, (WIN, c), 0) < SHIFT

    def gather(ref, i):
        pieces = []
        for j in range(*chunks[i]):
            for r in range(SHIFT):
                before = ref[r, j * WIN : (j + 1) * WIN, :]
                after = ref[r, (j + 1) * WIN : (j + 2) * WIN, :]
                pieces.append(jnp.where(earlier, after, before))
        return jnp.concatenate(pieces, axis=0)

    def first(i):
        slot = i % 2
        count = (chunks[i][1] - chunks[i][0]) * half

        def keep(target):
            def store(value):
                target[0:count] = value

            return store

        own = w.project_pieces(
            lambda: gather(own_ref, i),
            [(0, scale, keep(q_ref.at[slot]))]
            + [(1 + m, None, keep(kv_ref.at[slot, m, 0])) for m in range(2)],
        )
        halo = w.project_pieces(
            lambda: gather(halo_ref, i), [(1 + m, None, keep(kv_ref.at[slot, m, 1])) for m in range(2)]
        )
        return [skewed(list(pair)) for pair in zip(own, halo)]

    def second(i):
        slot = i % 2
        base = chunks[i][0]

        def window(j):
            rows = slice((j - base) * half, (j - base + 1) * half)

            def read():
                k, v = (
                    jnp.concatenate([kv_ref[slot, m, 0, rows], kv_ref[slot, m, 1, rows]], axis=0)
                    for m in range(2)
                )
                return q_ref[slot, rows], k, v

            def allowed():
                same = jnp.broadcast_to(query_ids[:, j : j + 1], (half, 128)) == key_ids[j : j + 1, :]
                return jnp.concatenate([same, same], axis=1)

            def write(value):
                att_ref[slot, rows] = value.astype(BF)

            return window_pieces(read, lambda: bias_ref[...], allowed, write, masks, ones)

        return skewed([window(j) for j in range(*chunks[i])])

    def third(i):
        base, stop = chunks[i]

        def store(out):
            for r in range(SHIFT):
                res_ref[r, base * WIN : stop * WIN, :] = jnp.concatenate(
                    [
                        out[n * half + r * WIN : n * half + (r + 1) * WIN]
                        for n in range(stop - base)
                    ],
                    axis=0,
                )

        return w.finish_pieces(
            lambda: gather(own_ref, i), lambda: att_ref[i % 2, 0 : (stop - base) * half], store
        )

    pipeline(len(chunks), first, second, third)
    low = lax.broadcasted_iota(jnp.int32, (SHIFT, cols, c), 1) % WIN < SHIFT
    result = jnp.where(low, res_ref[:, 0:cols, :], res_ref[:, WIN : WIN + cols, :]).astype(BF)
    if near:
        out_ref[...] = result
    else:
        out_ref[pl.ds(side * SHIFT, SHIFT)] = result
        out_ref[pl.ds((1 - side) * SHIFT, SHIFT)] = done_ref[...]


def call(kernel, out_shapes, scratch, *args, in_specs=None):
    specs = {} if in_specs is None else {"in_specs": in_specs}
    return pl.pallas_call(
        kernel,
        out_shape=out_shapes,
        scratch_shapes=scratch,
        compiler_params=pltpu.CompilerParams(vmem_limit_bytes=48 * 1024 * 1024),
        **specs,
    )(*args)


def in_hbm(value):
    return pltpu.with_memory_space_constraint(value, pltpu.HBM)


def neighbours(axis, by):
    size = lax.axis_size(axis)
    return [(i, i + by) for i in range(size) if 0 <= i + by < size]


def both_blocks(*args):
    image_tokens, labels, _ = args[:3]
    qkv_weight, bias_table, fc1_weight = args[5], args[7], args[10]
    tile_cols, c = image_tokens.shape[1:]
    groups = lax.axis_size("ch")
    swap = [(i, (i + 1) % groups) for i in range(groups)]
    part = qkv_weight.shape[3]
    hidden = fc1_weight.shape[2]
    entries = bias_table.shape[1]
    own_heads = bias_table.shape[2]
    tokens = WIN * WIN

    def others(value):
        found = [value]
        for _ in range(groups - 1):
            found.append(lax.ppermute(found[-1], "ch", swap))
        return found

    rows = 4 * part + (hidden // 128) * c + hidden + 3 * SMALL
    pack = jax.ShapeDtypeStruct((rows, 128), BF)
    edge = jax.ShapeDtypeStruct((WIN + 1, WIN, c), BF)
    args = list(args)
    args[5] = qkv_weight.transpose(0, 1, 3, 2)
    args[6] = args[6].transpose(1, 0, 2)
    args[7] = bias_table.transpose(0, 2, 1)
    staged = [pltpu.VMEM((2, WIN, 2 * WIN, c), BF)] + [pltpu.VMEM(a.shape, a.dtype) for a in args[1:]]
    own0, own1, left_edge, right_edge, rel2 = call(
        lambda *refs: pack_kernel(*refs, count=len(args)),
        (pack, pack, edge, edge, jax.ShapeDtypeStruct((tokens, 2 * tokens), jnp.int32)),
        staged + [pltpu.VMEM((SMALL, 128), F32), pltpu.SemaphoreType.DMA((len(args) + 1,))],
        *(in_hbm(a) for a in args),
        in_specs=[pl.BlockSpec(memory_space=pltpu.HBM)] * len(args),
    )
    packs0 = others(own0)
    left = lax.ppermute(right_edge, "col", neighbours("col", 1))
    right = lax.ppermute(left_edge, "col", neighbours("col", -1))
    packs1 = others(own1)

    sizes = dict(groups=groups, own_heads=own_heads, entries=entries, part=part, hidden=hidden)
    weights_scratch = [
        pltpu.VMEM((c, 3 * c), BF),
        pltpu.VMEM((c, c), BF),
        pltpu.VMEM((c, groups * hidden), BF),
        pltpu.VMEM((groups * hidden, c), BF),
        pltpu.VMEM((8, groups * hidden), F32),
    ]
    strip = jax.ShapeDtypeStruct((SHIFT, tile_cols + 2 * WIN, c), BF)
    bias_scratch = pltpu.VMEM((tokens, own_heads * groups * tokens), F32)
    wide = pltpu.VMEM((WIN, tile_cols + 2 * WIN, c), BF)
    half_wide = pltpu.VMEM((SHIFT, tile_cols + 2 * WIN, c), BF)
    bands = lax.axis_size(("row", "ch"))

    def swapped(value, first):
        pairs = [(m, m + 1) for m in range(first, bands - 1, 2)]
        return lax.ppermute(value, ("row", "ch"), pairs + [(j, i) for i, j in pairs])

    in_vmem = pl.BlockSpec(memory_space=pltpu.VMEM)
    near, rest, ids = call(
        lambda *refs: regular_kernel(*refs, **sizes),
        (
            strip,
            jax.ShapeDtypeStruct((SHIFT * (tile_cols + 2 * WIN), c), BF),
            jax.ShapeDtypeStruct((WIN, WIN, 128), BF),
        ),
        [
            bias_scratch, wide, half_wide,
            pltpu.VMEM(labels.shape, jnp.int32), pltpu.SemaphoreType.DMA((3,)),
            pltpu.VMEM((2, 3, 4 * tokens, c), BF), pltpu.VMEM((2, 2 * tokens, c), BF),
        ] + weights_scratch,
        in_hbm(image_tokens), in_hbm(labels), left, right, rel2, *packs0,
        in_specs=[pl.BlockSpec(memory_space=pltpu.HBM)] * 2 + [in_vmem] * (3 + groups),
    )
    near_halo = swapped(near, 0)
    far = call(
        lambda *refs: rest_kernel(*refs, **sizes),
        strip,
        [half_wide, pltpu.SemaphoreType.DMA((1,))] + weights_scratch,
        in_hbm(image_tokens), left, right, rest, ids, *packs0,
        in_specs=[pl.BlockSpec(memory_space=pltpu.HBM)] + [in_vmem] * (4 + groups),
    )
    far_halo = swapped(far, 1)
    chunks = even_split(tile_cols // WIN + 1, 7)
    most = max(stop - base for base, stop in chunks) * SHIFT * WIN
    strip_wide = pltpu.VMEM((SHIFT, tile_cols + 2 * WIN, c), F32)
    scratch = [
        pltpu.VMEM((SHIFT * WIN, own_heads * groups * tokens), F32), strip_wide, strip_wide,
        pltpu.VMEM((SHIFT, tile_cols + WIN, c), F32),
        pltpu.VMEM((2, most, c), BF), pltpu.VMEM((2, 2, 2, most, c), BF), pltpu.VMEM((2, most, c), BF),
    ] + weights_scratch
    near_out = call(
        lambda *refs: shifted_kernel(*refs, chunks=chunks, near=True, **sizes),
        jax.ShapeDtypeStruct((SHIFT, tile_cols, c), BF),
        scratch, near, near_halo, rel2, *packs1,
    )
    return call(
        lambda *refs: shifted_kernel(*refs, chunks=chunks, near=False, **sizes),
        jax.ShapeDtypeStruct(image_tokens.shape, BF),
        scratch, far, far_halo, rel2, *packs1, near_out,
    )


def solution(mesh):
    in_specs = (
        P(("row", "ch"), "col", None),
        P(("row", "ch"), "col"),
        P(),
        P(),
        P(),
        P(None, None, None, "ch"),
        P(None, None, "ch"),
        P(None, None, "ch"),
        P(None, "ch", None),
        P(),
        P(None, None, "ch"),
        P(None, "ch"),
        P(None, "ch", None),
        P(),
    )
    out_specs = P(("row", "ch"), "col", None)
    return jax.shard_map(
        both_blocks, mesh=mesh, in_specs=in_specs, out_specs=out_specs, check_vma=False
    )
```

```python
import math

import jax
import jax.numpy as jnp
from jax import lax
from jax.experimental import pallas as pl
from jax.experimental.pallas import tpu as pltpu
from jax.sharding import PartitionSpec as P


WIN = 8
SHIFT = 4
EPS = 1e-05
NEG = -1e30
LOG2E = math.log2(math.e)
BF = jnp.bfloat16
F32 = jnp.float32


def dot_nt(a, b):
    return lax.dot_general(a, b, (((1,), (1,)), ((), ())), preferred_element_type=F32)


def dot_nn(a, b):
    return lax.dot_general(a, b, (((1,), (0,)), ((), ())), preferred_element_type=F32)


def gelu(v):
    half = 0.5 * v
    return half + half * lax.erf(v * math.sqrt(0.5))


def head_masks(heads, depth, width):
    lane = lax.broadcasted_iota(jnp.int32, (WIN * WIN, width), 1)
    return [(lane // depth == h).astype(F32).astype(BF) for h in range(heads)]


def stack_heads(rows, masks):
    return jnp.concatenate([rows * mask for mask in masks], axis=0)


def window_pieces(read, bias, allowed, write, masks, ones):
    at = {}

    def score():
        q, k, at["v"] = read()
        at["s"] = dot_nt(q, stack_heads(k, masks))

    def reduce():
        scores = at["s"] + bias()
        if allowed is not None:
            scores = jnp.where(allowed(), scores, NEG)
        first = lax.broadcasted_iota(jnp.int32, (scores.shape[0], 128), 1) < WIN * WIN
        parts = []
        for start in range(0, scores.shape[1], 128):
            s = scores[:, start : start + 128]
            low = jnp.max(jnp.where(first, s, NEG), axis=-1, keepdims=True)
            high = jnp.max(jnp.where(first, NEG, s), axis=-1, keepdims=True)
            parts.append((s, jnp.where(first, low, high)))
        at["s"] = parts

    def mix():
        weights = jnp.concatenate([jnp.exp2(s - m).astype(BF) for s, m in at["s"]], axis=1)
        rhs = jnp.concatenate([stack_heads(at["v"], masks), ones], axis=1)
        at["o"] = dot_nn(weights, rhs)

    def store():
        width = at["o"].shape[1] // 2
        write(at["o"][:, :width] / at["o"][:, width:])

    return [score, reduce, mix, store]


def skewed(pipelines):
    depth = max(len(p) for p in pipelines)
    return [
        pipelines[n][t - n]
        for t in range(len(pipelines) + depth - 1)
        for n in range(len(pipelines))
        if 0 <= t - n < len(pipelines[n])
    ]


def offset(threads, lag):
    return [
        thread[t - n * lag]
        for t in range(max(len(thread) + n * lag for n, thread in enumerate(threads)))
        for n, thread in enumerate(threads)
        if 0 <= t - n * lag < len(thread)
    ]


def weave(*threads):
    order = sorted(
        ((k + 0.5) / len(thread), n, k) for n, thread in enumerate(threads) for k in range(len(thread))
    )
    for _, n, k in order:
        threads[n][k]()


def pick(low_rows, high_rows, skip, wide):
    rows = wide.shape[0]
    in_low = wide < 128
    low_index = jnp.minimum(wide, 127)
    high_index = jnp.maximum(wide - skip, 0)
    first = lax.broadcasted_iota(jnp.int32, wide.shape, 1) < WIN * WIN

    def of_head(h):
        low = jnp.broadcast_to(low_rows[h] * LOG2E, (rows, 128))
        high = jnp.broadcast_to(high_rows[h] * LOG2E, (rows, 128))
        return jnp.where(
            in_low,
            jnp.take_along_axis(low, low_index, axis=1),
            jnp.take_along_axis(high, high_index, axis=1),
        )

    return jnp.concatenate(
        [jnp.where(first, of_head(h), of_head(h + 1)) for h in range(0, len(low_rows), 2)], axis=1
    )


def split3(value):
    high = value.astype(BF)
    rest = value - high.astype(F32)
    middle = rest.astype(BF)
    return [high, middle, (rest - middle.astype(F32)).astype(BF)]


QKVB, FC1B, TABLE = 0, 3, 5
GAIN, SHIFTS, PROJB, FC2B = 9, 11, 13, 14
SMALL = 16


def pack_kernel(*refs, count):
    hbm, refs = refs[:count], refs[count:]
    (w0_ref, w1_ref, left_ref, right_ref, rel2_ref), refs = refs[:5], refs[5:]
    staged, small_ref, sems = refs[:count], refs[count], refs[count + 1]
    cols = hbm[0].shape[1]
    edge = 2 * WIN
    copies = [
        pltpu.make_async_copy(hbm[0].at[:, 0:edge], staged[0].at[0], sems.at[0]),
        pltpu.make_async_copy(hbm[0].at[:, cols - edge : cols], staged[0].at[1], sems.at[count]),
    ]
    copies += [pltpu.make_async_copy(hbm[k], staged[k], sems.at[k]) for k in range(1, count)]
    for copy in copies:
        copy.start()
    for copy in copies:
        copy.wait()
    (x, labels, rel, gain, shift, qkv, qkvb, table, proj, projb, fc1, fc1b, fc2, fc2b) = staged
    c = x.shape[3]
    part = qkv.shape[2]
    hidden = fc1.shape[2]
    entries = table.shape[2]
    for b, out in enumerate((w0_ref, w1_ref)):
        at = 0
        for m in range(3):
            out[at : at + part, :] = qkv[b, m]
            at += part
        out[at : at + part, :] = proj[b]
        at += part
        for start in range(0, hidden, 128):
            out[at : at + c, :] = fc1[b, :, start : start + 128]
            at += c
        out[at : at + hidden, :] = fc2[b]
        at += hidden
        small_ref[...] = jnp.zeros_like(small_ref)
        for m in range(3):
            small_ref[QKVB + m : QKVB + m + 1, 0:part] = qkvb[m, b : b + 1]
        for k in range(hidden // 128):
            small_ref[FC1B + k : FC1B + k + 1, :] = fc1b[b : b + 1, k * 128 : (k + 1) * 128]
        k = TABLE
        for h in range(table.shape[1]):
            for first in (0, entries - 128):
                small_ref[k : k + 1, :] = table[b, h : h + 1, first : first + 128]
                k += 1
        small_ref[GAIN : GAIN + 2, :] = gain[b]
        small_ref[SHIFTS : SHIFTS + 2, :] = shift[b]
        small_ref[PROJB : PROJB + 1, :] = projb[b : b + 1, :]
        small_ref[FC2B : FC2B + 1, :] = fc2b[b : b + 1, :]
        for piece in split3(small_ref[...]):
            out[at : at + SMALL, :] = piece
            at += SMALL
    ids = (labels[...] + 1).astype(F32).astype(BF)
    for r in range(WIN):
        left_ref[r] = x[0, r, 0:WIN]
        right_ref[r] = x[1, r, WIN:]
    left_ref[WIN] = ids[:, 0:128]
    right_ref[WIN] = ids[:, cols - 128 : cols]
    rel2_ref[...] = jnp.concatenate([rel[...], rel[...]], axis=1)


class Weights:

    def __init__(self, packs, scratch, c, part, hidden):
        self.qkv, self.proj, self.fc1, self.fc2, self.rows = scratch
        self.c = c
        self.packs = packs
        self.part, self.hidden = part, hidden
        self.start_small = 4 * part + (hidden // 128) * c + hidden

    def small(self, row, rows=1, width=128):
        out = []
        for p in self.packs:
            at = self.start_small
            value = sum(
                p[at + k * SMALL : at + (k + 1) * SMALL, :].astype(F32) for k in range(3)
            )
            out.append(value[row : row + rows, :width])
        return out

    def load_rows(self):
        c, part, hidden = self.c, self.part, self.hidden
        vectors = [self.small(GAIN + k)[0] for k in range(2)]
        vectors += [self.small(SHIFTS + k)[0] for k in range(2)]
        vectors += [self.small(PROJB)[0], self.small(FC2B)[0]]
        for k, row in enumerate(vectors):
            self.rows[k : k + 1, 0:c] = row
        self.rows[6:7, 0 : 3 * c] = jnp.concatenate(
            [v for m in range(3) for v in self.small(QKVB + m, width=part)], axis=1
        )
        rows = [self.small(FC1B + k) for k in range(hidden // 128)]
        self.rows[7:8, :] = jnp.concatenate(
            [row[g] for g in range(len(self.packs)) for row in rows], axis=1
        )

    def load_qkv(self):
        c, part = self.c, self.part
        for m in range(3):
            rows = jnp.concatenate([p[m * part : (m + 1) * part, :] for p in self.packs], axis=0)
            self.qkv[:, m * c : (m + 1) * c] = rows.astype(F32).T.astype(BF)

    def load_rest(self):
        c, part, hidden = self.c, self.part, self.hidden
        for g, p in enumerate(self.packs):
            at = 3 * part
            self.proj[g * part : (g + 1) * part, :] = p[at : at + part, :]
            at += part
            for k in range(hidden // 128):
                lane = g * hidden + k * 128
                self.fc1[:, lane : lane + 128] = p[at : at + c, :]
                at += c
            self.fc2[g * hidden : (g + 1) * hidden, :] = p[at : at + hidden, :]

    def row(self, k):
        return self.rows[k : k + 1, 0 : self.c]

    def bias(self, own_heads, skip, wide):
        rows = [self.small(TABLE + k) for k in range(2 * own_heads)]
        low = [rows[2 * h][g] for g in range(len(self.packs)) for h in range(own_heads)]
        high = [rows[2 * h + 1][g] for g in range(len(self.packs)) for h in range(own_heads)]
        return pick(low, high, skip, wide)

    def norm_pieces(self, at, k):
        def mean():
            x = at["x"]
            at["center"] = x - jnp.mean(x, axis=-1, keepdims=True)

        def spread():
            center = at["center"]
            at["spread"] = jnp.mean(center * center, axis=-1, keepdims=True)

        def normed():
            scaled = at["center"] * lax.rsqrt(at["spread"] + EPS)
            at["normed"] = (scaled * self.row(k) + self.row(2 + k)).astype(BF)

        return [mean, spread, normed]

    def project_pieces(self, load, stores, normed_load=None):
        at = {}
        c = self.c

        def begin():
            at["x"] = load()

        def product(m, scale, store):
            def dot():
                at[m] = dot_nn(at["normed"], self.qkv[:, m * c : (m + 1) * c])

            def keep():
                value = at.pop(m) + self.rows[6:7, m * c : (m + 1) * c]
                store((value if scale is None else value * scale).astype(BF))

            return dot, keep

        mean, spread, normed = self.norm_pieces(at, 0)
        made = [product(*entry) for entry in stores]

        def start():
            begin()
            mean()

        rest = [dot for dot, _ in made] + [keep for _, keep in made]
        if normed_load is None:
            return [start, spread, normed], rest

        def read():
            at["normed"] = normed_load()

        return [read] + rest

    def finish_pieces(self, load, attended, store):
        at = {}
        width = 256

        def project():
            at["p"] = dot_nn(attended(), self.proj[...])

        def begin():
            middle = (load() + at.pop("p") + self.row(4)).astype(BF).astype(F32)
            at["x"] = middle
            at["middle"] = middle

        mean, spread, normed = self.norm_pieces(at, 1)

        def start():
            begin()
            mean()

        def up(k):
            def dot():
                at["up", k] = dot_nn(at["normed"], self.fc1[:, k : k + width])

            return dot

        def act(k):
            def gate():
                at["act", k] = gelu(at.pop(("up", k)) + self.rows[7:8, k : k + width]).astype(BF)

            return gate

        def down(k):
            def dot():
                at["down", k] = dot_nn(at.pop(("act", k)), self.fc2[k : k + width, :])

            return dot

        def end():
            total = at["middle"] + self.row(5)
            for k in starts:
                total = total + at["down", k]
            store(total)

        starts = range(0, self.fc2.shape[0], width)
        chains = [[up(k), act(k), down(k)] for k in starts]
        return [project, start, spread, normed], skewed(chains) + [end]


def pipeline(chunks, extra, *makers):
    stages = [[stage for make in makers for stage in make(i)] for i in range(chunks)]
    depth = len(stages[0])
    for t in range(chunks + depth - 1):
        threads = [stages[t - d][d] for d in reversed(range(depth)) if 0 <= t - d < chunks]
        if t == 0:
            threads.append(extra)
        weave(*threads)


def parity():
    return (lax.axis_index("row") * lax.axis_size("ch") + lax.axis_index("ch")) % 2


def edge_ids(left_ref, right_ref, labels):
    lanes = jnp.concatenate(
        [left_ref[WIN].astype(F32), (labels + 1).astype(F32), right_ref[WIN].astype(F32)], axis=1
    )
    span = lanes.shape[1]
    lane = lax.broadcasted_iota(jnp.int32, (WIN, span), 1)
    match = lane % WIN == lax.broadcasted_iota(jnp.int32, (WIN, span), 0)
    spread = jnp.concatenate(
        [jnp.where(match, lanes[r : r + 1], 0.0) for r in range(WIN)], axis=0
    ).astype(BF)
    source = lax.broadcasted_iota(jnp.int32, (span, 128), 0)
    window = lax.broadcasted_iota(jnp.int32, (span, 128), 1)
    chosen = ((source - 128 + SHIFT) // WIN == window) & (source >= 128 - SHIFT)
    return dot_nn(spread, chosen.astype(F32).astype(BF)).reshape(WIN, WIN, 128).astype(BF)


class Rows:

    def __init__(self, weights, x_ref, out_ref, cols):
        self.w, self.x, self.out, self.cols = weights, x_ref, out_ref, cols

    def pieces(self, start, count, attended):
        span = slice(start * WIN, (start + count) * WIN)

        def load():
            block = self.x[:, span, :].astype(F32)
            return jnp.concatenate(
                [block[r, n * WIN : (n + 1) * WIN] for n in range(count) for r in range(SHIFT)], axis=0
            )

        def store(out):
            for r in range(SHIFT):
                rows = [
                    out[(n * SHIFT + r) * WIN : (n * SHIFT + r + 1) * WIN] for n in range(count)
                ]
                if start * WIN < self.cols:
                    self.out[r, span, :] = jnp.concatenate(rows, axis=0).astype(BF)
                else:
                    before = lax.broadcasted_iota(jnp.int32, rows[0].shape, 0) < SHIFT
                    self.out[r, span.start : span.start + WIN, :] = jnp.where(
                        before, rows[1], rows[0]
                    ).astype(BF)

        return self.w.finish_pieces(load, attended, store)


def block0_chunks(cols, size=4):
    wins = cols // WIN
    return [(n, min(size, wins - n)) for n in range(0, wins, size)] + [(wins, 2)]


def put_edges(x_ref, left_ref, right_ref, cols, base=0):
    for r in range(x_ref.shape[0]):
        x_ref[r, cols : cols + 2 * WIN, :] = jnp.concatenate(
            [left_ref[base + r], right_ref[base + r]], axis=0
        )


def norm_kernel(x_hbm, left_ref, right_ref, pack_ref, normed_ref, x_ref, rows_ref, sem, *, part, hidden):
    cols = x_hbm.shape[1]
    x_copy = pltpu.make_async_copy(x_hbm, x_ref.at[:, 0:cols], sem.at[0])
    x_copy.start()
    w = Weights([pack_ref], (None, None, None, None, rows_ref), x_ref.shape[2], part, hidden)
    for k in range(2):
        rows_ref[k : k + 1, :] = w.small(GAIN + k)[0]
        rows_ref[2 + k : 3 + k, :] = w.small(SHIFTS + k)[0]
    put_edges(x_ref, left_ref, right_ref, cols)
    x_copy.wait()
    tokens = WIN * WIN

    def chunk(start, count):
        at = {}

        def begin():
            block = x_ref[:, start * WIN : (start + count) * WIN, :].astype(F32)
            at["x"] = jnp.concatenate(
                [block[r, n * WIN : (n + 1) * WIN] for n in range(count) for r in range(WIN)], axis=0
            )

        def keep():
            normed_ref[start * tokens : (start + count) * tokens] = at["normed"]

        mean, spread, normed = w.norm_pieces(at, 0)
        return [begin, mean, spread, normed, keep]

    wins = cols // WIN + 2
    for piece in offset([chunk(n, 2) for n in range(0, wins, 2)], 1):
        piece()


def regular_kernel(
    x_hbm, labels_hbm, left_ref, right_ref, rel_ref, normed_ref, *refs,
    groups, own_heads, entries, part, hidden,
):
    packs, refs = refs[:groups], refs[groups:]
    (near_ref, rest_ref, ids_ref, bias_ref, side_ref), refs = refs[:5], refs[5:]
    (labels_ref, sems, qkv_ref, att_ref), scratch = refs[:4], refs[4:]
    side = 1 - parity()
    cols = x_hbm.shape[1]
    labels_copy = pltpu.make_async_copy(labels_hbm, labels_ref, sems.at[0])
    side_copy = pltpu.make_async_copy(
        x_hbm.at[pl.ds(side * SHIFT, SHIFT)], side_ref.at[:, 0:cols], sems.at[1]
    )
    labels_copy.start()
    side_copy.start()
    c = side_ref.shape[2]
    heads = own_heads * groups
    depth = c // heads
    tokens = WIN * WIN
    half = SHIFT * WIN
    scale = depth ** (-0.5) * LOG2E
    w = Weights(packs, scratch, c, part, hidden)
    masks = head_masks(heads, depth, c)
    ones = jnp.concatenate(masks, axis=0)
    w.load_rows()
    w.load_qkv()

    def pick_bias():
        bias_ref[...] = w.bias(own_heads, entries - 128, rel_ref[...])

    def put_ids():
        ids_ref[...] = edge_ids(left_ref, right_ref, labels_ref[...])

    labels_copy.wait()
    side_copy.wait()
    put_edges(side_ref, left_ref, right_ref, cols, side * SHIFT)
    extra = [pick_bias, put_ids, w.load_rest]
    chunks = block0_chunks(cols)
    finish = Rows(w, side_ref, near_ref, cols)

    def first(i):
        start, count = chunks[i]

        def keep(m):
            def store(value):
                qkv_ref[i % 2, m, 0 : count * tokens] = value

            return store

        rows = slice(start * tokens, (start + count) * tokens)
        entries_of = [(0, scale, keep(0)), (1, None, keep(1)), (2, None, keep(2))]
        return [w.project_pieces(None, entries_of, lambda: normed_ref[rows])]

    def second(i):
        start, count = chunks[i]

        def window(n):
            rows = slice(n * tokens, (n + 1) * tokens)

            def write(value):
                low, high = value[:half], value[half:]
                att_ref[i % 2, n * half : (n + 1) * half] = jnp.where(side == 0, low, high).astype(BF)
                rest_ref[(start + n) * half : (start + n + 1) * half] = jnp.where(
                    side == 0, high, low
                ).astype(BF)

            return window_pieces(
                lambda: [qkv_ref[i % 2, m, rows] for m in range(3)],
                lambda: bias_ref[...], None, write, masks, ones,
            )

        return [skewed([window(n) for n in range(count)])]

    def third(i):
        start, count = chunks[i]
        return finish.pieces(start, count, lambda: att_ref[i % 2, 0 : count * half])

    pipeline(len(chunks), extra, first, second, third)
    for r in range(SHIFT):
        near_ref[r, cols + WIN :, :] = ids_ref[side * SHIFT + r]


def rest_kernel(x_hbm, left_ref, right_ref, att_ref, ids_ref, *refs, groups, own_heads, entries, part, hidden):
    packs, refs = refs[:groups], refs[groups:]
    (far_ref, x_ref, sems), scratch = refs[:3], refs[3:]
    cols = x_hbm.shape[1]
    side = parity()
    x_copy = pltpu.make_async_copy(
        x_hbm.at[pl.ds(side * SHIFT, SHIFT)], x_ref.at[:, 0:cols], sems.at[0]
    )
    x_copy.start()
    w = Weights(packs, scratch, x_ref.shape[2], part, hidden)
    w.load_rows()
    w.load_rest()
    put_edges(x_ref, left_ref, right_ref, cols, side * SHIFT)
    finish = Rows(w, x_ref, far_ref, cols)
    half = SHIFT * WIN
    for r in range(SHIFT):
        far_ref[r, cols + WIN :, :] = ids_ref[side * SHIFT + r]
    x_copy.wait()
    threads = []
    for start, count in block0_chunks(cols, 8):
        rows = slice(start * half, (start + count) * half)
        threads.append(sum(finish.pieces(start, count, lambda rows=rows: att_ref[rows]), []))
    for piece in offset(threads, 3):
        piece()


def even_split(count, most):
    parts = -(-count // most)
    return [(count * k // parts, count * (k + 1) // parts) for k in range(parts)]


def shifted_kernel(own_in, halo_in, rel_ref, *refs, chunks, near, groups, own_heads, entries, part, hidden):
    packs, refs = refs[:groups], refs[groups:]
    if not near:
        done_ref, refs = refs[0], refs[1:]
    (out_ref, bias_ref, own_ref, halo_ref, res_ref), refs = refs[:5], refs[5:]
    (q_ref, kv_ref, att_ref), scratch = refs[:3], refs[3:]
    side = 1 - parity() if near else parity()
    c = own_in.shape[2]
    cols = out_ref.shape[1]
    heads = own_heads * groups
    depth = c // heads
    half = SHIFT * WIN
    tokens = WIN * WIN
    scale = depth ** (-0.5) * LOG2E
    w = Weights(packs, scratch, c, part, hidden)
    w.load_rows()
    masks = head_masks(heads, depth, c)
    ones = jnp.concatenate(masks, axis=0)

    def pick_bias():
        rel = rel_ref[...]
        rel = jnp.concatenate(
            [
                jnp.concatenate([rel[a + SHIFT : a + WIN], rel[a : a + SHIFT]], axis=0)
                for a in range(0, tokens, WIN)
            ],
            axis=0,
        )
        lane = lax.broadcasted_iota(jnp.int32, rel.shape, 1)
        rel = jnp.where(lane % WIN < SHIFT, pltpu.roll(rel, 128 - SHIFT, 1), pltpu.roll(rel, SHIFT, 1))
        rel = jnp.where(side == 0, pltpu.roll(rel[half:], half, 1), rel[:half])
        bias_ref[...] = w.bias(own_heads, entries - 128, rel)

    parts = []
    for dst, src in ((own_ref, own_in), (halo_ref, halo_in)):
        value = src[...].astype(F32)
        edge = value[:, cols : cols + WIN]
        dst[:, 0:WIN, :] = edge
        dst[:, WIN : WIN + cols, :] = value[:, :cols]
        dst[:, WIN + cols :, :] = edge
        parts.append(value[:, cols + WIN :].reshape(half, 128))
    query_ids = parts[0]
    key_ids = jnp.concatenate(parts + parts, axis=0).T
    earlier = lax.broadcasted_iota(jnp.int32, (WIN, c), 0) < SHIFT

    def gather(ref, i):
        pieces = []
        for j in range(*chunks[i]):
            for r in range(SHIFT):
                before = ref[r, j * WIN : (j + 1) * WIN, :]
                after = ref[r, (j + 1) * WIN : (j + 2) * WIN, :]
                pieces.append(jnp.where(earlier, after, before))
        return jnp.concatenate(pieces, axis=0)

    def first(i):
        slot = i % 2
        count = (chunks[i][1] - chunks[i][0]) * half

        def keep(target):
            def store(value):
                target[0:count] = value

            return store

        own = w.project_pieces(
            lambda: gather(own_ref, i),
            [(0, scale, keep(q_ref.at[slot]))]
            + [(1 + m, None, keep(kv_ref.at[slot, m, 0])) for m in range(2)],
        )
        halo = w.project_pieces(
            lambda: gather(halo_ref, i), [(1 + m, None, keep(kv_ref.at[slot, m, 1])) for m in range(2)]
        )
        return [skewed(list(pair)) for pair in zip(own, halo)]

    def second(i):
        slot = i % 2
        base = chunks[i][0]

        def window(j):
            rows = slice((j - base) * half, (j - base + 1) * half)

            def read():
                k, v = (
                    jnp.concatenate([kv_ref[slot, m, 0, rows], kv_ref[slot, m, 1, rows]], axis=0)
                    for m in range(2)
                )
                return q_ref[slot, rows], k, v

            def allowed():
                same = jnp.broadcast_to(query_ids[:, j : j + 1], (half, 128)) == key_ids[j : j + 1, :]
                return jnp.concatenate([same, same], axis=1)

            def write(value):
                att_ref[slot, rows] = value.astype(BF)

            return window_pieces(read, lambda: bias_ref[...], allowed, write, masks, ones)

        return [skewed([window(j) for j in range(*chunks[i])])]

    def third(i):
        base, stop = chunks[i]

        def store(out):
            for r in range(SHIFT):
                res_ref[r, base * WIN : stop * WIN, :] = jnp.concatenate(
                    [
                        out[n * half + r * WIN : n * half + (r + 1) * WIN]
                        for n in range(stop - base)
                    ],
                    axis=0,
                )

        return w.finish_pieces(
            lambda: gather(own_ref, i), lambda: att_ref[i % 2, 0 : (stop - base) * half], store
        )

    pipeline(len(chunks), [w.load_qkv, pick_bias, w.load_rest], first, second, third)
    low = lax.broadcasted_iota(jnp.int32, (SHIFT, cols, c), 1) % WIN < SHIFT
    result = jnp.where(low, res_ref[:, 0:cols, :], res_ref[:, WIN : WIN + cols, :]).astype(BF)
    if near:
        out_ref[...] = result
    else:
        out_ref[pl.ds(side * SHIFT, SHIFT)] = result
        out_ref[pl.ds((1 - side) * SHIFT, SHIFT)] = done_ref[...]


def call(kernel, out_shapes, scratch, *args, in_specs=None):
    specs = {} if in_specs is None else {"in_specs": in_specs}
    return pl.pallas_call(
        kernel,
        out_shape=out_shapes,
        scratch_shapes=scratch,
        compiler_params=pltpu.CompilerParams(vmem_limit_bytes=48 * 1024 * 1024),
        **specs,
    )(*args)


def in_hbm(value):
    return pltpu.with_memory_space_constraint(value, pltpu.HBM)


def neighbours(axis, by):
    size = lax.axis_size(axis)
    return [(i, i + by) for i in range(size) if 0 <= i + by < size]


def both_blocks(*args):
    image_tokens, labels, _ = args[:3]
    qkv_weight, bias_table, fc1_weight = args[5], args[7], args[10]
    tile_cols, c = image_tokens.shape[1:]
    groups = lax.axis_size("ch")
    swap = [(i, (i + 1) % groups) for i in range(groups)]
    part = qkv_weight.shape[3]
    hidden = fc1_weight.shape[2]
    entries = bias_table.shape[1]
    own_heads = bias_table.shape[2]
    tokens = WIN * WIN

    def others(value):
        found = [value]
        for _ in range(groups - 1):
            found.append(lax.ppermute(found[-1], "ch", swap))
        return found

    rows = 4 * part + (hidden // 128) * c + hidden + 3 * SMALL
    pack = jax.ShapeDtypeStruct((rows, 128), BF)
    edge = jax.ShapeDtypeStruct((WIN + 1, WIN, c), BF)
    args = list(args)
    args[5] = qkv_weight.transpose(0, 1, 3, 2)
    args[6] = args[6].transpose(1, 0, 2)
    args[7] = bias_table.transpose(0, 2, 1)
    staged = [pltpu.VMEM((2, WIN, 2 * WIN, c), BF)] + [pltpu.VMEM(a.shape, a.dtype) for a in args[1:]]
    own0, own1, left_edge, right_edge, rel2 = call(
        lambda *refs: pack_kernel(*refs, count=len(args)),
        (pack, pack, edge, edge, jax.ShapeDtypeStruct((tokens, 2 * tokens), jnp.int32)),
        staged + [pltpu.VMEM((SMALL, 128), F32), pltpu.SemaphoreType.DMA((len(args) + 1,))],
        *(in_hbm(a) for a in args),
        in_specs=[pl.BlockSpec(memory_space=pltpu.HBM)] * len(args),
    )
    packs0 = others(own0)
    left = lax.ppermute(right_edge, "col", neighbours("col", 1))
    right = lax.ppermute(left_edge, "col", neighbours("col", -1))
    packs1 = others(own1)

    sizes = dict(groups=groups, own_heads=own_heads, entries=entries, part=part, hidden=hidden)
    weights_scratch = [
        pltpu.VMEM((c, 3 * c), BF),
        pltpu.VMEM((c, c), BF),
        pltpu.VMEM((c, groups * hidden), BF),
        pltpu.VMEM((groups * hidden, c), BF),
        pltpu.VMEM((8, groups * hidden), F32),
    ]
    strip = jax.ShapeDtypeStruct((SHIFT, tile_cols + 2 * WIN, c), BF)
    bias_scratch = pltpu.VMEM((tokens, own_heads * groups * tokens), F32)
    wide = pltpu.VMEM((WIN, tile_cols + 2 * WIN, c), BF)
    half_wide = pltpu.VMEM((SHIFT, tile_cols + 2 * WIN, c), BF)
    bands = lax.axis_size(("row", "ch"))

    def swapped(value, first):
        pairs = [(m, m + 1) for m in range(first, bands - 1, 2)]
        return lax.ppermute(value, ("row", "ch"), pairs + [(j, i) for i, j in pairs])

    in_vmem = pl.BlockSpec(memory_space=pltpu.VMEM)
    normed = call(
        lambda *refs: norm_kernel(*refs, part=part, hidden=hidden),
        jax.ShapeDtypeStruct((tokens * (tile_cols // WIN + 2), c), BF),
        [wide, pltpu.VMEM((4, c), F32), pltpu.SemaphoreType.DMA((1,))],
        in_hbm(image_tokens), left, right, own0,
        in_specs=[pl.BlockSpec(memory_space=pltpu.HBM)] + [in_vmem] * 3,
    )
    near, rest, ids = call(
        lambda *refs: regular_kernel(*refs, **sizes),
        (
            strip,
            jax.ShapeDtypeStruct((SHIFT * (tile_cols + 2 * WIN), c), BF),
            jax.ShapeDtypeStruct((WIN, WIN, 128), BF),
        ),
        [
            bias_scratch, half_wide,
            pltpu.VMEM(labels.shape, jnp.int32), pltpu.SemaphoreType.DMA((2,)),
            pltpu.VMEM((2, 3, 4 * tokens, c), BF), pltpu.VMEM((2, 2 * tokens, c), BF),
        ] + weights_scratch,
        in_hbm(image_tokens), in_hbm(labels), left, right, rel2, normed, *packs0,
        in_specs=[pl.BlockSpec(memory_space=pltpu.HBM)] * 2 + [in_vmem] * (4 + groups),
    )
    near_halo = swapped(near, 0)
    far = call(
        lambda *refs: rest_kernel(*refs, **sizes),
        strip,
        [half_wide, pltpu.SemaphoreType.DMA((1,))] + weights_scratch,
        in_hbm(image_tokens), left, right, rest, ids, *packs0,
        in_specs=[pl.BlockSpec(memory_space=pltpu.HBM)] + [in_vmem] * (4 + groups),
    )
    far_halo = swapped(far, 1)
    chunks = even_split(tile_cols // WIN + 1, 11)
    most = max(stop - base for base, stop in chunks) * SHIFT * WIN
    strip_wide = pltpu.VMEM((SHIFT, tile_cols + 2 * WIN, c), F32)
    scratch = [
        pltpu.VMEM((SHIFT * WIN, own_heads * groups * tokens), F32), strip_wide, strip_wide,
        pltpu.VMEM((SHIFT, tile_cols + WIN, c), F32),
        pltpu.VMEM((2, most, c), BF), pltpu.VMEM((2, 2, 2, most, c), BF), pltpu.VMEM((2, most, c), BF),
    ] + weights_scratch
    near_out = call(
        lambda *refs: shifted_kernel(*refs, chunks=chunks, near=True, **sizes),
        jax.ShapeDtypeStruct((SHIFT, tile_cols, c), BF),
        scratch, near, near_halo, rel2, *packs1,
    )
    return call(
        lambda *refs: shifted_kernel(*refs, chunks=chunks, near=False, **sizes),
        jax.ShapeDtypeStruct(image_tokens.shape, BF),
        scratch, far, far_halo, rel2, *packs1, near_out,
    )


def solution(mesh):
    in_specs = (
        P(("row", "ch"), "col", None),
        P(("row", "ch"), "col"),
        P(),
        P(),
        P(),
        P(None, None, None, "ch"),
        P(None, None, "ch"),
        P(None, None, "ch"),
        P(None, "ch", None),
        P(),
        P(None, None, "ch"),
        P(None, "ch"),
        P(None, "ch", None),
        P(),
    )
    out_specs = P(("row", "ch"), "col", None)
    return jax.shard_map(
        both_blocks, mesh=mesh, in_specs=in_specs, out_specs=out_specs, check_vma=False
    )
```

```python
import math

import jax
import jax.numpy as jnp
from jax import lax
from jax.experimental import pallas as pl
from jax.experimental.pallas import tpu as pltpu
from jax.sharding import PartitionSpec as P


WIN = 8
SHIFT = 4
EPS = 1e-05
NEG = -1e30
LOG2E = math.log2(math.e)
BF = jnp.bfloat16
F32 = jnp.float32


def dot_nt(a, b):
    return lax.dot_general(a, b, (((1,), (1,)), ((), ())), preferred_element_type=F32)


def dot_nn(a, b):
    return lax.dot_general(a, b, (((1,), (0,)), ((), ())), preferred_element_type=F32)


def gelu(v):
    half = 0.5 * v
    return half + half * lax.erf(v * math.sqrt(0.5))


def head_masks(heads, depth, width):
    lane = lax.broadcasted_iota(jnp.int32, (WIN * WIN, width), 1)
    return [(lane // depth == h).astype(F32).astype(BF) for h in range(heads)]


def stack_heads(rows, masks):
    return jnp.concatenate([rows * mask for mask in masks], axis=0)


def window_pieces(read, bias, allowed, write, masks, ones):
    at = {}

    def score():
        q, k, at["v"] = read()
        at["s"] = dot_nt(q, stack_heads(k, masks))

    def reduce():
        scores = at["s"] + bias()
        if allowed is not None:
            scores = jnp.where(allowed(), scores, NEG)
        first = lax.broadcasted_iota(jnp.int32, (scores.shape[0], 128), 1) < WIN * WIN
        parts = []
        for start in range(0, scores.shape[1], 128):
            s = scores[:, start : start + 128]
            low = jnp.max(jnp.where(first, s, NEG), axis=-1, keepdims=True)
            high = jnp.max(jnp.where(first, NEG, s), axis=-1, keepdims=True)
            parts.append((s, jnp.where(first, low, high)))
        at["s"] = parts

    def mix():
        weights = jnp.concatenate([jnp.exp2(s - m).astype(BF) for s, m in at["s"]], axis=1)
        rhs = jnp.concatenate([stack_heads(at["v"], masks), ones], axis=1)
        at["o"] = dot_nn(weights, rhs)

    def store():
        width = at["o"].shape[1] // 2
        write(at["o"][:, :width] / at["o"][:, width:])

    return [score, reduce, mix, store]


def skewed(pipelines):
    depth = max(len(p) for p in pipelines)
    return [
        pipelines[n][t - n]
        for t in range(len(pipelines) + depth - 1)
        for n in range(len(pipelines))
        if 0 <= t - n < len(pipelines[n])
    ]


def offset(threads, lag):
    return [
        thread[t - n * lag]
        for t in range(max(len(thread) + n * lag for n, thread in enumerate(threads)))
        for n, thread in enumerate(threads)
        if 0 <= t - n * lag < len(thread)
    ]


def weave(*threads):
    order = sorted(
        ((k + 0.5) / len(thread), n, k) for n, thread in enumerate(threads) for k in range(len(thread))
    )
    for _, n, k in order:
        threads[n][k]()


def pick(low_rows, high_rows, skip, wide):
    rows = wide.shape[0]
    in_low = wide < 128
    low_index = jnp.minimum(wide, 127)
    high_index = jnp.maximum(wide - skip, 0)
    first = lax.broadcasted_iota(jnp.int32, wide.shape, 1) < WIN * WIN

    def of_head(h):
        low = jnp.broadcast_to(low_rows[h] * LOG2E, (rows, 128))
        high = jnp.broadcast_to(high_rows[h] * LOG2E, (rows, 128))
        return jnp.where(
            in_low,
            jnp.take_along_axis(low, low_index, axis=1),
            jnp.take_along_axis(high, high_index, axis=1),
        )

    return jnp.concatenate(
        [jnp.where(first, of_head(h), of_head(h + 1)) for h in range(0, len(low_rows), 2)], axis=1
    )


def split3(value):
    high = value.astype(BF)
    rest = value - high.astype(F32)
    middle = rest.astype(BF)
    return [high, middle, (rest - middle.astype(F32)).astype(BF)]


QKVB, FC1B, TABLE = 0, 3, 5
GAIN, SHIFTS, PROJB, FC2B = 9, 11, 13, 14
SMALL = 16


def pack_kernel(*refs, count):
    hbm, refs = refs[:count], refs[count:]
    (w0_ref, w1_ref, left_ref, right_ref, rel2_ref), refs = refs[:5], refs[5:]
    staged, small_ref, sems = refs[:count], refs[count], refs[count + 1]
    cols = hbm[0].shape[1]
    edge = 2 * WIN
    copies = [
        pltpu.make_async_copy(hbm[0].at[:, 0:edge], staged[0].at[0], sems.at[0]),
        pltpu.make_async_copy(hbm[0].at[:, cols - edge : cols], staged[0].at[1], sems.at[count]),
    ]
    copies += [pltpu.make_async_copy(hbm[k], staged[k], sems.at[k]) for k in range(1, count)]
    for copy in copies:
        copy.start()
    for copy in copies:
        copy.wait()
    (x, labels, rel, gain, shift, qkv, qkvb, table, proj, projb, fc1, fc1b, fc2, fc2b) = staged
    c = x.shape[3]
    part = qkv.shape[2]
    hidden = fc1.shape[2]
    entries = table.shape[2]
    for b, out in enumerate((w0_ref, w1_ref)):
        at = 0
        for m in range(3):
            out[at : at + part, :] = qkv[b, m]
            at += part
        out[at : at + part, :] = proj[b]
        at += part
        for start in range(0, hidden, 128):
            out[at : at + c, :] = fc1[b, :, start : start + 128]
            at += c
        out[at : at + hidden, :] = fc2[b]
        at += hidden
        small_ref[...] = jnp.zeros_like(small_ref)
        for m in range(3):
            small_ref[QKVB + m : QKVB + m + 1, 0:part] = qkvb[m, b : b + 1]
        for k in range(hidden // 128):
            small_ref[FC1B + k : FC1B + k + 1, :] = fc1b[b : b + 1, k * 128 : (k + 1) * 128]
        k = TABLE
        for h in range(table.shape[1]):
            for first in (0, entries - 128):
                small_ref[k : k + 1, :] = table[b, h : h + 1, first : first + 128]
                k += 1
        small_ref[GAIN : GAIN + 2, :] = gain[b]
        small_ref[SHIFTS : SHIFTS + 2, :] = shift[b]
        small_ref[PROJB : PROJB + 1, :] = projb[b : b + 1, :]
        small_ref[FC2B : FC2B + 1, :] = fc2b[b : b + 1, :]
        for piece in split3(small_ref[...]):
            out[at : at + SMALL, :] = piece
            at += SMALL
    ids = (labels[...] + 1).astype(F32).astype(BF)
    for r in range(WIN):
        left_ref[r] = x[0, r, 0:WIN]
        right_ref[r] = x[1, r, WIN:]
    left_ref[WIN] = ids[:, 0:128]
    right_ref[WIN] = ids[:, cols - 128 : cols]
    rel2_ref[...] = jnp.concatenate([rel[...], rel[...]], axis=1)


class Weights:

    def __init__(self, packs, scratch, c, part, hidden):
        self.qkv, self.proj, self.fc1, self.fc2, self.rows = scratch
        self.c = c
        self.packs = packs
        self.part, self.hidden = part, hidden
        self.start_small = 4 * part + (hidden // 128) * c + hidden

    def small(self, row, rows=1, width=128):
        out = []
        for p in self.packs:
            at = self.start_small
            value = sum(
                p[at + k * SMALL : at + (k + 1) * SMALL, :].astype(F32) for k in range(3)
            )
            out.append(value[row : row + rows, :width])
        return out

    def load_rows(self):
        c, part, hidden = self.c, self.part, self.hidden
        vectors = [self.small(GAIN + k)[0] for k in range(2)]
        vectors += [self.small(SHIFTS + k)[0] for k in range(2)]
        vectors += [self.small(PROJB)[0], self.small(FC2B)[0]]
        for k, row in enumerate(vectors):
            self.rows[k : k + 1, 0:c] = row
        self.rows[6:7, 0 : 3 * c] = jnp.concatenate(
            [v for m in range(3) for v in self.small(QKVB + m, width=part)], axis=1
        )
        rows = [self.small(FC1B + k) for k in range(hidden // 128)]
        self.rows[7:8, :] = jnp.concatenate(
            [row[g] for g in range(len(self.packs)) for row in rows], axis=1
        )

    def load_qkv(self):
        c, part = self.c, self.part
        for m in range(3):
            rows = jnp.concatenate([p[m * part : (m + 1) * part, :] for p in self.packs], axis=0)
            self.qkv[:, m * c : (m + 1) * c] = rows.astype(F32).T.astype(BF)

    def load_rest(self):
        c, part, hidden = self.c, self.part, self.hidden
        for g, p in enumerate(self.packs):
            at = 3 * part
            self.proj[g * part : (g + 1) * part, :] = p[at : at + part, :]
            at += part
            for k in range(hidden // 128):
                lane = g * hidden + k * 128
                self.fc1[:, lane : lane + 128] = p[at : at + c, :]
                at += c
            self.fc2[g * hidden : (g + 1) * hidden, :] = p[at : at + hidden, :]

    def row(self, k):
        return self.rows[k : k + 1, 0 : self.c]

    def bias(self, own_heads, skip, wide):
        rows = [self.small(TABLE + k) for k in range(2 * own_heads)]
        low = [rows[2 * h][g] for g in range(len(self.packs)) for h in range(own_heads)]
        high = [rows[2 * h + 1][g] for g in range(len(self.packs)) for h in range(own_heads)]
        return pick(low, high, skip, wide)

    def norm_pieces(self, at, k):
        def mean():
            x = at["x"]
            at["center"] = x - jnp.mean(x, axis=-1, keepdims=True)

        def spread():
            center = at["center"]
            at["spread"] = jnp.mean(center * center, axis=-1, keepdims=True)

        def normed():
            scaled = at["center"] * lax.rsqrt(at["spread"] + EPS)
            at["normed"] = (scaled * self.row(k) + self.row(2 + k)).astype(BF)

        return [mean, spread, normed]

    def project_pieces(self, load, stores, normed_load=None):
        at = {}
        c = self.c

        def begin():
            at["x"] = load()

        def product(m, scale, store):
            def dot():
                at[m] = dot_nn(at["normed"], self.qkv[:, m * c : (m + 1) * c])

            def keep():
                value = at.pop(m) + self.rows[6:7, m * c : (m + 1) * c]
                store((value if scale is None else value * scale).astype(BF))

            return dot, keep

        mean, spread, normed = self.norm_pieces(at, 0)
        made = [product(*entry) for entry in stores]

        def start():
            begin()
            mean()

        rest = [dot for dot, _ in made] + [keep for _, keep in made]
        if normed_load is None:
            return [start, spread, normed], rest

        def read():
            at["normed"] = normed_load()

        return [read] + rest

    def finish_pieces(self, load, attended, store):
        at = {}
        width = 256

        def project():
            at["p"] = dot_nn(attended(), self.proj[...])

        def begin():
            middle = (load() + at.pop("p") + self.row(4)).astype(BF).astype(F32)
            at["x"] = middle
            at["middle"] = middle

        mean, spread, normed = self.norm_pieces(at, 1)

        def start():
            begin()
            mean()

        def up(k):
            def dot():
                at["up", k] = dot_nn(at["normed"], self.fc1[:, k : k + width])

            return dot

        def act(k):
            def gate():
                at["act", k] = gelu(at.pop(("up", k)) + self.rows[7:8, k : k + width]).astype(BF)

            return gate

        def down(k):
            def dot():
                at["down", k] = dot_nn(at.pop(("act", k)), self.fc2[k : k + width, :])

            return dot

        def end():
            total = at["middle"] + self.row(5)
            for k in starts:
                total = total + at["down", k]
            store(total)

        starts = range(0, self.fc2.shape[0], width)
        chains = [[up(k), act(k), down(k)] for k in starts]
        return [project, start, spread, normed], skewed(chains) + [end]


def pipeline(chunks, extra, *makers):
    stages = [[stage for make in makers for stage in make(i)] for i in range(chunks)]
    depth = len(stages[0])
    for t in range(chunks + depth - 1):
        threads = [stages[t - d][d] for d in reversed(range(depth)) if 0 <= t - d < chunks]
        if t == 0:
            threads.append(extra)
        weave(*threads)


def parity():
    return (lax.axis_index("row") * lax.axis_size("ch") + lax.axis_index("ch")) % 2


def edge_ids(left_ref, right_ref, labels):
    lanes = jnp.concatenate(
        [left_ref[WIN].astype(F32), (labels + 1).astype(F32), right_ref[WIN].astype(F32)], axis=1
    )
    span = lanes.shape[1]
    lane = lax.broadcasted_iota(jnp.int32, (WIN, span), 1)
    match = lane % WIN == lax.broadcasted_iota(jnp.int32, (WIN, span), 0)
    spread = jnp.concatenate(
        [jnp.where(match, lanes[r : r + 1], 0.0) for r in range(WIN)], axis=0
    ).astype(BF)
    source = lax.broadcasted_iota(jnp.int32, (span, 128), 0)
    window = lax.broadcasted_iota(jnp.int32, (span, 128), 1)
    chosen = ((source - 128 + SHIFT) // WIN == window) & (source >= 128 - SHIFT)
    return dot_nn(spread, chosen.astype(F32).astype(BF)).reshape(WIN, WIN, 128).astype(BF)


class Rows:

    def __init__(self, weights, x_ref, out_ref, cols):
        self.w, self.x, self.out, self.cols = weights, x_ref, out_ref, cols

    def pieces(self, start, count, attended):
        span = slice(start * WIN, (start + count) * WIN)

        def load():
            block = self.x[:, span, :].astype(F32)
            return jnp.concatenate(
                [block[r, n * WIN : (n + 1) * WIN] for n in range(count) for r in range(SHIFT)], axis=0
            )

        def store(out):
            for r in range(SHIFT):
                rows = [
                    out[(n * SHIFT + r) * WIN : (n * SHIFT + r + 1) * WIN] for n in range(count)
                ]
                if start * WIN < self.cols:
                    self.out[r, span, :] = jnp.concatenate(rows, axis=0).astype(BF)
                else:
                    before = lax.broadcasted_iota(jnp.int32, rows[0].shape, 0) < SHIFT
                    self.out[r, span.start : span.start + WIN, :] = jnp.where(
                        before, rows[1], rows[0]
                    ).astype(BF)

        return self.w.finish_pieces(load, attended, store)


def block0_chunks(cols, size=4):
    wins = cols // WIN
    return [(n, min(size, wins - n)) for n in range(0, wins, size)] + [(wins, 2)]


def put_edges(x_ref, left_ref, right_ref, cols, base=0):
    for r in range(x_ref.shape[0]):
        x_ref[r, cols : cols + 2 * WIN, :] = jnp.concatenate(
            [left_ref[base + r], right_ref[base + r]], axis=0
        )


def norm_kernel(x_hbm, pack_ref, normed_ref, x_ref, rows_ref, sem, *, part, hidden):
    cols = x_hbm.shape[1]
    x_copy = pltpu.make_async_copy(x_hbm, x_ref, sem.at[0])
    x_copy.start()
    w = Weights([pack_ref], (None, None, None, None, rows_ref), x_ref.shape[2], part, hidden)
    for k in range(2):
        rows_ref[k : k + 1, :] = w.small(GAIN + k)[0]
        rows_ref[2 + k : 3 + k, :] = w.small(SHIFTS + k)[0]
    x_copy.wait()
    tokens = WIN * WIN

    def chunk(start, count):
        at = {}

        def begin():
            block = x_ref[:, start * WIN : (start + count) * WIN, :].astype(F32)
            at["x"] = jnp.concatenate(
                [block[r, n * WIN : (n + 1) * WIN] for n in range(count) for r in range(WIN)], axis=0
            )

        def keep():
            normed_ref[start * tokens : (start + count) * tokens] = at["normed"]

        mean, spread, normed = w.norm_pieces(at, 0)
        return [begin, mean, spread, normed, keep]

    wins = cols // WIN
    for piece in offset([chunk(n, min(4, wins - n)) for n in range(0, wins, 4)], 1):
        piece()


def regular_kernel(
    x_hbm, labels_hbm, left_ref, right_ref, rel_ref, normed_ref, *refs,
    groups, own_heads, entries, part, hidden,
):
    packs, refs = refs[:groups], refs[groups:]
    (near_ref, rest_ref, ids_ref, bias_ref, side_ref), refs = refs[:5], refs[5:]
    (labels_ref, sems, qkv_ref, att_ref), scratch = refs[:4], refs[4:]
    side = 1 - parity()
    cols = x_hbm.shape[1]
    labels_copy = pltpu.make_async_copy(labels_hbm, labels_ref, sems.at[0])
    side_copy = pltpu.make_async_copy(
        x_hbm.at[pl.ds(side * SHIFT, SHIFT)], side_ref.at[:, 0:cols], sems.at[1]
    )
    labels_copy.start()
    side_copy.start()
    c = side_ref.shape[2]
    heads = own_heads * groups
    depth = c // heads
    tokens = WIN * WIN
    half = SHIFT * WIN
    scale = depth ** (-0.5) * LOG2E
    w = Weights(packs, scratch, c, part, hidden)
    masks = head_masks(heads, depth, c)
    ones = jnp.concatenate(masks, axis=0)
    w.load_rows()
    w.load_qkv()

    def pick_bias():
        bias_ref[...] = w.bias(own_heads, entries - 128, rel_ref[...])

    def put_ids():
        ids_ref[...] = edge_ids(left_ref, right_ref, labels_ref[...])

    labels_copy.wait()
    side_copy.wait()
    put_edges(side_ref, left_ref, right_ref, cols, side * SHIFT)
    extra = [pick_bias, put_ids, w.load_rest]
    chunks = block0_chunks(cols)
    finish = Rows(w, side_ref, near_ref, cols)

    def first(i):
        start, count = chunks[i]

        def keep(m):
            def store(value):
                qkv_ref[i % 2, m, 0 : count * tokens] = value

            return store

        rows = slice(start * tokens, (start + count) * tokens)
        entries_of = [(0, scale, keep(0)), (1, None, keep(1)), (2, None, keep(2))]
        if start * WIN < cols:
            return [w.project_pieces(None, entries_of, lambda: normed_ref[rows])]

        def edges():
            return jnp.concatenate(
                [e[0:WIN].astype(F32).reshape(tokens, c) for e in (left_ref, right_ref)], axis=0
            )

        norm, rest = w.project_pieces(edges, entries_of)
        return [norm + rest]

    def second(i):
        start, count = chunks[i]

        def window(n):
            rows = slice(n * tokens, (n + 1) * tokens)

            def write(value):
                low, high = value[:half], value[half:]
                att_ref[i % 2, n * half : (n + 1) * half] = jnp.where(side == 0, low, high).astype(BF)
                rest_ref[(start + n) * half : (start + n + 1) * half] = jnp.where(
                    side == 0, high, low
                ).astype(BF)

            return window_pieces(
                lambda: [qkv_ref[i % 2, m, rows] for m in range(3)],
                lambda: bias_ref[...], None, write, masks, ones,
            )

        return [skewed([window(n) for n in range(count)])]

    def third(i):
        start, count = chunks[i]
        return finish.pieces(start, count, lambda: att_ref[i % 2, 0 : count * half])

    pipeline(len(chunks), extra, first, second, third)
    for r in range(SHIFT):
        near_ref[r, cols + WIN :, :] = ids_ref[side * SHIFT + r]


def rest_kernel(x_hbm, left_ref, right_ref, att_ref, ids_ref, *refs, groups, own_heads, entries, part, hidden):
    packs, refs = refs[:groups], refs[groups:]
    (far_ref, x_ref, sems), scratch = refs[:3], refs[3:]
    cols = x_hbm.shape[1]
    side = parity()
    x_copy = pltpu.make_async_copy(
        x_hbm.at[pl.ds(side * SHIFT, SHIFT)], x_ref.at[:, 0:cols], sems.at[0]
    )
    x_copy.start()
    w = Weights(packs, scratch, x_ref.shape[2], part, hidden)
    w.load_rows()
    w.load_rest()
    put_edges(x_ref, left_ref, right_ref, cols, side * SHIFT)
    finish = Rows(w, x_ref, far_ref, cols)
    half = SHIFT * WIN
    for r in range(SHIFT):
        far_ref[r, cols + WIN :, :] = ids_ref[side * SHIFT + r]
    x_copy.wait()
    threads = []
    for start, count in block0_chunks(cols, 8):
        rows = slice(start * half, (start + count) * half)
        threads.append(sum(finish.pieces(start, count, lambda rows=rows: att_ref[rows]), []))
    for piece in offset(threads, 3):
        piece()


def even_split(count, most):
    parts = -(-count // most)
    return [(count * k // parts, count * (k + 1) // parts) for k in range(parts)]


def shifted_kernel(own_in, halo_in, rel_ref, *refs, chunks, near, groups, own_heads, entries, part, hidden):
    packs, refs = refs[:groups], refs[groups:]
    side = 1 - parity() if near else parity()
    copies = []
    if not near:
        done_ref, out_hbm, out_ref, sems = refs[0], refs[1], refs[2], refs[3]
        refs = refs[2:3] + refs[4:]
        copies.append(
            pltpu.make_async_copy(done_ref, out_hbm.at[pl.ds((1 - side) * SHIFT, SHIFT)], sems.at[0])
        )
        copies[0].start()
    (out_ref, bias_ref, own_ref, halo_ref, res_ref), refs = refs[:5], refs[5:]
    (q_ref, kv_ref, att_ref), scratch = refs[:3], refs[3:]
    c = own_in.shape[2]
    cols = out_ref.shape[1]
    heads = own_heads * groups
    depth = c // heads
    half = SHIFT * WIN
    tokens = WIN * WIN
    scale = depth ** (-0.5) * LOG2E
    w = Weights(packs, scratch, c, part, hidden)
    w.load_rows()
    masks = head_masks(heads, depth, c)
    ones = jnp.concatenate(masks, axis=0)

    def pick_bias():
        rel = rel_ref[...]
        rel = jnp.concatenate(
            [
                jnp.concatenate([rel[a + SHIFT : a + WIN], rel[a : a + SHIFT]], axis=0)
                for a in range(0, tokens, WIN)
            ],
            axis=0,
        )
        lane = lax.broadcasted_iota(jnp.int32, rel.shape, 1)
        rel = jnp.where(lane % WIN < SHIFT, pltpu.roll(rel, 128 - SHIFT, 1), pltpu.roll(rel, SHIFT, 1))
        rel = jnp.where(side == 0, pltpu.roll(rel[half:], half, 1), rel[:half])
        bias_ref[...] = w.bias(own_heads, entries - 128, rel)

    parts = []
    for dst, src in ((own_ref, own_in), (halo_ref, halo_in)):
        value = src[...].astype(F32)
        edge = value[:, cols : cols + WIN]
        dst[:, 0:WIN, :] = edge
        dst[:, WIN : WIN + cols, :] = value[:, :cols]
        dst[:, WIN + cols :, :] = edge
        parts.append(value[:, cols + WIN :].reshape(half, 128))
    query_ids = parts[0]
    key_ids = jnp.concatenate(parts + parts, axis=0).T
    earlier = lax.broadcasted_iota(jnp.int32, (WIN, c), 0) < SHIFT

    def gather(ref, i):
        pieces = []
        for j in range(*chunks[i]):
            for r in range(SHIFT):
                before = ref[r, j * WIN : (j + 1) * WIN, :]
                after = ref[r, (j + 1) * WIN : (j + 2) * WIN, :]
                pieces.append(jnp.where(earlier, after, before))
        return jnp.concatenate(pieces, axis=0)

    def first(i):
        slot = i % 2
        count = (chunks[i][1] - chunks[i][0]) * half

        def keep(target):
            def store(value):
                target[0:count] = value

            return store

        own = w.project_pieces(
            lambda: gather(own_ref, i),
            [(0, scale, keep(q_ref.at[slot]))]
            + [(1 + m, None, keep(kv_ref.at[slot, m, 0])) for m in range(2)],
        )
        halo = w.project_pieces(
            lambda: gather(halo_ref, i), [(1 + m, None, keep(kv_ref.at[slot, m, 1])) for m in range(2)]
        )
        return [skewed(list(pair)) for pair in zip(own, halo)]

    def second(i):
        slot = i % 2
        base = chunks[i][0]

        def window(j):
            rows = slice((j - base) * half, (j - base + 1) * half)

            def read():
                k, v = (
                    jnp.concatenate([kv_ref[slot, m, 0, rows], kv_ref[slot, m, 1, rows]], axis=0)
                    for m in range(2)
                )
                return q_ref[slot, rows], k, v

            def allowed():
                same = jnp.broadcast_to(query_ids[:, j : j + 1], (half, 128)) == key_ids[j : j + 1, :]
                return jnp.concatenate([same, same], axis=1)

            def write(value):
                att_ref[slot, rows] = value.astype(BF)

            return window_pieces(read, lambda: bias_ref[...], allowed, write, masks, ones)

        return [skewed([window(j) for j in range(*chunks[i])])]

    def third(i):
        base, stop = chunks[i]

        def store(out):
            for r in range(SHIFT):
                res_ref[r, base * WIN : stop * WIN, :] = jnp.concatenate(
                    [
                        out[n * half + r * WIN : n * half + (r + 1) * WIN]
                        for n in range(stop - base)
                    ],
                    axis=0,
                )
            begin = (base - 1) // 2 * 2 * WIN if i else 0
            end = (stop - 1) // 2 * 2 * WIN if i + 1 < len(chunks) else cols
            low = lax.broadcasted_iota(jnp.int32, (SHIFT, end - begin, c), 1) % WIN < SHIFT
            out_ref[:, begin:end, :] = jnp.where(
                low, res_ref[:, begin:end, :], res_ref[:, begin + WIN : end + WIN, :]
            ).astype(BF)
            if not near:
                copies.append(
                    pltpu.make_async_copy(
                        out_ref.at[:, begin:end],
                        out_hbm.at[pl.ds(side * SHIFT, SHIFT), begin:end],
                        sems.at[1 + i],
                    )
                )
                copies[-1].start()

        return w.finish_pieces(
            lambda: gather(own_ref, i), lambda: att_ref[i % 2, 0 : (stop - base) * half], store
        )

    pipeline(len(chunks), [w.load_qkv, pick_bias, w.load_rest], first, second, third)
    for copy in copies:
        copy.wait()


def call(kernel, out_shapes, scratch, *args, **specs):
    return pl.pallas_call(
        kernel,
        out_shape=out_shapes,
        scratch_shapes=scratch,
        compiler_params=pltpu.CompilerParams(vmem_limit_bytes=48 * 1024 * 1024),
        **specs,
    )(*args)


def in_hbm(value):
    return pltpu.with_memory_space_constraint(value, pltpu.HBM)


def neighbours(axis, by):
    size = lax.axis_size(axis)
    return [(i, i + by) for i in range(size) if 0 <= i + by < size]


def both_blocks(*args):
    image_tokens, labels, _ = args[:3]
    qkv_weight, bias_table, fc1_weight = args[5], args[7], args[10]
    tile_cols, c = image_tokens.shape[1:]
    groups = lax.axis_size("ch")
    swap = [(i, (i + 1) % groups) for i in range(groups)]
    part = qkv_weight.shape[3]
    hidden = fc1_weight.shape[2]
    entries = bias_table.shape[1]
    own_heads = bias_table.shape[2]
    tokens = WIN * WIN

    def others(value):
        found = [value]
        for _ in range(groups - 1):
            found.append(lax.ppermute(found[-1], "ch", swap))
        return found

    rows = 4 * part + (hidden // 128) * c + hidden + 3 * SMALL
    pack = jax.ShapeDtypeStruct((rows, 128), BF)
    edge = jax.ShapeDtypeStruct((WIN + 1, WIN, c), BF)
    args = list(args)
    args[5] = qkv_weight.transpose(0, 1, 3, 2)
    args[6] = args[6].transpose(1, 0, 2)
    args[7] = bias_table.transpose(0, 2, 1)
    staged = [pltpu.VMEM((2, WIN, 2 * WIN, c), BF)] + [pltpu.VMEM(a.shape, a.dtype) for a in args[1:]]
    own0, own1, left_edge, right_edge, rel2 = call(
        lambda *refs: pack_kernel(*refs, count=len(args)),
        (pack, pack, edge, edge, jax.ShapeDtypeStruct((tokens, 2 * tokens), jnp.int32)),
        staged + [pltpu.VMEM((SMALL, 128), F32), pltpu.SemaphoreType.DMA((len(args) + 1,))],
        *(in_hbm(a) for a in args),
        in_specs=[pl.BlockSpec(memory_space=pltpu.HBM)] * len(args),
    )
    packs0 = others(own0)
    left = lax.ppermute(right_edge, "col", neighbours("col", 1))
    right = lax.ppermute(left_edge, "col", neighbours("col", -1))
    packs1 = others(own1)

    sizes = dict(groups=groups, own_heads=own_heads, entries=entries, part=part, hidden=hidden)
    weights_scratch = [
        pltpu.VMEM((c, 3 * c), BF),
        pltpu.VMEM((c, c), BF),
        pltpu.VMEM((c, groups * hidden), BF),
        pltpu.VMEM((groups * hidden, c), BF),
        pltpu.VMEM((8, groups * hidden), F32),
    ]
    strip = jax.ShapeDtypeStruct((SHIFT, tile_cols + 2 * WIN, c), BF)
    bias_scratch = pltpu.VMEM((tokens, own_heads * groups * tokens), F32)
    half_wide = pltpu.VMEM((SHIFT, tile_cols + 2 * WIN, c), BF)
    bands = lax.axis_size(("row", "ch"))

    def swapped(value, first):
        pairs = [(m, m + 1) for m in range(first, bands - 1, 2)]
        return lax.ppermute(value, ("row", "ch"), pairs + [(j, i) for i, j in pairs])

    in_vmem = pl.BlockSpec(memory_space=pltpu.VMEM)
    normed = call(
        lambda *refs: norm_kernel(*refs, part=part, hidden=hidden),
        jax.ShapeDtypeStruct((tokens * (tile_cols // WIN), c), BF),
        [
            pltpu.VMEM(image_tokens.shape, BF), pltpu.VMEM((4, c), F32),
            pltpu.SemaphoreType.DMA((1,)),
        ],
        in_hbm(image_tokens), own0,
        in_specs=[pl.BlockSpec(memory_space=pltpu.HBM), in_vmem],
    )
    near, rest, ids = call(
        lambda *refs: regular_kernel(*refs, **sizes),
        (
            strip,
            jax.ShapeDtypeStruct((SHIFT * (tile_cols + 2 * WIN), c), BF),
            jax.ShapeDtypeStruct((WIN, WIN, 128), BF),
        ),
        [
            bias_scratch, half_wide,
            pltpu.VMEM(labels.shape, jnp.int32), pltpu.SemaphoreType.DMA((2,)),
            pltpu.VMEM((2, 3, 4 * tokens, c), BF), pltpu.VMEM((2, 2 * tokens, c), BF),
        ] + weights_scratch,
        in_hbm(image_tokens), in_hbm(labels), left, right, rel2, normed, *packs0,
        in_specs=[pl.BlockSpec(memory_space=pltpu.HBM)] * 2 + [in_vmem] * (4 + groups),
    )
    near_halo = swapped(near, 0)
    far = call(
        lambda *refs: rest_kernel(*refs, **sizes),
        strip,
        [half_wide, pltpu.SemaphoreType.DMA((1,))] + weights_scratch,
        in_hbm(image_tokens), left, right, rest, ids, *packs0,
        in_specs=[pl.BlockSpec(memory_space=pltpu.HBM)] + [in_vmem] * (4 + groups),
    )
    far_halo = swapped(far, 1)
    chunks = even_split(tile_cols // WIN + 1, 11)
    most = max(stop - base for base, stop in chunks) * SHIFT * WIN
    strip_wide = pltpu.VMEM((SHIFT, tile_cols + 2 * WIN, c), F32)
    scratch = [
        pltpu.VMEM((SHIFT * WIN, own_heads * groups * tokens), F32), strip_wide, strip_wide,
        pltpu.VMEM((SHIFT, tile_cols + WIN, c), F32),
        pltpu.VMEM((2, most, c), BF), pltpu.VMEM((2, 2, 2, most, c), BF), pltpu.VMEM((2, most, c), BF),
    ] + weights_scratch
    near_out = call(
        lambda *refs: shifted_kernel(*refs, chunks=chunks, near=True, **sizes),
        jax.ShapeDtypeStruct((SHIFT, tile_cols, c), BF),
        scratch, near, near_halo, rel2, *packs1,
    )
    return call(
        lambda *refs: shifted_kernel(*refs, chunks=chunks, near=False, **sizes),
        jax.ShapeDtypeStruct(image_tokens.shape, BF),
        [pltpu.VMEM((SHIFT, tile_cols, c), BF), pltpu.SemaphoreType.DMA((1 + len(chunks),))] + scratch,
        far, far_halo, rel2, *packs1, near_out,
        out_specs=pl.BlockSpec(memory_space=pltpu.HBM),
    )


def solution(mesh):
    in_specs = (
        P(("row", "ch"), "col", None),
        P(("row", "ch"), "col"),
        P(),
        P(),
        P(),
        P(None, None, None, "ch"),
        P(None, None, "ch"),
        P(None, None, "ch"),
        P(None, "ch", None),
        P(),
        P(None, None, "ch"),
        P(None, "ch"),
        P(None, "ch", None),
        P(),
    )
    out_specs = P(("row", "ch"), "col", None)
    return jax.shard_map(
        both_blocks, mesh=mesh, in_specs=in_specs, out_specs=out_specs, check_vma=False
    )
```

```python
import math

import jax
import jax.numpy as jnp
from jax import lax
from jax.experimental import pallas as pl
from jax.experimental.pallas import tpu as pltpu
from jax.sharding import PartitionSpec as P


WIN = 8
SHIFT = 4
EPS = 1e-05
NEG = -1e30
LOG2E = math.log2(math.e)
BF = jnp.bfloat16
F32 = jnp.float32


def dot_nt(a, b):
    return lax.dot_general(a, b, (((1,), (1,)), ((), ())), preferred_element_type=F32)


def dot_nn(a, b):
    return lax.dot_general(a, b, (((1,), (0,)), ((), ())), preferred_element_type=F32)


def gelu(v):
    half = 0.5 * v
    return half + half * lax.erf(v * math.sqrt(0.5))


def head_masks(heads, depth, width):
    lane = lax.broadcasted_iota(jnp.int32, (WIN * WIN, width), 1)
    return [(lane // depth == h).astype(F32).astype(BF) for h in range(heads)]


def stack_heads(rows, masks):
    return jnp.concatenate([rows * mask for mask in masks], axis=0)


def window_pieces(read, bias, allowed, write, masks, ones):
    at = {}

    def score():
        q, k, at["v"] = read()
        at["s"] = dot_nt(q, stack_heads(k, masks))

    def reduce():
        scores = at["s"] + bias()
        if allowed is not None:
            scores = jnp.where(allowed(), scores, NEG)
        first = lax.broadcasted_iota(jnp.int32, (scores.shape[0], 128), 1) < WIN * WIN
        parts = []
        for start in range(0, scores.shape[1], 128):
            s = scores[:, start : start + 128]
            low = jnp.max(jnp.where(first, s, NEG), axis=-1, keepdims=True)
            high = jnp.max(jnp.where(first, NEG, s), axis=-1, keepdims=True)
            parts.append((s, jnp.where(first, low, high)))
        at["s"] = parts

    def mix():
        weights = jnp.concatenate([jnp.exp2(s - m).astype(BF) for s, m in at["s"]], axis=1)
        rhs = jnp.concatenate([stack_heads(at["v"], masks), ones], axis=1)
        at["o"] = dot_nn(weights, rhs)

    def store():
        width = at["o"].shape[1] // 2
        write(at["o"][:, :width] / at["o"][:, width:])

    return [score, reduce, mix, store]


def skewed(pipelines):
    depth = max(len(p) for p in pipelines)
    return [
        pipelines[n][t - n]
        for t in range(len(pipelines) + depth - 1)
        for n in range(len(pipelines))
        if 0 <= t - n < len(pipelines[n])
    ]


def offset(threads, lag):
    return [
        thread[t - n * lag]
        for t in range(max(len(thread) + n * lag for n, thread in enumerate(threads)))
        for n, thread in enumerate(threads)
        if 0 <= t - n * lag < len(thread)
    ]


def grouped(pipelines, size):
    groups = [pipelines[n : n + size] for n in range(0, len(pipelines), size)]
    return [
        [lambda k=k, group=group: [p[k]() for p in group] for k in range(len(group[0]))]
        for group in groups
    ]


def weave(*threads):
    order = sorted(
        ((k + 0.5) / len(thread), n, k) for n, thread in enumerate(threads) for k in range(len(thread))
    )
    for _, n, k in order:
        threads[n][k]()


def pick(low_rows, high_rows, skip, wide):
    rows = wide.shape[0]
    in_low = wide < 128
    low_index = jnp.minimum(wide, 127)
    high_index = jnp.maximum(wide - skip, 0)
    first = lax.broadcasted_iota(jnp.int32, wide.shape, 1) < WIN * WIN

    def of_head(h):
        low = jnp.broadcast_to(low_rows[h] * LOG2E, (rows, 128))
        high = jnp.broadcast_to(high_rows[h] * LOG2E, (rows, 128))
        return jnp.where(
            in_low,
            jnp.take_along_axis(low, low_index, axis=1),
            jnp.take_along_axis(high, high_index, axis=1),
        )

    return jnp.concatenate(
        [jnp.where(first, of_head(h), of_head(h + 1)) for h in range(0, len(low_rows), 2)], axis=1
    )


def split3(value):
    high = value.astype(BF)
    rest = value - high.astype(F32)
    middle = rest.astype(BF)
    return [high, middle, (rest - middle.astype(F32)).astype(BF)]


QKVB, FC1B, TABLE = 0, 3, 5
GAIN, SHIFTS, PROJB, FC2B = 9, 11, 13, 14
SMALL = 16


def pack_kernel(*refs, count):
    hbm, refs = refs[:count], refs[count:]
    (w0_ref, w1_ref, left_ref, right_ref, rel2_ref), refs = refs[:5], refs[5:]
    staged, small_ref, sems = refs[:count], refs[count], refs[count + 1]
    cols = hbm[0].shape[1]
    edge = 2 * WIN
    copies = [
        pltpu.make_async_copy(hbm[0].at[:, 0:edge], staged[0].at[0], sems.at[0]),
        pltpu.make_async_copy(hbm[0].at[:, cols - edge : cols], staged[0].at[1], sems.at[count]),
    ]
    copies += [pltpu.make_async_copy(hbm[k], staged[k], sems.at[k]) for k in range(1, count)]
    for copy in copies:
        copy.start()
    for copy in copies:
        copy.wait()
    (x, labels, rel, gain, shift, qkv, qkvb, table, proj, projb, fc1, fc1b, fc2, fc2b) = staged
    c = x.shape[3]
    part = qkv.shape[2]
    hidden = fc1.shape[2]
    entries = table.shape[2]
    for b, out in enumerate((w0_ref, w1_ref)):
        at = 0
        for m in range(3):
            out[at : at + part, :] = qkv[b, m]
            at += part
        out[at : at + part, :] = proj[b]
        at += part
        for start in range(0, hidden, 128):
            out[at : at + c, :] = fc1[b, :, start : start + 128]
            at += c
        out[at : at + hidden, :] = fc2[b]
        at += hidden
        small_ref[...] = jnp.zeros_like(small_ref)
        for m in range(3):
            small_ref[QKVB + m : QKVB + m + 1, 0:part] = qkvb[m, b : b + 1]
        for k in range(hidden // 128):
            small_ref[FC1B + k : FC1B + k + 1, :] = fc1b[b : b + 1, k * 128 : (k + 1) * 128]
        k = TABLE
        for h in range(table.shape[1]):
            for first in (0, entries - 128):
                small_ref[k : k + 1, :] = table[b, h : h + 1, first : first + 128]
                k += 1
        small_ref[GAIN : GAIN + 2, :] = gain[b]
        small_ref[SHIFTS : SHIFTS + 2, :] = shift[b]
        small_ref[PROJB : PROJB + 1, :] = projb[b : b + 1, :]
        small_ref[FC2B : FC2B + 1, :] = fc2b[b : b + 1, :]
        for piece in split3(small_ref[...]):
            out[at : at + SMALL, :] = piece
            at += SMALL
    ids = (labels[...] + 1).astype(F32).astype(BF)
    for r in range(WIN):
        left_ref[r] = x[0, r, 0:WIN]
        right_ref[r] = x[1, r, WIN:]
    left_ref[WIN] = ids[:, 0:128]
    right_ref[WIN] = ids[:, cols - 128 : cols]
    rel2_ref[...] = jnp.concatenate([rel[...], rel[...]], axis=1)


class Weights:

    def __init__(self, packs, scratch, c, part, hidden):
        self.qkv, self.proj, self.fc1, self.fc2, self.rows = scratch
        self.c = c
        self.packs = packs
        self.part, self.hidden = part, hidden
        self.start_small = 4 * part + (hidden // 128) * c + hidden

    def small(self, row, rows=1, width=128):
        out = []
        for p in self.packs:
            at = self.start_small
            value = sum(
                p[at + k * SMALL : at + (k + 1) * SMALL, :].astype(F32) for k in range(3)
            )
            out.append(value[row : row + rows, :width])
        return out

    def load_rows(self):
        c, part, hidden = self.c, self.part, self.hidden
        vectors = [self.small(GAIN + k)[0] for k in range(2)]
        vectors += [self.small(SHIFTS + k)[0] for k in range(2)]
        vectors += [self.small(PROJB)[0], self.small(FC2B)[0]]
        for k, row in enumerate(vectors):
            self.rows[k : k + 1, 0:c] = row
        self.rows[6:7, 0 : 3 * c] = jnp.concatenate(
            [v for m in range(3) for v in self.small(QKVB + m, width=part)], axis=1
        )
        rows = [self.small(FC1B + k) for k in range(hidden // 128)]
        self.rows[7:8, :] = jnp.concatenate(
            [row[g] for g in range(len(self.packs)) for row in rows], axis=1
        )

    def load_qkv(self):
        c, part = self.c, self.part
        for m in range(3):
            rows = jnp.concatenate([p[m * part : (m + 1) * part, :] for p in self.packs], axis=0)
            self.qkv[:, m * c : (m + 1) * c] = rows.astype(F32).T.astype(BF)

    def load_rest(self):
        c, part, hidden = self.c, self.part, self.hidden
        for g, p in enumerate(self.packs):
            at = 3 * part
            self.proj[g * part : (g + 1) * part, :] = p[at : at + part, :]
            at += part
            for k in range(hidden // 128):
                lane = g * hidden + k * 128
                self.fc1[:, lane : lane + 128] = p[at : at + c, :]
                at += c
            self.fc2[g * hidden : (g + 1) * hidden, :] = p[at : at + hidden, :]

    def row(self, k):
        return self.rows[k : k + 1, 0 : self.c]

    def bias(self, own_heads, skip, wide):
        rows = [self.small(TABLE + k) for k in range(2 * own_heads)]
        low = [rows[2 * h][g] for g in range(len(self.packs)) for h in range(own_heads)]
        high = [rows[2 * h + 1][g] for g in range(len(self.packs)) for h in range(own_heads)]
        return pick(low, high, skip, wide)

    def norm_pieces(self, at, k):
        def mean():
            x = at["x"]
            at["center"] = x - jnp.mean(x, axis=-1, keepdims=True)

        def spread():
            center = at["center"]
            at["spread"] = jnp.mean(center * center, axis=-1, keepdims=True)

        def normed():
            scaled = at["center"] * lax.rsqrt(at["spread"] + EPS)
            at["normed"] = (scaled * self.row(k) + self.row(2 + k)).astype(BF)

        return [mean, spread, normed]

    def project_pieces(self, load, stores, normed_load=None):
        at = {}
        c = self.c

        def begin():
            at["x"] = load()

        def product(m, scale, store):
            def dot():
                at[m] = dot_nn(at["normed"], self.qkv[:, m * c : (m + 1) * c])

            def keep():
                value = at.pop(m) + self.rows[6:7, m * c : (m + 1) * c]
                store((value if scale is None else value * scale).astype(BF))

            return dot, keep

        mean, spread, normed = self.norm_pieces(at, 0)
        made = [product(*entry) for entry in stores]

        def start():
            begin()
            mean()

        rest = [dot for dot, _ in made] + [keep for _, keep in made]
        if normed_load is None:
            return [start, spread, normed], rest

        def read():
            at["normed"] = normed_load()

        return [read] + rest

    def finish_pieces(self, load, attended, store):
        at = {}
        width = 256

        def project():
            at["p"] = dot_nn(attended(), self.proj[...])

        def begin():
            middle = (load() + at.pop("p") + self.row(4)).astype(BF).astype(F32)
            at["x"] = middle
            at["middle"] = middle

        mean, spread, normed = self.norm_pieces(at, 1)

        def start():
            begin()
            mean()

        def up(k):
            def dot():
                at["up", k] = dot_nn(at["normed"], self.fc1[:, k : k + width])

            return dot

        def act(k):
            def gate():
                at["act", k] = gelu(at.pop(("up", k)) + self.rows[7:8, k : k + width]).astype(BF)

            return gate

        def down(k):
            def dot():
                at["down", k] = dot_nn(at.pop(("act", k)), self.fc2[k : k + width, :])

            return dot

        def end():
            total = at["middle"] + self.row(5)
            for k in starts:
                total = total + at["down", k]
            store(total)

        starts = range(0, self.fc2.shape[0], width)
        chains = [[up(k), act(k), down(k)] for k in starts]
        return [project, start, spread, normed], skewed(chains) + [end]


def pipeline(chunks, extra, *makers):
    stages = [[stage for make in makers for stage in make(i)] for i in range(chunks)]
    depth = len(stages[0])
    for t in range(chunks + depth - 1):
        threads = [stages[t - d][d] for d in reversed(range(depth)) if 0 <= t - d < chunks]
        threads.append(extra.get(t, []))
        weave(*threads)


def parity():
    return (lax.axis_index("row") * lax.axis_size("ch") + lax.axis_index("ch")) % 2


def edge_ids(left_ref, right_ref, labels):
    lanes = jnp.concatenate(
        [left_ref[WIN].astype(F32), (labels + 1).astype(F32), right_ref[WIN].astype(F32)], axis=1
    )
    span = lanes.shape[1]
    lane = lax.broadcasted_iota(jnp.int32, (WIN, span), 1)
    match = lane % WIN == lax.broadcasted_iota(jnp.int32, (WIN, span), 0)
    spread = jnp.concatenate(
        [jnp.where(match, lanes[r : r + 1], 0.0) for r in range(WIN)], axis=0
    ).astype(BF)
    source = lax.broadcasted_iota(jnp.int32, (span, 128), 0)
    window = lax.broadcasted_iota(jnp.int32, (span, 128), 1)
    chosen = ((source - 128 + SHIFT) // WIN == window) & (source >= 128 - SHIFT)
    return dot_nn(spread, chosen.astype(F32).astype(BF)).reshape(WIN, WIN, 128).astype(BF)


class Rows:

    def __init__(self, weights, x_ref, out_ref, cols):
        self.w, self.x, self.out, self.cols = weights, x_ref, out_ref, cols

    def pieces(self, start, count, attended):
        span = slice(start * WIN, (start + count) * WIN)

        def load():
            block = self.x[:, span, :].astype(F32)
            return jnp.concatenate(
                [block[r, n * WIN : (n + 1) * WIN] for n in range(count) for r in range(SHIFT)], axis=0
            )

        def store(out):
            for r in range(SHIFT):
                rows = [
                    out[(n * SHIFT + r) * WIN : (n * SHIFT + r + 1) * WIN] for n in range(count)
                ]
                if start * WIN < self.cols:
                    self.out[r, span, :] = jnp.concatenate(rows, axis=0).astype(BF)
                else:
                    before = lax.broadcasted_iota(jnp.int32, rows[0].shape, 0) < SHIFT
                    self.out[r, span.start : span.start + WIN, :] = jnp.where(
                        before, rows[1], rows[0]
                    ).astype(BF)

        return self.w.finish_pieces(load, attended, store)


def block0_chunks(cols, size=16):
    wins = cols // WIN
    return [(n, min(size, wins - n)) for n in range(0, wins, size)] + [(wins, 2)]


def put_edges(x_ref, left_ref, right_ref, cols, base=0):
    for r in range(x_ref.shape[0]):
        x_ref[r, cols : cols + 2 * WIN, :] = jnp.concatenate(
            [left_ref[base + r], right_ref[base + r]], axis=0
        )


def norm_kernel(x_hbm, pack_ref, normed_ref, x_ref, rows_ref, sem, *, part, hidden):
    cols = x_hbm.shape[1]
    x_copy = pltpu.make_async_copy(x_hbm, x_ref, sem.at[0])
    x_copy.start()
    w = Weights([pack_ref], (None, None, None, None, rows_ref), x_ref.shape[2], part, hidden)
    for k in range(2):
        rows_ref[k : k + 1, :] = w.small(GAIN + k)[0]
        rows_ref[2 + k : 3 + k, :] = w.small(SHIFTS + k)[0]
    x_copy.wait()
    tokens = WIN * WIN

    def chunk(start, count):
        at = {}

        def begin():
            block = x_ref[:, start * WIN : (start + count) * WIN, :].astype(F32)
            at["x"] = jnp.concatenate(
                [block[r, n * WIN : (n + 1) * WIN] for n in range(count) for r in range(WIN)], axis=0
            )

        def keep():
            normed_ref[start * tokens : (start + count) * tokens] = at["normed"]

        mean, spread, normed = w.norm_pieces(at, 0)
        return [begin, mean, spread, normed, keep]

    wins = cols // WIN
    for piece in offset([chunk(n, min(4, wins - n)) for n in range(0, wins, 4)], 1):
        piece()


def regular_kernel(
    x_hbm, labels_hbm, left_ref, right_ref, rel_ref, normed_ref, *refs,
    groups, own_heads, entries, part, hidden,
):
    packs, refs = refs[:groups], refs[groups:]
    (near_ref, rest_ref, ids_ref, bias_ref, side_ref), refs = refs[:5], refs[5:]
    (labels_ref, sems, qkv_ref, att_ref), scratch = refs[:4], refs[4:]
    side = 1 - parity()
    cols = x_hbm.shape[1]
    labels_copy = pltpu.make_async_copy(labels_hbm, labels_ref, sems.at[0])
    side_copy = pltpu.make_async_copy(
        x_hbm.at[pl.ds(side * SHIFT, SHIFT)], side_ref.at[:, 0:cols], sems.at[1]
    )
    labels_copy.start()
    side_copy.start()
    c = side_ref.shape[2]
    heads = own_heads * groups
    depth = c // heads
    tokens = WIN * WIN
    half = SHIFT * WIN
    scale = depth ** (-0.5) * LOG2E
    w = Weights(packs, scratch, c, part, hidden)
    masks = head_masks(heads, depth, c)
    ones = jnp.concatenate(masks, axis=0)
    w.load_rows()
    w.load_qkv()

    def pick_bias():
        bias_ref[...] = w.bias(own_heads, entries - 128, rel_ref[...])

    def put_ids():
        ids_ref[...] = edge_ids(left_ref, right_ref, labels_ref[...])

    labels_copy.wait()
    side_copy.wait()
    put_edges(side_ref, left_ref, right_ref, cols, side * SHIFT)
    extra = [pick_bias, put_ids, w.load_rest]
    chunks = block0_chunks(cols)
    finish = Rows(w, side_ref, near_ref, cols)

    def first(i):
        start, count = chunks[i]

        def keep(m):
            def store(value):
                qkv_ref[i % 2, m, 0 : count * tokens] = value

            return store

        rows = slice(start * tokens, (start + count) * tokens)
        entries_of = [(0, scale, keep(0)), (1, None, keep(1)), (2, None, keep(2))]
        if start * WIN < cols:
            return [w.project_pieces(None, entries_of, lambda: normed_ref[rows])]

        def edges():
            return jnp.concatenate(
                [e[0:WIN].astype(F32).reshape(tokens, c) for e in (left_ref, right_ref)], axis=0
            )

        norm, rest = w.project_pieces(edges, entries_of)
        return [norm + rest]

    def second(i):
        start, count = chunks[i]

        def window(n):
            rows = slice(n * tokens, (n + 1) * tokens)

            def write(value):
                low, high = value[:half], value[half:]
                att_ref[i % 2, n * half : (n + 1) * half] = jnp.where(side == 0, low, high).astype(BF)
                rest_ref[(start + n) * half : (start + n + 1) * half] = jnp.where(
                    side == 0, high, low
                ).astype(BF)

            return window_pieces(
                lambda: [qkv_ref[i % 2, m, rows] for m in range(3)],
                lambda: bias_ref[...], None, write, masks, ones,
            )

        return [skewed(grouped([window(n) for n in range(count)], 99))]

    def third(i):
        start, count = chunks[i]
        return finish.pieces(start, count, lambda: att_ref[i % 2, 0 : count * half])

    pipeline(len(chunks), {0: extra}, first, second, third)
    for r in range(SHIFT):
        near_ref[r, cols + WIN :, :] = ids_ref[side * SHIFT + r]


def rest_kernel(
    x_hbm, left_ref, right_ref, att_ref, ids_ref, near_ref, *refs,
    chunks, groups, own_heads, entries, part, hidden,
):
    packs, next_packs, refs = refs[:groups], refs[groups : 2 * groups], refs[2 * groups :]
    (far_ref, qkv_ref, x_ref, strip_ref, next_qkv, next_rows, sems), scratch = refs[:7], refs[7:]
    cols = x_hbm.shape[1]
    side = parity()
    x_copy = pltpu.make_async_copy(
        x_hbm.at[pl.ds(side * SHIFT, SHIFT)], x_ref.at[:, 0:cols], sems.at[0]
    )
    x_copy.start()
    w = Weights(packs, scratch, x_ref.shape[2], part, hidden)
    w.load_rows()
    w.load_rest()
    put_edges(x_ref, left_ref, right_ref, cols, side * SHIFT)
    finish = Rows(w, x_ref, far_ref, cols)
    half = SHIFT * WIN
    for r in range(SHIFT):
        far_ref[r, cols + WIN :, :] = ids_ref[side * SHIFT + r]
    x_copy.wait()
    threads = []
    for start, count in block0_chunks(cols, 8):
        rows = slice(start * half, (start + count) * half)
        threads.append(sum(finish.pieces(start, count, lambda rows=rows: att_ref[rows]), []))
    c = x_ref.shape[2]
    scale = (c // (own_heads * groups)) ** (-0.5) * LOG2E
    following = Weights(next_packs, (next_qkv, None, None, None, next_rows), c, part, hidden)
    following.load_rows()
    following.load_qkv()
    spread_message(near_ref, strip_ref)
    owns = [own_pieces(following, strip_ref, qkv_ref, span, scale) for span in chunks]
    weave(offset(threads, 3), offset(owns, 5))


def even_split(count, most):
    parts = -(-count // most)
    return [(count * k // parts, count * (k + 1) // parts) for k in range(parts)]


def spread_message(src, dst):
    cols = src.shape[1] - 2 * WIN
    value = src[...].astype(F32)
    edge = value[:, cols : cols + WIN]
    dst[:, 0:WIN, :] = edge
    dst[:, WIN : WIN + cols, :] = value[:, :cols]
    dst[:, WIN + cols :, :] = edge
    return value[:, cols + WIN :].reshape(SHIFT * WIN, 128)


def gather(ref, span):
    earlier = lax.broadcasted_iota(jnp.int32, (WIN, ref.shape[2]), 0) < SHIFT
    pieces = []
    for j in range(*span):
        for r in range(SHIFT):
            before = ref[r, j * WIN : (j + 1) * WIN, :]
            after = ref[r, (j + 1) * WIN : (j + 2) * WIN, :]
            pieces.append(jnp.where(earlier, after, before))
    return jnp.concatenate(pieces, axis=0)


def own_pieces(w, strip, qkv, span, scale):
    rows = slice(span[0] * SHIFT * WIN, span[1] * SHIFT * WIN)

    def keep(m):
        def store(value):
            qkv[m, rows] = value

        return store

    norm, rest = w.project_pieces(
        lambda: gather(strip, span), [(m, None if m else scale, keep(m)) for m in range(3)]
    )
    return norm + rest


def shifted_kernel(
    own_in, halo_in, qkv_in, rel_ref, *refs, chunks, near, groups, own_heads, entries, part, hidden
):
    packs, refs = refs[:groups], refs[groups:]
    side = 1 - parity() if near else parity()
    copies = []
    if near:
        next_in, out_ref, next_qkv, next_ref = refs[:4]
        refs = refs[4:]
    else:
        done_ref, out_hbm, out_ref, sems = refs[:4]
        refs = refs[4:]
        copies.append(
            pltpu.make_async_copy(done_ref, out_hbm.at[pl.ds((1 - side) * SHIFT, SHIFT)], sems.at[0])
        )
        copies[0].start()
    (bias_ref, own_ref, halo_ref, res_ref), refs = refs[:4], refs[4:]
    (kv_ref, att_ref), scratch = refs[:2], refs[2:]
    c = own_in.shape[2]
    cols = out_ref.shape[1]
    heads = own_heads * groups
    depth = c // heads
    half = SHIFT * WIN
    tokens = WIN * WIN
    scale = depth ** (-0.5) * LOG2E
    w = Weights(packs, scratch, c, part, hidden)
    w.load_rows()
    masks = head_masks(heads, depth, c)
    ones = jnp.concatenate(masks, axis=0)

    def pick_bias():
        rel = rel_ref[...]
        rel = jnp.concatenate(
            [
                jnp.concatenate([rel[a + SHIFT : a + WIN], rel[a : a + SHIFT]], axis=0)
                for a in range(0, tokens, WIN)
            ],
            axis=0,
        )
        lane = lax.broadcasted_iota(jnp.int32, rel.shape, 1)
        rel = jnp.where(lane % WIN < SHIFT, pltpu.roll(rel, 128 - SHIFT, 1), pltpu.roll(rel, SHIFT, 1))
        rel = jnp.where(side == 0, pltpu.roll(rel[half:], half, 1), rel[:half])
        bias_ref[...] = w.bias(own_heads, entries - 128, rel)

    halo_ids = spread_message(halo_in, halo_ref)
    query_ids = spread_message(own_in, own_ref)
    key_ids = jnp.concatenate([query_ids, halo_ids] * 2, axis=0).T

    def first(i):
        slot = i % 2
        count = (chunks[i][1] - chunks[i][0]) * half

        def keep(target):
            def store(value):
                target[0:count] = value

            return store

        norm, rest = w.project_pieces(
            lambda: gather(halo_ref, chunks[i]),
            [(1 + m, None, keep(kv_ref.at[slot, m])) for m in range(2)],
        )
        return [norm, rest]

    def second(i):
        slot = i % 2
        base = chunks[i][0]

        def window(j):
            rows = slice((j - base) * half, (j - base + 1) * half)
            own = slice(j * half, (j + 1) * half)

            def read():
                k, v = (
                    jnp.concatenate([qkv_in[1 + m, own], kv_ref[slot, m, rows]], axis=0)
                    for m in range(2)
                )
                return qkv_in[0, own], k, v

            def allowed():
                same = jnp.broadcast_to(query_ids[:, j : j + 1], (half, 128)) == key_ids[j : j + 1, :]
                return jnp.concatenate([same, same], axis=1)

            def write(value):
                att_ref[slot, rows] = value.astype(BF)

            return window_pieces(read, lambda: bias_ref[...], allowed, write, masks, ones)

        return [skewed(grouped([window(j) for j in range(*chunks[i])], 99))]

    def third(i):
        base, stop = chunks[i]

        def store(out):
            for r in range(SHIFT):
                res_ref[r, base * WIN : stop * WIN, :] = jnp.concatenate(
                    [
                        out[n * half + r * WIN : n * half + (r + 1) * WIN]
                        for n in range(stop - base)
                    ],
                    axis=0,
                )
            begin = (base - 1) // 2 * 2 * WIN if i else 0
            end = (stop - 1) // 2 * 2 * WIN if i + 1 < len(chunks) else cols
            low = lax.broadcasted_iota(jnp.int32, (SHIFT, end - begin, c), 1) % WIN < SHIFT
            out_ref[:, begin:end, :] = jnp.where(
                low, res_ref[:, begin:end, :], res_ref[:, begin + WIN : end + WIN, :]
            ).astype(BF)
            if not near:
                copies.append(
                    pltpu.make_async_copy(
                        out_ref.at[:, begin:end],
                        out_hbm.at[pl.ds(side * SHIFT, SHIFT), begin:end],
                        sems.at[1 + i],
                    )
                )
                copies[-1].start()

        return w.finish_pieces(
            lambda: gather(own_ref, chunks[i]), lambda: att_ref[i % 2, 0 : (stop - base) * half], store
        )

    extra = {0: [w.load_qkv, pick_bias, w.load_rest]}
    if near:
        spread_message(next_in, next_ref)
        last = len(chunks) + 4
        for n, span in enumerate(chunks):
            extra[last - len(chunks) + n] = own_pieces(w, next_ref, next_qkv, span, scale)
    pipeline(len(chunks), extra, first, second, third)
    for copy in copies:
        copy.wait()


def call(kernel, out_shapes, scratch, *args, **specs):
    return pl.pallas_call(
        kernel,
        out_shape=out_shapes,
        scratch_shapes=scratch,
        compiler_params=pltpu.CompilerParams(vmem_limit_bytes=48 * 1024 * 1024),
        **specs,
    )(*args)


def in_hbm(value):
    return pltpu.with_memory_space_constraint(value, pltpu.HBM)


def neighbours(axis, by):
    size = lax.axis_size(axis)
    return [(i, i + by) for i in range(size) if 0 <= i + by < size]


def both_blocks(*args):
    image_tokens, labels, _ = args[:3]
    qkv_weight, bias_table, fc1_weight = args[5], args[7], args[10]
    tile_cols, c = image_tokens.shape[1:]
    groups = lax.axis_size("ch")
    swap = [(i, (i + 1) % groups) for i in range(groups)]
    part = qkv_weight.shape[3]
    hidden = fc1_weight.shape[2]
    entries = bias_table.shape[1]
    own_heads = bias_table.shape[2]
    tokens = WIN * WIN

    def others(value):
        found = [value]
        for _ in range(groups - 1):
            found.append(lax.ppermute(found[-1], "ch", swap))
        return found

    rows = 4 * part + (hidden // 128) * c + hidden + 3 * SMALL
    pack = jax.ShapeDtypeStruct((rows, 128), BF)
    edge = jax.ShapeDtypeStruct((WIN + 1, WIN, c), BF)
    args = list(args)
    args[5] = qkv_weight.transpose(0, 1, 3, 2)
    args[6] = args[6].transpose(1, 0, 2)
    args[7] = bias_table.transpose(0, 2, 1)
    staged = [pltpu.VMEM((2, WIN, 2 * WIN, c), BF)] + [pltpu.VMEM(a.shape, a.dtype) for a in args[1:]]
    own0, own1, left_edge, right_edge, rel2 = call(
        lambda *refs: pack_kernel(*refs, count=len(args)),
        (pack, pack, edge, edge, jax.ShapeDtypeStruct((tokens, 2 * tokens), jnp.int32)),
        staged + [pltpu.VMEM((SMALL, 128), F32), pltpu.SemaphoreType.DMA((len(args) + 1,))],
        *(in_hbm(a) for a in args),
        in_specs=[pl.BlockSpec(memory_space=pltpu.HBM)] * len(args),
    )
    packs0 = others(own0)
    left = lax.ppermute(right_edge, "col", neighbours("col", 1))
    right = lax.ppermute(left_edge, "col", neighbours("col", -1))
    packs1 = others(own1)

    sizes = dict(groups=groups, own_heads=own_heads, entries=entries, part=part, hidden=hidden)
    weights_scratch = [
        pltpu.VMEM((c, 3 * c), BF),
        pltpu.VMEM((c, c), BF),
        pltpu.VMEM((c, groups * hidden), BF),
        pltpu.VMEM((groups * hidden, c), BF),
        pltpu.VMEM((8, groups * hidden), F32),
    ]
    strip = jax.ShapeDtypeStruct((SHIFT, tile_cols + 2 * WIN, c), BF)
    bias_scratch = pltpu.VMEM((tokens, own_heads * groups * tokens), F32)
    half_wide = pltpu.VMEM((SHIFT, tile_cols + 2 * WIN, c), BF)
    bands = lax.axis_size(("row", "ch"))

    def swapped(value, first):
        pairs = [(m, m + 1) for m in range(first, bands - 1, 2)]
        return lax.ppermute(value, ("row", "ch"), pairs + [(j, i) for i, j in pairs])

    in_vmem = pl.BlockSpec(memory_space=pltpu.VMEM)
    normed = call(
        lambda *refs: norm_kernel(*refs, part=part, hidden=hidden),
        jax.ShapeDtypeStruct((tokens * (tile_cols // WIN), c), BF),
        [
            pltpu.VMEM(image_tokens.shape, BF), pltpu.VMEM((4, c), F32),
            pltpu.SemaphoreType.DMA((1,)),
        ],
        in_hbm(image_tokens), own0,
        in_specs=[pl.BlockSpec(memory_space=pltpu.HBM), in_vmem],
    )
    near, rest, ids = call(
        lambda *refs: regular_kernel(*refs, **sizes),
        (
            strip,
            jax.ShapeDtypeStruct((SHIFT * (tile_cols + 2 * WIN), c), BF),
            jax.ShapeDtypeStruct((WIN, WIN, 128), BF),
        ),
        [
            bias_scratch, half_wide,
            pltpu.VMEM(labels.shape, jnp.int32), pltpu.SemaphoreType.DMA((2,)),
            pltpu.VMEM((2, 3, 16 * tokens, c), BF), pltpu.VMEM((2, 8 * tokens, c), BF),
        ] + weights_scratch,
        in_hbm(image_tokens), in_hbm(labels), left, right, rel2, normed, *packs0,
        in_specs=[pl.BlockSpec(memory_space=pltpu.HBM)] * 2 + [in_vmem] * (4 + groups),
    )
    near_halo = swapped(near, 0)
    chunks = even_split(tile_cols // WIN + 1, 17)
    own_qkv = jax.ShapeDtypeStruct((3, (tile_cols // WIN + 1) * SHIFT * WIN, c), BF)
    strip_wide = pltpu.VMEM((SHIFT, tile_cols + 2 * WIN, c), F32)
    far, near_qkv = call(
        lambda *refs: rest_kernel(*refs, chunks=chunks, **sizes),
        (strip, own_qkv),
        [
            half_wide, strip_wide, weights_scratch[0], weights_scratch[-1],
            pltpu.SemaphoreType.DMA((1,)),
        ] + weights_scratch,
        in_hbm(image_tokens), left, right, rest, ids, near, *packs0, *packs1,
        in_specs=[pl.BlockSpec(memory_space=pltpu.HBM)] + [in_vmem] * (5 + 2 * groups),
    )
    far_halo = swapped(far, 1)
    most = max(stop - base for base, stop in chunks) * SHIFT * WIN
    scratch = [
        pltpu.VMEM((SHIFT * WIN, own_heads * groups * tokens), F32), strip_wide, strip_wide,
        pltpu.VMEM((SHIFT, tile_cols + WIN, c), F32),
        pltpu.VMEM((2, 2, most, c), BF), pltpu.VMEM((2, most, c), BF),
    ] + weights_scratch
    near_out, far_qkv = call(
        lambda *refs: shifted_kernel(*refs, chunks=chunks, near=True, **sizes),
        (jax.ShapeDtypeStruct((SHIFT, tile_cols, c), BF), own_qkv),
        [strip_wide] + scratch,
        near, near_halo, near_qkv, rel2, *packs1, far,
    )
    return call(
        lambda *refs: shifted_kernel(*refs, chunks=chunks, near=False, **sizes),
        jax.ShapeDtypeStruct(image_tokens.shape, BF),
        [pltpu.VMEM((SHIFT, tile_cols, c), BF), pltpu.SemaphoreType.DMA((1 + len(chunks),))] + scratch,
        far, far_halo, far_qkv, rel2, *packs1, near_out,
        out_specs=pl.BlockSpec(memory_space=pltpu.HBM),
    )


def solution(mesh):
    in_specs = (
        P(("row", "ch"), "col", None),
        P(("row", "ch"), "col"),
        P(),
        P(),
        P(),
        P(None, None, None, "ch"),
        P(None, None, "ch"),
        P(None, None, "ch"),
        P(None, "ch", None),
        P(),
        P(None, None, "ch"),
        P(None, "ch"),
        P(None, "ch", None),
        P(),
    )
    out_specs = P(("row", "ch"), "col", None)
    return jax.shard_map(
        both_blocks, mesh=mesh, in_specs=in_specs, out_specs=out_specs, check_vma=False
    )
```

```python
import math

import jax
import jax.numpy as jnp
from jax import lax
from jax.experimental import pallas as pl
from jax.experimental.pallas import tpu as pltpu
from jax.sharding import PartitionSpec as P


WIN = 8
SHIFT = 4
EPS = 1e-05
NEG = -1e30
LOG2E = math.log2(math.e)
BF = jnp.bfloat16
F32 = jnp.float32


def dot_nt(a, b):
    return lax.dot_general(a, b, (((1,), (1,)), ((), ())), preferred_element_type=F32)


def dot_nn(a, b):
    return lax.dot_general(a, b, (((1,), (0,)), ((), ())), preferred_element_type=F32)


def gelu(v):
    half = 0.5 * v
    return half + half * lax.erf(v * math.sqrt(0.5))


def head_masks(heads, depth, width):
    lane = lax.broadcasted_iota(jnp.int32, (WIN * WIN, width), 1)
    return [(lane // depth == h).astype(F32).astype(BF) for h in range(heads)]


def stack_heads(rows, masks):
    return jnp.concatenate([rows * mask for mask in masks], axis=0)


def window_pieces(read, bias, allowed, write, masks, ones):
    at = {}

    def score():
        q, k, at["v"] = read()
        at["s"] = dot_nt(q, stack_heads(k, masks))

    def reduce():
        scores = at["s"] + bias()
        if allowed is not None:
            scores = jnp.where(allowed(), scores, NEG)
        first = lax.broadcasted_iota(jnp.int32, (scores.shape[0], 128), 1) < WIN * WIN
        parts = []
        for start in range(0, scores.shape[1], 128):
            s = scores[:, start : start + 128]
            low = jnp.max(jnp.where(first, s, NEG), axis=-1, keepdims=True)
            high = jnp.max(jnp.where(first, NEG, s), axis=-1, keepdims=True)
            parts.append((s, jnp.where(first, low, high)))
        at["s"] = parts

    def mix():
        weights = jnp.concatenate([jnp.exp2(s - m).astype(BF) for s, m in at["s"]], axis=1)
        rhs = jnp.concatenate([stack_heads(at["v"], masks), ones], axis=1)
        at["o"] = dot_nn(weights, rhs)

    def store():
        width = at["o"].shape[1] // 2
        write(at["o"][:, :width] / at["o"][:, width:])

    return [score, reduce, mix, store]


def skewed(pipelines):
    depth = max(len(p) for p in pipelines)
    return [
        pipelines[n][t - n]
        for t in range(len(pipelines) + depth - 1)
        for n in range(len(pipelines))
        if 0 <= t - n < len(pipelines[n])
    ]


def offset(threads, lag):
    return [
        thread[t - n * lag]
        for t in range(max(len(thread) + n * lag for n, thread in enumerate(threads)))
        for n, thread in enumerate(threads)
        if 0 <= t - n * lag < len(thread)
    ]


def grouped(pipelines, size):
    groups = [pipelines[n : n + size] for n in range(0, len(pipelines), size)]
    return [
        [lambda k=k, group=group: [p[k]() for p in group] for k in range(len(group[0]))]
        for group in groups
    ]


def weave(*threads):
    order = sorted(
        ((k + 0.5) / len(thread), n, k) for n, thread in enumerate(threads) for k in range(len(thread))
    )
    for _, n, k in order:
        threads[n][k]()


def pick(low_rows, high_rows, skip, wide):
    rows = wide.shape[0]
    in_low = wide < 128
    low_index = jnp.minimum(wide, 127)
    high_index = jnp.maximum(wide - skip, 0)
    first = lax.broadcasted_iota(jnp.int32, wide.shape, 1) < WIN * WIN

    def of_head(h):
        low = jnp.broadcast_to(low_rows[h] * LOG2E, (rows, 128))
        high = jnp.broadcast_to(high_rows[h] * LOG2E, (rows, 128))
        return jnp.where(
            in_low,
            jnp.take_along_axis(low, low_index, axis=1),
            jnp.take_along_axis(high, high_index, axis=1),
        )

    return jnp.concatenate(
        [jnp.where(first, of_head(h), of_head(h + 1)) for h in range(0, len(low_rows), 2)], axis=1
    )


def split3(value):
    high = value.astype(BF)
    rest = value - high.astype(F32)
    middle = rest.astype(BF)
    return [high, middle, (rest - middle.astype(F32)).astype(BF)]


QKVB, FC1B, TABLE = 0, 3, 5
GAIN, SHIFTS, PROJB, FC2B = 9, 11, 13, 14
SMALL = 16


def pack_kernel(*refs, count):
    hbm, refs = refs[:count], refs[count:]
    (w0_ref, w1_ref, left_ref, right_ref, rel2_ref), refs = refs[:5], refs[5:]
    staged, small_ref, sems = refs[:count], refs[count], refs[count + 1]
    cols = hbm[0].shape[1]
    edge = 2 * WIN
    copies = [
        pltpu.make_async_copy(hbm[0].at[:, 0:edge], staged[0].at[0], sems.at[0]),
        pltpu.make_async_copy(hbm[0].at[:, cols - edge : cols], staged[0].at[1], sems.at[count]),
    ]
    copies += [pltpu.make_async_copy(hbm[k], staged[k], sems.at[k]) for k in range(1, count)]
    for copy in copies:
        copy.start()
    for copy in copies:
        copy.wait()
    (x, labels, rel, gain, shift, qkv, qkvb, table, proj, projb, fc1, fc1b, fc2, fc2b) = staged
    c = x.shape[3]
    part = qkv.shape[2]
    hidden = fc1.shape[2]
    entries = table.shape[2]
    for b, out in enumerate((w0_ref, w1_ref)):
        at = 0
        for m in range(3):
            out[at : at + part, :] = qkv[b, m]
            at += part
        out[at : at + part, :] = proj[b]
        at += part
        for start in range(0, hidden, 128):
            out[at : at + c, :] = fc1[b, :, start : start + 128]
            at += c
        out[at : at + hidden, :] = fc2[b]
        at += hidden
        small_ref[...] = jnp.zeros_like(small_ref)
        for m in range(3):
            small_ref[QKVB + m : QKVB + m + 1, 0:part] = qkvb[m, b : b + 1]
        for k in range(hidden // 128):
            small_ref[FC1B + k : FC1B + k + 1, :] = fc1b[b : b + 1, k * 128 : (k + 1) * 128]
        k = TABLE
        for h in range(table.shape[1]):
            for first in (0, entries - 128):
                small_ref[k : k + 1, :] = table[b, h : h + 1, first : first + 128]
                k += 1
        small_ref[GAIN : GAIN + 2, :] = gain[b]
        small_ref[SHIFTS : SHIFTS + 2, :] = shift[b]
        small_ref[PROJB : PROJB + 1, :] = projb[b : b + 1, :]
        small_ref[FC2B : FC2B + 1, :] = fc2b[b : b + 1, :]
        for piece in split3(small_ref[...]):
            out[at : at + SMALL, :] = piece
            at += SMALL
    ids = (labels[...] + 1).astype(F32).astype(BF)
    for r in range(WIN):
        left_ref[r] = x[0, r, 0:WIN]
        right_ref[r] = x[1, r, WIN:]
    left_ref[WIN] = ids[:, 0:128]
    right_ref[WIN] = ids[:, cols - 128 : cols]
    rel2_ref[...] = jnp.concatenate([rel[...], rel[...]], axis=1)


class Weights:

    def __init__(self, packs, scratch, c, part, hidden):
        self.qkv, self.proj, self.fc1, self.fc2, self.rows = scratch
        self.c = c
        self.packs = packs
        self.part, self.hidden = part, hidden
        self.start_small = 4 * part + (hidden // 128) * c + hidden

    def small(self, row, rows=1, width=128):
        out = []
        for p in self.packs:
            at = self.start_small
            value = sum(
                p[at + k * SMALL : at + (k + 1) * SMALL, :].astype(F32) for k in range(3)
            )
            out.append(value[row : row + rows, :width])
        return out

    def load_rows(self):
        c, part, hidden = self.c, self.part, self.hidden
        vectors = [self.small(GAIN + k)[0] for k in range(2)]
        vectors += [self.small(SHIFTS + k)[0] for k in range(2)]
        vectors += [self.small(PROJB)[0], self.small(FC2B)[0]]
        for k, row in enumerate(vectors):
            self.rows[k : k + 1, 0:c] = row
        self.rows[6:7, 0 : 3 * c] = jnp.concatenate(
            [v for m in range(3) for v in self.small(QKVB + m, width=part)], axis=1
        )
        rows = [self.small(FC1B + k) for k in range(hidden // 128)]
        self.rows[7:8, :] = jnp.concatenate(
            [row[g] for g in range(len(self.packs)) for row in rows], axis=1
        )

    def load_qkv(self):
        c, part = self.c, self.part
        for m in range(3):
            rows = jnp.concatenate([p[m * part : (m + 1) * part, :] for p in self.packs], axis=0)
            self.qkv[:, m * c : (m + 1) * c] = rows.astype(F32).T.astype(BF)

    def load_rest(self):
        c, part, hidden = self.c, self.part, self.hidden
        for g, p in enumerate(self.packs):
            at = 3 * part
            self.proj[g * part : (g + 1) * part, :] = p[at : at + part, :]
            at += part
            for k in range(hidden // 128):
                lane = g * hidden + k * 128
                self.fc1[:, lane : lane + 128] = p[at : at + c, :]
                at += c
            self.fc2[g * hidden : (g + 1) * hidden, :] = p[at : at + hidden, :]

    def row(self, k):
        return self.rows[k : k + 1, 0 : self.c]

    def bias(self, own_heads, skip, wide):
        rows = [self.small(TABLE + k) for k in range(2 * own_heads)]
        low = [rows[2 * h][g] for g in range(len(self.packs)) for h in range(own_heads)]
        high = [rows[2 * h + 1][g] for g in range(len(self.packs)) for h in range(own_heads)]
        return pick(low, high, skip, wide)

    def norm_pieces(self, at, k):
        def mean():
            x = at["x"]
            at["center"] = x - jnp.mean(x, axis=-1, keepdims=True)

        def spread():
            center = at["center"]
            at["spread"] = jnp.mean(center * center, axis=-1, keepdims=True)

        def normed():
            scaled = at["center"] * lax.rsqrt(at["spread"] + EPS)
            at["normed"] = (scaled * self.row(k) + self.row(2 + k)).astype(BF)

        return [mean, spread, normed]

    def project_pieces(self, load, stores, normed_load=None):
        at = {}
        c = self.c

        def begin():
            at["x"] = load()

        def product(m, scale, store):
            def dot():
                at[m] = dot_nn(at["normed"], self.qkv[:, m * c : (m + 1) * c])

            def keep():
                value = at.pop(m) + self.rows[6:7, m * c : (m + 1) * c]
                store((value if scale is None else value * scale).astype(BF))

            return dot, keep

        mean, spread, normed = self.norm_pieces(at, 0)
        made = [product(*entry) for entry in stores]

        def start():
            begin()
            mean()

        rest = [dot for dot, _ in made] + [keep for _, keep in made]
        if normed_load is None:
            return [start, spread, normed], rest

        def read():
            at["normed"] = normed_load()

        return [read] + rest

    def finish_pieces(self, load, attended, store):
        at = {}
        width = 256

        def project():
            at["p"] = dot_nn(attended(), self.proj[...])

        def begin():
            middle = (load() + at.pop("p") + self.row(4)).astype(BF).astype(F32)
            at["x"] = middle
            at["middle"] = middle

        mean, spread, normed = self.norm_pieces(at, 1)

        def start():
            begin()
            mean()

        def up(k):
            def dot():
                at["up", k] = dot_nn(at["normed"], self.fc1[:, k : k + width])

            return dot

        def act(k):
            def gate():
                at["act", k] = gelu(at.pop(("up", k)) + self.rows[7:8, k : k + width]).astype(BF)

            return gate

        def down(k):
            def dot():
                at["down", k] = dot_nn(at.pop(("act", k)), self.fc2[k : k + width, :])

            return dot

        def end():
            total = at["middle"] + self.row(5)
            for k in starts:
                total = total + at["down", k]
            store(total)

        starts = range(0, self.fc2.shape[0], width)
        chains = [[up(k), act(k), down(k)] for k in starts]
        return [project, start, spread, normed], skewed(chains) + [end]


def pipeline(chunks, extra, *makers):
    stages = [[stage for make in makers for stage in make(i)] for i in range(chunks)]
    depth = len(stages[0])
    for t in range(chunks + depth - 1):
        threads = [stages[t - d][d] for d in reversed(range(depth)) if 0 <= t - d < chunks]
        threads.append(extra.get(t, []))
        weave(*threads)


def parity():
    return (lax.axis_index("row") * lax.axis_size("ch") + lax.axis_index("ch")) % 2


def edge_ids(left_ref, right_ref, labels):
    lanes = jnp.concatenate(
        [left_ref[WIN].astype(F32), (labels + 1).astype(F32), right_ref[WIN].astype(F32)], axis=1
    )
    span = lanes.shape[1]
    lane = lax.broadcasted_iota(jnp.int32, (WIN, span), 1)
    match = lane % WIN == lax.broadcasted_iota(jnp.int32, (WIN, span), 0)
    spread = jnp.concatenate(
        [jnp.where(match, lanes[r : r + 1], 0.0) for r in range(WIN)], axis=0
    ).astype(BF)
    source = lax.broadcasted_iota(jnp.int32, (span, 128), 0)
    window = lax.broadcasted_iota(jnp.int32, (span, 128), 1)
    chosen = ((source - 128 + SHIFT) // WIN == window) & (source >= 128 - SHIFT)
    return dot_nn(spread, chosen.astype(F32).astype(BF)).reshape(WIN, WIN, 128).astype(BF)


class Rows:

    def __init__(self, weights, x_ref, edge_ref, out_ref):
        self.w, self.x, self.edge, self.out = weights, x_ref, edge_ref, out_ref
        self.cols = x_ref.shape[1]

    def pieces(self, start, count, attended):
        span = slice(start * WIN, (start + count) * WIN)

        def load():
            inside = start * WIN < self.cols
            block = (self.x[:, span, :] if inside else self.edge[...]).astype(F32)
            return jnp.concatenate(
                [block[r, n * WIN : (n + 1) * WIN] for n in range(count) for r in range(SHIFT)], axis=0
            )

        def store(out):
            for r in range(SHIFT):
                rows = [
                    out[(n * SHIFT + r) * WIN : (n * SHIFT + r + 1) * WIN] for n in range(count)
                ]
                if start * WIN < self.cols:
                    self.out[r, span, :] = jnp.concatenate(rows, axis=0).astype(BF)
                else:
                    before = lax.broadcasted_iota(jnp.int32, rows[0].shape, 0) < SHIFT
                    self.out[r, span.start : span.start + WIN, :] = jnp.where(
                        before, rows[1], rows[0]
                    ).astype(BF)

        return self.w.finish_pieces(load, attended, store)


def block0_chunks(cols, size=16):
    wins = cols // WIN
    return [(n, min(size, wins - n)) for n in range(0, wins, size)] + [(wins, 2)]


def put_edges(edge_ref, left_ref, right_ref, side):
    for r in range(SHIFT):
        edge_ref[r] = jnp.concatenate(
            [left_ref[side * SHIFT + r], right_ref[side * SHIFT + r]], axis=0
        )


def norm_kernel(
    x_hbm, labels_hbm, pack_ref, normed_ref, near_ref, far_ref, labels_ref, x_ref, rows_ref, sem,
    *, part, hidden,
):
    sides = [
        pltpu.make_async_copy(x_hbm.at[pl.ds(side * SHIFT, SHIFT)], target, sem.at[k])
        for k, side, target in ((1, 1 - parity(), near_ref), (2, parity(), far_ref))
    ]
    sides.append(pltpu.make_async_copy(labels_hbm, labels_ref, sem.at[3]))
    cols = x_hbm.shape[1]
    x_copy = pltpu.make_async_copy(x_hbm, x_ref, sem.at[0])
    x_copy.start()
    for copy in sides:
        copy.start()
    w = Weights([pack_ref], (None, None, None, None, rows_ref), x_ref.shape[2], part, hidden)
    for k in range(2):
        rows_ref[k : k + 1, :] = w.small(GAIN + k)[0]
        rows_ref[2 + k : 3 + k, :] = w.small(SHIFTS + k)[0]
    x_copy.wait()
    tokens = WIN * WIN

    def chunk(start, count):
        at = {}

        def begin():
            block = x_ref[:, start * WIN : (start + count) * WIN, :].astype(F32)
            at["x"] = jnp.concatenate(
                [block[r, n * WIN : (n + 1) * WIN] for n in range(count) for r in range(WIN)], axis=0
            )

        def keep():
            normed_ref[start * tokens : (start + count) * tokens] = at["normed"]

        mean, spread, normed = w.norm_pieces(at, 0)
        return [begin, mean, spread, normed, keep]

    wins = cols // WIN
    for piece in offset([chunk(n, min(4, wins - n)) for n in range(0, wins, 4)], 1):
        piece()
    for copy in sides:
        copy.wait()


def regular_kernel(
    x_ref, labels_ref, left_ref, right_ref, rel_ref, normed_ref, *refs,
    groups, own_heads, entries, part, hidden,
):
    packs, refs = refs[:groups], refs[groups:]
    (near_ref, rest_ref, ids_ref, bias_ref, edge_ref), refs = refs[:5], refs[5:]
    (qkv_ref, att_ref), scratch = refs[:2], refs[2:]
    side = 1 - parity()
    cols = x_ref.shape[1]
    c = x_ref.shape[2]
    heads = own_heads * groups
    depth = c // heads
    tokens = WIN * WIN
    half = SHIFT * WIN
    scale = depth ** (-0.5) * LOG2E
    w = Weights(packs, scratch, c, part, hidden)
    masks = head_masks(heads, depth, c)
    ones = jnp.concatenate(masks, axis=0)
    w.load_rows()
    w.load_qkv()

    def pick_bias():
        bias_ref[...] = w.bias(own_heads, entries - 128, rel_ref[...])

    def put_ids():
        ids_ref[...] = edge_ids(left_ref, right_ref, labels_ref[...])

    put_edges(edge_ref, left_ref, right_ref, side)
    extra = {0: [pick_bias, put_ids, w.load_rest]}
    chunks = block0_chunks(cols)
    finish = Rows(w, x_ref, edge_ref, near_ref)

    def first(i):
        start, count = chunks[i]

        def keep(m):
            def store(value):
                qkv_ref[i % 2, m, 0 : count * tokens] = value

            return store

        rows = slice(start * tokens, (start + count) * tokens)
        entries_of = [(0, scale, keep(0)), (1, None, keep(1)), (2, None, keep(2))]
        if start * WIN < cols:
            return [w.project_pieces(None, entries_of, lambda: normed_ref[rows])]

        def edges():
            return jnp.concatenate(
                [e[0:WIN].astype(F32).reshape(tokens, c) for e in (left_ref, right_ref)], axis=0
            )

        norm, rest = w.project_pieces(edges, entries_of)
        return [norm + rest]

    def second(i):
        start, count = chunks[i]

        def window(n):
            rows = slice(n * tokens, (n + 1) * tokens)

            def write(value):
                low, high = value[:half], value[half:]
                att_ref[i % 2, n * half : (n + 1) * half] = jnp.where(side == 0, low, high).astype(BF)
                rest_ref[(start + n) * half : (start + n + 1) * half] = jnp.where(
                    side == 0, high, low
                ).astype(BF)

            return window_pieces(
                lambda: [qkv_ref[i % 2, m, rows] for m in range(3)],
                lambda: bias_ref[...], None, write, masks, ones,
            )

        return [skewed(grouped([window(n) for n in range(count)], 99))]

    def third(i):
        start, count = chunks[i]
        return finish.pieces(start, count, lambda: att_ref[i % 2, 0 : count * half])

    pipeline(len(chunks), extra, first, second, third)
    for r in range(SHIFT):
        near_ref[r, cols + WIN :, :] = ids_ref[side * SHIFT + r]


def rest_kernel(
    x_ref, left_ref, right_ref, att_ref, ids_ref, near_ref, *refs,
    chunks, groups, own_heads, entries, part, hidden,
):
    packs, next_packs, refs = refs[:groups], refs[groups : 2 * groups], refs[2 * groups :]
    (far_ref, qkv_ref, edge_ref, strip_ref, next_qkv, next_rows), scratch = refs[:6], refs[6:]
    cols = x_ref.shape[1]
    side = parity()
    w = Weights(packs, scratch, x_ref.shape[2], part, hidden)
    w.load_rows()
    w.load_rest()
    put_edges(edge_ref, left_ref, right_ref, side)
    finish = Rows(w, x_ref, edge_ref, far_ref)
    half = SHIFT * WIN
    for r in range(SHIFT):
        far_ref[r, cols + WIN :, :] = ids_ref[side * SHIFT + r]
    threads = []
    for start, count in block0_chunks(cols, 8):
        rows = slice(start * half, (start + count) * half)
        threads.append(sum(finish.pieces(start, count, lambda rows=rows: att_ref[rows]), []))
    c = x_ref.shape[2]
    scale = (c // (own_heads * groups)) ** (-0.5) * LOG2E
    following = Weights(next_packs, (next_qkv, None, None, None, next_rows), c, part, hidden)
    following.load_rows()
    following.load_qkv()
    spread_message(near_ref, strip_ref)
    owns = [own_pieces(following, strip_ref, qkv_ref, span, scale) for span in chunks]
    weave(offset(threads, 3), offset(owns, 5))


def even_split(count, most):
    parts = -(-count // most)
    return [(count * k // parts, count * (k + 1) // parts) for k in range(parts)]


def spread_message(src, dst):
    cols = src.shape[1] - 2 * WIN
    value = src[...].astype(F32)
    edge = value[:, cols : cols + WIN]
    dst[:, 0:WIN, :] = edge
    dst[:, WIN : WIN + cols, :] = value[:, :cols]
    dst[:, WIN + cols :, :] = edge
    return value[:, cols + WIN :].reshape(SHIFT * WIN, 128)


def gather(ref, span):
    earlier = lax.broadcasted_iota(jnp.int32, (WIN, ref.shape[2]), 0) < SHIFT
    pieces = []
    for j in range(*span):
        for r in range(SHIFT):
            before = ref[r, j * WIN : (j + 1) * WIN, :]
            after = ref[r, (j + 1) * WIN : (j + 2) * WIN, :]
            pieces.append(jnp.where(earlier, after, before))
    return jnp.concatenate(pieces, axis=0)


def own_pieces(w, strip, qkv, span, scale):
    rows = slice(span[0] * SHIFT * WIN, span[1] * SHIFT * WIN)

    def keep(m):
        def store(value):
            qkv[m, rows] = value

        return store

    norm, rest = w.project_pieces(
        lambda: gather(strip, span), [(m, None if m else scale, keep(m)) for m in range(3)]
    )
    return norm + rest


def shifted_kernel(
    own_in, halo_in, qkv_in, rel_ref, *refs, chunks, near, groups, own_heads, entries, part, hidden
):
    packs, refs = refs[:groups], refs[groups:]
    side = 1 - parity() if near else parity()
    copies = []
    if near:
        next_in, out_ref, next_qkv, next_ref = refs[:4]
        refs = refs[4:]
    else:
        done_ref, out_hbm, out_ref, sems = refs[:4]
        refs = refs[4:]
        copies.append(
            pltpu.make_async_copy(done_ref, out_hbm.at[pl.ds((1 - side) * SHIFT, SHIFT)], sems.at[0])
        )
        copies[0].start()
    (bias_ref, own_ref, halo_ref, res_ref), refs = refs[:4], refs[4:]
    (kv_ref, att_ref), scratch = refs[:2], refs[2:]
    c = own_in.shape[2]
    cols = out_ref.shape[1]
    heads = own_heads * groups
    depth = c // heads
    half = SHIFT * WIN
    tokens = WIN * WIN
    scale = depth ** (-0.5) * LOG2E
    w = Weights(packs, scratch, c, part, hidden)
    w.load_rows()
    masks = head_masks(heads, depth, c)
    ones = jnp.concatenate(masks, axis=0)

    def pick_bias():
        rel = rel_ref[...]
        rel = jnp.concatenate(
            [
                jnp.concatenate([rel[a + SHIFT : a + WIN], rel[a : a + SHIFT]], axis=0)
                for a in range(0, tokens, WIN)
            ],
            axis=0,
        )
        lane = lax.broadcasted_iota(jnp.int32, rel.shape, 1)
        rel = jnp.where(lane % WIN < SHIFT, pltpu.roll(rel, 128 - SHIFT, 1), pltpu.roll(rel, SHIFT, 1))
        rel = jnp.where(side == 0, pltpu.roll(rel[half:], half, 1), rel[:half])
        bias_ref[...] = w.bias(own_heads, entries - 128, rel)

    halo_ids = spread_message(halo_in, halo_ref)
    query_ids = spread_message(own_in, own_ref)
    key_ids = jnp.concatenate([query_ids, halo_ids] * 2, axis=0).T

    def first(i):
        slot = i % 2
        count = (chunks[i][1] - chunks[i][0]) * half

        def keep(target):
            def store(value):
                target[0:count] = value

            return store

        norm, rest = w.project_pieces(
            lambda: gather(halo_ref, chunks[i]),
            [(1 + m, None, keep(kv_ref.at[slot, m])) for m in range(2)],
        )
        return [norm, rest]

    def second(i):
        slot = i % 2
        base = chunks[i][0]

        def window(j):
            rows = slice((j - base) * half, (j - base + 1) * half)
            own = slice(j * half, (j + 1) * half)

            def read():
                k, v = (
                    jnp.concatenate([qkv_in[1 + m, own], kv_ref[slot, m, rows]], axis=0)
                    for m in range(2)
                )
                return qkv_in[0, own], k, v

            def allowed():
                same = jnp.broadcast_to(query_ids[:, j : j + 1], (half, 128)) == key_ids[j : j + 1, :]
                return jnp.concatenate([same, same], axis=1)

            def write(value):
                att_ref[slot, rows] = value.astype(BF)

            return window_pieces(read, lambda: bias_ref[...], allowed, write, masks, ones)

        return [skewed(grouped([window(j) for j in range(*chunks[i])], 99))]

    def third(i):
        base, stop = chunks[i]

        def store(out):
            for r in range(SHIFT):
                res_ref[r, base * WIN : stop * WIN, :] = jnp.concatenate(
                    [
                        out[n * half + r * WIN : n * half + (r + 1) * WIN]
                        for n in range(stop - base)
                    ],
                    axis=0,
                )
            begin = (base - 1) // 2 * 2 * WIN if i else 0
            end = (stop - 1) // 2 * 2 * WIN if i + 1 < len(chunks) else cols
            low = lax.broadcasted_iota(jnp.int32, (SHIFT, end - begin, c), 1) % WIN < SHIFT
            out_ref[:, begin:end, :] = jnp.where(
                low, res_ref[:, begin:end, :], res_ref[:, begin + WIN : end + WIN, :]
            ).astype(BF)
            if not near:
                copies.append(
                    pltpu.make_async_copy(
                        out_ref.at[:, begin:end],
                        out_hbm.at[pl.ds(side * SHIFT, SHIFT), begin:end],
                        sems.at[1 + i],
                    )
                )
                copies[-1].start()

        return w.finish_pieces(
            lambda: gather(own_ref, chunks[i]), lambda: att_ref[i % 2, 0 : (stop - base) * half], store
        )

    extra = {0: [w.load_qkv, pick_bias, w.load_rest]}
    if near:
        spread_message(next_in, next_ref)
        last = len(chunks) + 4
        for n, span in enumerate(chunks):
            extra[last - len(chunks) + n] = own_pieces(w, next_ref, next_qkv, span, scale)
    pipeline(len(chunks), extra, first, second, third)
    for copy in copies:
        copy.wait()


def call(kernel, out_shapes, scratch, *args, **specs):
    return pl.pallas_call(
        kernel,
        out_shape=out_shapes,
        scratch_shapes=scratch,
        compiler_params=pltpu.CompilerParams(vmem_limit_bytes=48 * 1024 * 1024),
        **specs,
    )(*args)


def in_hbm(value):
    return pltpu.with_memory_space_constraint(value, pltpu.HBM)


def neighbours(axis, by):
    size = lax.axis_size(axis)
    return [(i, i + by) for i in range(size) if 0 <= i + by < size]


def both_blocks(*args):
    image_tokens, labels, _ = args[:3]
    qkv_weight, bias_table, fc1_weight = args[5], args[7], args[10]
    tile_cols, c = image_tokens.shape[1:]
    groups = lax.axis_size("ch")
    swap = [(i, (i + 1) % groups) for i in range(groups)]
    part = qkv_weight.shape[3]
    hidden = fc1_weight.shape[2]
    entries = bias_table.shape[1]
    own_heads = bias_table.shape[2]
    tokens = WIN * WIN

    def others(value):
        found = [value]
        for _ in range(groups - 1):
            found.append(lax.ppermute(found[-1], "ch", swap))
        return found

    rows = 4 * part + (hidden // 128) * c + hidden + 3 * SMALL
    pack = jax.ShapeDtypeStruct((rows, 128), BF)
    edge = jax.ShapeDtypeStruct((WIN + 1, WIN, c), BF)
    args = list(args)
    args[5] = qkv_weight.transpose(0, 1, 3, 2)
    args[6] = args[6].transpose(1, 0, 2)
    args[7] = bias_table.transpose(0, 2, 1)
    staged = [pltpu.VMEM((2, WIN, 2 * WIN, c), BF)] + [pltpu.VMEM(a.shape, a.dtype) for a in args[1:]]
    own0, own1, left_edge, right_edge, rel2 = call(
        lambda *refs: pack_kernel(*refs, count=len(args)),
        (pack, pack, edge, edge, jax.ShapeDtypeStruct((tokens, 2 * tokens), jnp.int32)),
        staged + [pltpu.VMEM((SMALL, 128), F32), pltpu.SemaphoreType.DMA((len(args) + 1,))],
        *(in_hbm(a) for a in args),
        in_specs=[pl.BlockSpec(memory_space=pltpu.HBM)] * len(args),
    )
    packs0 = others(own0)
    left = lax.ppermute(right_edge, "col", neighbours("col", 1))
    right = lax.ppermute(left_edge, "col", neighbours("col", -1))
    packs1 = others(own1)

    sizes = dict(groups=groups, own_heads=own_heads, entries=entries, part=part, hidden=hidden)
    weights_scratch = [
        pltpu.VMEM((c, 3 * c), BF),
        pltpu.VMEM((c, c), BF),
        pltpu.VMEM((c, groups * hidden), BF),
        pltpu.VMEM((groups * hidden, c), BF),
        pltpu.VMEM((8, groups * hidden), F32),
    ]
    strip = jax.ShapeDtypeStruct((SHIFT, tile_cols + 2 * WIN, c), BF)
    bias_scratch = pltpu.VMEM((tokens, own_heads * groups * tokens), F32)
    beside = pltpu.VMEM((SHIFT, 2 * WIN, c), BF)
    half_tile = jax.ShapeDtypeStruct((SHIFT, tile_cols, c), BF)
    bands = lax.axis_size(("row", "ch"))

    def swapped(value, first):
        pairs = [(m, m + 1) for m in range(first, bands - 1, 2)]
        return lax.ppermute(value, ("row", "ch"), pairs + [(j, i) for i, j in pairs])

    in_vmem = pl.BlockSpec(memory_space=pltpu.VMEM)
    normed, x_near, x_far, own_labels = call(
        lambda *refs: norm_kernel(*refs, part=part, hidden=hidden),
        (
            jax.ShapeDtypeStruct((tokens * (tile_cols // WIN), c), BF), half_tile, half_tile,
            jax.ShapeDtypeStruct(labels.shape, labels.dtype),
        ),
        [
            pltpu.VMEM(image_tokens.shape, BF), pltpu.VMEM((4, c), F32),
            pltpu.SemaphoreType.DMA((4,)),
        ],
        in_hbm(image_tokens), in_hbm(labels), own0,
        in_specs=[pl.BlockSpec(memory_space=pltpu.HBM)] * 2 + [in_vmem],
    )
    near, rest, ids = call(
        lambda *refs: regular_kernel(*refs, **sizes),
        (
            strip,
            jax.ShapeDtypeStruct((SHIFT * (tile_cols + 2 * WIN), c), BF),
            jax.ShapeDtypeStruct((WIN, WIN, 128), BF),
        ),
        [
            bias_scratch, beside,
            pltpu.VMEM((2, 3, 16 * tokens, c), BF), pltpu.VMEM((2, 8 * tokens, c), BF),
        ] + weights_scratch,
        x_near, own_labels, left, right, rel2, normed, *packs0,
    )
    near_halo = swapped(near, 0)
    chunks = even_split(tile_cols // WIN + 1, 17)
    own_qkv = jax.ShapeDtypeStruct((3, (tile_cols // WIN + 1) * SHIFT * WIN, c), BF)
    strip_wide = pltpu.VMEM((SHIFT, tile_cols + 2 * WIN, c), F32)
    far, near_qkv = call(
        lambda *refs: rest_kernel(*refs, chunks=chunks, **sizes),
        (strip, own_qkv),
        [beside, strip_wide, weights_scratch[0], weights_scratch[-1]] + weights_scratch,
        x_far, left, right, rest, ids, near, *packs0, *packs1,
    )
    far_halo = swapped(far, 1)
    most = max(stop - base for base, stop in chunks) * SHIFT * WIN
    scratch = [
        pltpu.VMEM((SHIFT * WIN, own_heads * groups * tokens), F32), strip_wide, strip_wide,
        pltpu.VMEM((SHIFT, tile_cols + WIN, c), F32),
        pltpu.VMEM((2, 2, most, c), BF), pltpu.VMEM((2, most, c), BF),
    ] + weights_scratch
    near_out, far_qkv = call(
        lambda *refs: shifted_kernel(*refs, chunks=chunks, near=True, **sizes),
        (jax.ShapeDtypeStruct((SHIFT, tile_cols, c), BF), own_qkv),
        [strip_wide] + scratch,
        near, near_halo, near_qkv, rel2, *packs1, far,
    )
    return call(
        lambda *refs: shifted_kernel(*refs, chunks=chunks, near=False, **sizes),
        jax.ShapeDtypeStruct(image_tokens.shape, BF),
        [pltpu.VMEM((SHIFT, tile_cols, c), BF), pltpu.SemaphoreType.DMA((1 + len(chunks),))] + scratch,
        far, far_halo, far_qkv, rel2, *packs1, near_out,
        out_specs=pl.BlockSpec(memory_space=pltpu.HBM),
    )


def solution(mesh):
    in_specs = (
        P(("row", "ch"), "col", None),
        P(("row", "ch"), "col"),
        P(),
        P(),
        P(),
        P(None, None, None, "ch"),
        P(None, None, "ch"),
        P(None, None, "ch"),
        P(None, "ch", None),
        P(),
        P(None, None, "ch"),
        P(None, "ch"),
        P(None, "ch", None),
        P(),
    )
    out_specs = P(("row", "ch"), "col", None)
    return jax.shard_map(
        both_blocks, mesh=mesh, in_specs=in_specs, out_specs=out_specs, check_vma=False
    )
```

```python
import math

import jax
import jax.numpy as jnp
from jax import lax
from jax.experimental import pallas as pl
from jax.experimental.pallas import tpu as pltpu
from jax.sharding import PartitionSpec as P


WIN = 8
SHIFT = 4
EPS = 1e-05
NEG = -1e30
LOG2E = math.log2(math.e)
BF = jnp.bfloat16
F32 = jnp.float32


def dot_nt(a, b):
    return lax.dot_general(a, b, (((1,), (1,)), ((), ())), preferred_element_type=F32)


def dot_nn(a, b):
    return lax.dot_general(a, b, (((1,), (0,)), ((), ())), preferred_element_type=F32)


def gelu(v):
    half = 0.5 * v
    return half + half * lax.erf(v * math.sqrt(0.5))


def head_masks(heads, depth, width):
    lane = lax.broadcasted_iota(jnp.int32, (WIN * WIN, width), 1)
    return [(lane // depth == h).astype(F32).astype(BF) for h in range(heads)]


def stack_heads(rows, masks):
    return jnp.concatenate([rows * mask for mask in masks], axis=0)


def window_pieces(read, bias, allowed, write, masks, ones):
    at = {}

    def score():
        q, k, at["v"] = read()
        at["s"] = dot_nt(q, stack_heads(k, masks))

    def reduce():
        scores = at["s"] + bias()
        if allowed is not None:
            scores = jnp.where(allowed(), scores, NEG)
        first = lax.broadcasted_iota(jnp.int32, (scores.shape[0], 128), 1) < WIN * WIN
        parts = []
        for start in range(0, scores.shape[1], 128):
            s = scores[:, start : start + 128]
            low = jnp.max(jnp.where(first, s, NEG), axis=-1, keepdims=True)
            high = jnp.max(jnp.where(first, NEG, s), axis=-1, keepdims=True)
            parts.append((s, jnp.where(first, low, high)))
        at["s"] = parts

    def mix():
        weights = jnp.concatenate([jnp.exp2(s - m).astype(BF) for s, m in at["s"]], axis=1)
        rhs = jnp.concatenate([stack_heads(at["v"], masks), ones], axis=1)
        at["o"] = dot_nn(weights, rhs)

    def store():
        width = at["o"].shape[1] // 2
        write(at["o"][:, :width] / at["o"][:, width:])

    return [score, reduce, mix, store]


def skewed(pipelines):
    depth = max(len(p) for p in pipelines)
    return [
        pipelines[n][t - n]
        for t in range(len(pipelines) + depth - 1)
        for n in range(len(pipelines))
        if 0 <= t - n < len(pipelines[n])
    ]


def offset(threads, lag):
    return [
        thread[t - n * lag]
        for t in range(max(len(thread) + n * lag for n, thread in enumerate(threads)))
        for n, thread in enumerate(threads)
        if 0 <= t - n * lag < len(thread)
    ]


def grouped(pipelines, size):
    groups = [pipelines[n : n + size] for n in range(0, len(pipelines), size)]
    return [
        [lambda k=k, group=group: [p[k]() for p in group] for k in range(len(group[0]))]
        for group in groups
    ]


def weave(*threads):
    order = sorted(
        ((k + 0.5) / len(thread), n, k) for n, thread in enumerate(threads) for k in range(len(thread))
    )
    for _, n, k in order:
        threads[n][k]()


def pick(low_rows, high_rows, skip, wide):
    rows = wide.shape[0]
    in_low = wide < 128
    low_index = jnp.minimum(wide, 127)
    high_index = jnp.maximum(wide - skip, 0)
    first = lax.broadcasted_iota(jnp.int32, wide.shape, 1) < WIN * WIN

    def of_head(h):
        low = jnp.broadcast_to(low_rows[h] * LOG2E, (rows, 128))
        high = jnp.broadcast_to(high_rows[h] * LOG2E, (rows, 128))
        return jnp.where(
            in_low,
            jnp.take_along_axis(low, low_index, axis=1),
            jnp.take_along_axis(high, high_index, axis=1),
        )

    return jnp.concatenate(
        [jnp.where(first, of_head(h), of_head(h + 1)) for h in range(0, len(low_rows), 2)], axis=1
    )


def split3(value):
    high = value.astype(BF)
    rest = value - high.astype(F32)
    middle = rest.astype(BF)
    return [high, middle, (rest - middle.astype(F32)).astype(BF)]


QKVB, FC1B, TABLE = 0, 3, 5
GAIN, SHIFTS, PROJB, FC2B = 9, 11, 13, 14
SMALL = 16


def pack_kernel(*refs, count):
    hbm, refs = refs[:count], refs[count:]
    (w0_ref, w1_ref, left_ref, right_ref, rel2_ref), refs = refs[:5], refs[5:]
    staged, small_ref, sems = refs[:count], refs[count], refs[count + 1]
    cols = hbm[0].shape[1]
    edge = 2 * WIN
    copies = [
        pltpu.make_async_copy(hbm[0].at[:, 0:edge], staged[0].at[0], sems.at[0]),
        pltpu.make_async_copy(hbm[0].at[:, cols - edge : cols], staged[0].at[1], sems.at[count]),
    ]
    copies += [pltpu.make_async_copy(hbm[k], staged[k], sems.at[k]) for k in range(1, count)]
    for copy in copies:
        copy.start()
    for copy in copies:
        copy.wait()
    (x, labels, rel, gain, shift, qkv, qkvb, table, proj, projb, fc1, fc1b, fc2, fc2b) = staged
    c = x.shape[3]
    part = qkv.shape[2]
    hidden = fc1.shape[2]
    entries = table.shape[2]
    for b, out in enumerate((w0_ref, w1_ref)):
        at = 0
        for m in range(3):
            out[at : at + part, :] = qkv[b, m]
            at += part
        out[at : at + part, :] = proj[b]
        at += part
        for start in range(0, hidden, 128):
            out[at : at + c, :] = fc1[b, :, start : start + 128]
            at += c
        out[at : at + hidden, :] = fc2[b]
        at += hidden
        small_ref[...] = jnp.zeros_like(small_ref)
        for m in range(3):
            small_ref[QKVB + m : QKVB + m + 1, 0:part] = qkvb[m, b : b + 1]
        for k in range(hidden // 128):
            small_ref[FC1B + k : FC1B + k + 1, :] = fc1b[b : b + 1, k * 128 : (k + 1) * 128]
        k = TABLE
        for h in range(table.shape[1]):
            for first in (0, entries - 128):
                small_ref[k : k + 1, :] = table[b, h : h + 1, first : first + 128]
                k += 1
        small_ref[GAIN : GAIN + 2, :] = gain[b]
        small_ref[SHIFTS : SHIFTS + 2, :] = shift[b]
        small_ref[PROJB : PROJB + 1, :] = projb[b : b + 1, :]
        small_ref[FC2B : FC2B + 1, :] = fc2b[b : b + 1, :]
        for piece in split3(small_ref[...]):
            out[at : at + SMALL, :] = piece
            at += SMALL
    ids = (labels[...] + 1).astype(F32).astype(BF)
    for r in range(WIN):
        left_ref[r] = x[0, r, 0:WIN]
        right_ref[r] = x[1, r, WIN:]
    left_ref[WIN] = ids[:, 0:128]
    right_ref[WIN] = ids[:, cols - 128 : cols]
    rel2_ref[...] = jnp.concatenate([rel[...], rel[...]], axis=1)


class Weights:

    def __init__(self, packs, scratch, c, part, hidden):
        self.qkv, self.proj, self.fc1, self.fc2, self.rows = scratch
        self.c = c
        self.packs = packs
        self.part, self.hidden = part, hidden
        self.start_small = 4 * part + (hidden // 128) * c + hidden

    def small(self, row, rows=1, width=128):
        out = []
        for p in self.packs:
            at = self.start_small
            value = sum(
                p[at + k * SMALL : at + (k + 1) * SMALL, :].astype(F32) for k in range(3)
            )
            out.append(value[row : row + rows, :width])
        return out

    def load_rows(self):
        c, part, hidden = self.c, self.part, self.hidden
        vectors = [self.small(GAIN + k)[0] for k in range(2)]
        vectors += [self.small(SHIFTS + k)[0] for k in range(2)]
        vectors += [self.small(PROJB)[0], self.small(FC2B)[0]]
        for k, row in enumerate(vectors):
            self.rows[k : k + 1, 0:c] = row
        self.rows[6:7, 0 : 3 * c] = jnp.concatenate(
            [v for m in range(3) for v in self.small(QKVB + m, width=part)], axis=1
        )
        rows = [self.small(FC1B + k) for k in range(hidden // 128)]
        self.rows[7:8, :] = jnp.concatenate(
            [row[g] for g in range(len(self.packs)) for row in rows], axis=1
        )

    def load_qkv(self):
        c, part = self.c, self.part
        for m in range(3):
            rows = jnp.concatenate([p[m * part : (m + 1) * part, :] for p in self.packs], axis=0)
            self.qkv[:, m * c : (m + 1) * c] = rows.astype(F32).T.astype(BF)

    def load_rest(self):
        c, part, hidden = self.c, self.part, self.hidden
        for g, p in enumerate(self.packs):
            at = 3 * part
            self.proj[g * part : (g + 1) * part, :] = p[at : at + part, :]
            at += part
            for k in range(hidden // 128):
                lane = g * hidden + k * 128
                self.fc1[:, lane : lane + 128] = p[at : at + c, :]
                at += c
            self.fc2[g * hidden : (g + 1) * hidden, :] = p[at : at + hidden, :]

    def row(self, k):
        return self.rows[k : k + 1, 0 : self.c]

    def bias(self, own_heads, skip, wide):
        rows = [self.small(TABLE + k) for k in range(2 * own_heads)]
        low = [rows[2 * h][g] for g in range(len(self.packs)) for h in range(own_heads)]
        high = [rows[2 * h + 1][g] for g in range(len(self.packs)) for h in range(own_heads)]
        return pick(low, high, skip, wide)

    def norm_pieces(self, at, k):
        def mean():
            x = at["x"]
            at["center"] = x - jnp.mean(x, axis=-1, keepdims=True)

        def spread():
            center = at["center"]
            at["spread"] = jnp.mean(center * center, axis=-1, keepdims=True)

        def normed():
            scaled = at["center"] * lax.rsqrt(at["spread"] + EPS)
            at["normed"] = (scaled * self.row(k) + self.row(2 + k)).astype(BF)

        return [mean, spread, normed]

    def project_pieces(self, load, stores, normed_load=None):
        at = {}
        c = self.c

        def begin():
            at["x"] = load()

        def product(m, scale, store):
            def dot():
                at[m] = dot_nn(at["normed"], self.qkv[:, m * c : (m + 1) * c])

            def keep():
                value = at.pop(m) + self.rows[6:7, m * c : (m + 1) * c]
                store((value if scale is None else value * scale).astype(BF))

            return dot, keep

        mean, spread, normed = self.norm_pieces(at, 0)
        made = [product(*entry) for entry in stores]

        def start():
            begin()
            mean()

        rest = [dot for dot, _ in made] + [keep for _, keep in made]
        if normed_load is None:
            return [start, spread, normed], rest

        def read():
            at["normed"] = normed_load()

        return [read] + rest

    def finish_pieces(self, load, attended, store):
        at = {}
        width = 256

        def project():
            at["p"] = dot_nn(attended(), self.proj[...])

        def begin():
            middle = (load() + at.pop("p") + self.row(4)).astype(BF).astype(F32)
            at["x"] = middle
            at["middle"] = middle

        mean, spread, normed = self.norm_pieces(at, 1)

        def start():
            begin()
            mean()

        def up(k):
            def dot():
                at["up", k] = dot_nn(at["normed"], self.fc1[:, k : k + width])

            return dot

        def act(k):
            def gate():
                at["act", k] = gelu(at.pop(("up", k)) + self.rows[7:8, k : k + width]).astype(BF)

            return gate

        def down(k):
            def dot():
                at["down", k] = dot_nn(at.pop(("act", k)), self.fc2[k : k + width, :])

            return dot

        def end():
            total = at["middle"] + self.row(5)
            for k in starts:
                total = total + at["down", k]
            store(total)

        starts = range(0, self.fc2.shape[0], width)
        chains = [[up(k), act(k), down(k)] for k in starts]
        return [project, start, spread, normed], skewed(chains) + [end]


def pipeline(chunks, extra, *makers):
    stages = [[stage for make in makers for stage in make(i)] for i in range(chunks)]
    depth = len(stages[0])
    for t in range(chunks + depth - 1):
        threads = [stages[t - d][d] for d in reversed(range(depth)) if 0 <= t - d < chunks]
        threads.append(extra.get(t, []))
        weave(*threads)


def parity():
    return (lax.axis_index("row") * lax.axis_size("ch") + lax.axis_index("ch")) % 2


def edge_ids(left_ref, right_ref, labels):
    lanes = jnp.concatenate(
        [left_ref[WIN].astype(F32), (labels + 1).astype(F32), right_ref[WIN].astype(F32)], axis=1
    )
    span = lanes.shape[1]
    lane = lax.broadcasted_iota(jnp.int32, (WIN, span), 1)
    match = lane % WIN == lax.broadcasted_iota(jnp.int32, (WIN, span), 0)
    spread = jnp.concatenate(
        [jnp.where(match, lanes[r : r + 1], 0.0) for r in range(WIN)], axis=0
    ).astype(BF)
    source = lax.broadcasted_iota(jnp.int32, (span, 128), 0)
    window = lax.broadcasted_iota(jnp.int32, (span, 128), 1)
    chosen = ((source - 128 + SHIFT) // WIN == window) & (source >= 128 - SHIFT)
    return dot_nn(spread, chosen.astype(F32).astype(BF)).reshape(WIN, WIN, 128).astype(BF)


class Rows:

    def __init__(self, weights, x_ref, edge_ref, out_ref):
        self.w, self.x, self.edge, self.out = weights, x_ref, edge_ref, out_ref
        self.cols = x_ref.shape[1]

    def pieces(self, start, count, attended):
        span = slice(start * WIN, (start + count) * WIN)

        def load():
            inside = start * WIN < self.cols
            block = (self.x[:, span, :] if inside else self.edge[...]).astype(F32)
            return jnp.concatenate(
                [block[r, n * WIN : (n + 1) * WIN] for n in range(count) for r in range(SHIFT)], axis=0
            )

        def store(out):
            for r in range(SHIFT):
                rows = [
                    out[(n * SHIFT + r) * WIN : (n * SHIFT + r + 1) * WIN] for n in range(count)
                ]
                if start * WIN < self.cols:
                    self.out[r, span, :] = jnp.concatenate(rows, axis=0).astype(BF)
                else:
                    before = lax.broadcasted_iota(jnp.int32, rows[0].shape, 0) < SHIFT
                    self.out[r, span.start : span.start + WIN, :] = jnp.where(
                        before, rows[1], rows[0]
                    ).astype(BF)

        return self.w.finish_pieces(load, attended, store)


def block0_chunks(cols, size=16):
    wins = cols // WIN
    return [(n, min(size, wins - n)) for n in range(0, wins, size)] + [(wins, 2)]


def put_edges(edge_ref, left_ref, right_ref, side):
    for r in range(SHIFT):
        edge_ref[r] = jnp.concatenate(
            [left_ref[side * SHIFT + r], right_ref[side * SHIFT + r]], axis=0
        )


def norm_kernel(
    x_hbm, labels_hbm, pack_ref, normed_ref, near_ref, far_ref, labels_ref, x_ref, rows_ref, sem,
    *, part, hidden,
):
    sides = [
        pltpu.make_async_copy(x_hbm.at[pl.ds(side * SHIFT, SHIFT)], target, sem.at[k])
        for k, side, target in ((1, 1 - parity(), near_ref), (2, parity(), far_ref))
    ]
    sides.append(pltpu.make_async_copy(labels_hbm, labels_ref, sem.at[3]))
    cols = x_hbm.shape[1]
    x_copy = pltpu.make_async_copy(x_hbm, x_ref, sem.at[0])
    x_copy.start()
    for copy in sides:
        copy.start()
    w = Weights([pack_ref], (None, None, None, None, rows_ref), x_ref.shape[2], part, hidden)
    for k in range(2):
        rows_ref[k : k + 1, :] = w.small(GAIN + k)[0]
        rows_ref[2 + k : 3 + k, :] = w.small(SHIFTS + k)[0]
    x_copy.wait()
    tokens = WIN * WIN

    def chunk(start, count):
        at = {}

        def begin():
            block = x_ref[:, start * WIN : (start + count) * WIN, :].astype(F32)
            at["x"] = jnp.concatenate(
                [block[r, n * WIN : (n + 1) * WIN] for n in range(count) for r in range(WIN)], axis=0
            )

        def keep():
            normed_ref[start * tokens : (start + count) * tokens] = at["normed"]

        mean, spread, normed = w.norm_pieces(at, 0)
        return [begin, mean, spread, normed, keep]

    wins = cols // WIN
    for piece in offset([chunk(n, min(4, wins - n)) for n in range(0, wins, 4)], 1):
        piece()
    for copy in sides:
        copy.wait()


def regular_kernel(
    x_ref, labels_ref, left_ref, right_ref, rel_ref, normed_ref, *refs,
    groups, own_heads, entries, part, hidden,
):
    packs, refs = refs[:groups], refs[groups:]
    (near_ref, rest_ref, ids_ref, bias_ref, edge_ref), refs = refs[:5], refs[5:]
    (qkv_ref, att_ref), scratch = refs[:2], refs[2:]
    side = 1 - parity()
    cols = x_ref.shape[1]
    c = x_ref.shape[2]
    heads = own_heads * groups
    depth = c // heads
    tokens = WIN * WIN
    half = SHIFT * WIN
    scale = depth ** (-0.5) * LOG2E
    w = Weights(packs, scratch, c, part, hidden)
    masks = head_masks(heads, depth, c)
    ones = jnp.concatenate(masks, axis=0)
    w.load_rows()
    w.load_qkv()

    def pick_bias():
        bias_ref[...] = w.bias(own_heads, entries - 128, rel_ref[...])

    def put_ids():
        ids_ref[...] = edge_ids(left_ref, right_ref, labels_ref[...])

    put_edges(edge_ref, left_ref, right_ref, side)
    extra = {0: [pick_bias, put_ids, w.load_rest]}
    chunks = block0_chunks(cols)
    finish = Rows(w, x_ref, edge_ref, near_ref)

    def first(i):
        start, count = chunks[i]

        def keep(m):
            def store(value):
                qkv_ref[i % 2, m, 0 : count * tokens] = value

            return store

        rows = slice(start * tokens, (start + count) * tokens)
        entries_of = [(0, scale, keep(0)), (1, None, keep(1)), (2, None, keep(2))]
        if start * WIN < cols:
            return [w.project_pieces(None, entries_of, lambda: normed_ref[rows])]

        def edges():
            return jnp.concatenate(
                [e[0:WIN].astype(F32).reshape(tokens, c) for e in (left_ref, right_ref)], axis=0
            )

        norm, rest = w.project_pieces(edges, entries_of)
        return [norm + rest]

    def second(i):
        start, count = chunks[i]

        def window(n):
            rows = slice(n * tokens, (n + 1) * tokens)

            def write(value):
                low, high = value[:half], value[half:]
                att_ref[i % 2, n * half : (n + 1) * half] = jnp.where(side == 0, low, high).astype(BF)
                rest_ref[(start + n) * half : (start + n + 1) * half] = jnp.where(
                    side == 0, high, low
                ).astype(BF)

            return window_pieces(
                lambda: [qkv_ref[i % 2, m, rows] for m in range(3)],
                lambda: bias_ref[...], None, write, masks, ones,
            )

        return [skewed(grouped([window(n) for n in range(count)], 99))]

    def third(i):
        start, count = chunks[i]
        return finish.pieces(start, count, lambda: att_ref[i % 2, 0 : count * half])

    pipeline(len(chunks), extra, first, second, third)
    for r in range(SHIFT):
        near_ref[r, cols + WIN :, :] = ids_ref[side * SHIFT + r]


def rest_kernel(
    x_ref, left_ref, right_ref, att_ref, ids_ref, near_ref, *refs,
    chunks, groups, own_heads, entries, part, hidden,
):
    packs, next_packs, refs = refs[:groups], refs[groups : 2 * groups], refs[2 * groups :]
    (far_ref, qkv_ref, far_qkv_ref, edge_ref, strip_ref, next_qkv, next_rows), scratch = refs[:7], refs[7:]
    cols = x_ref.shape[1]
    side = parity()
    w = Weights(packs, scratch, x_ref.shape[2], part, hidden)
    w.load_rows()
    w.load_rest()
    put_edges(edge_ref, left_ref, right_ref, side)
    finish = Rows(w, x_ref, edge_ref, far_ref)
    half = SHIFT * WIN
    for r in range(SHIFT):
        far_ref[r, cols + WIN :, :] = ids_ref[side * SHIFT + r]
    threads = []
    for start, count in block0_chunks(cols, 8):
        rows = slice(start * half, (start + count) * half)
        threads.append(sum(finish.pieces(start, count, lambda rows=rows: att_ref[rows]), []))
    c = x_ref.shape[2]
    scale = (c // (own_heads * groups)) ** (-0.5) * LOG2E
    following = Weights(next_packs, (next_qkv, None, None, None, next_rows), c, part, hidden)
    following.load_rows()
    following.load_qkv()
    spread_message(near_ref, strip_ref)
    owns = [own_pieces(following, strip_ref, qkv_ref, span, scale) for span in chunks]
    weave(offset(threads, 3), offset(owns, 5))
    spread_message(far_ref, strip_ref)
    for piece in offset([own_pieces(following, strip_ref, far_qkv_ref, span, scale) for span in chunks], 1):
        piece()


def even_split(count, most):
    parts = -(-count // most)
    return [(count * k // parts, count * (k + 1) // parts) for k in range(parts)]


def spread_message(src, dst):
    cols = src.shape[1] - 2 * WIN
    value = src[...].astype(F32)
    edge = value[:, cols : cols + WIN]
    dst[:, 0:WIN, :] = edge
    dst[:, WIN : WIN + cols, :] = value[:, :cols]
    dst[:, WIN + cols :, :] = edge
    return value[:, cols + WIN :].reshape(SHIFT * WIN, 128)


def gather(ref, span):
    earlier = lax.broadcasted_iota(jnp.int32, (WIN, ref.shape[2]), 0) < SHIFT
    pieces = []
    for j in range(*span):
        for r in range(SHIFT):
            before = ref[r, j * WIN : (j + 1) * WIN, :]
            after = ref[r, (j + 1) * WIN : (j + 2) * WIN, :]
            pieces.append(jnp.where(earlier, after, before))
    return jnp.concatenate(pieces, axis=0)


def own_pieces(w, strip, qkv, span, scale):
    rows = slice(span[0] * SHIFT * WIN, span[1] * SHIFT * WIN)

    def keep(m):
        def store(value):
            qkv[m, rows] = value

        return store

    norm, rest = w.project_pieces(
        lambda: gather(strip, span), [(m, None if m else scale, keep(m)) for m in range(3)]
    )
    return norm + rest


def shifted_kernel(
    own_in, halo_in, qkv_in, rel_ref, *refs, chunks, near, groups, own_heads, entries, part, hidden
):
    packs, refs = refs[:groups], refs[groups:]
    side = 1 - parity() if near else parity()
    copies = []
    if near:
        out_ref, refs = refs[0], refs[1:]
    else:
        done_ref, out_hbm, out_ref, sems = refs[:4]
        refs = refs[4:]
        copies.append(
            pltpu.make_async_copy(done_ref, out_hbm.at[pl.ds((1 - side) * SHIFT, SHIFT)], sems.at[0])
        )
        copies[0].start()
    (bias_ref, own_ref, halo_ref, res_ref), refs = refs[:4], refs[4:]
    (kv_ref, att_ref), scratch = refs[:2], refs[2:]
    c = own_in.shape[2]
    cols = out_ref.shape[1]
    heads = own_heads * groups
    depth = c // heads
    half = SHIFT * WIN
    tokens = WIN * WIN
    w = Weights(packs, scratch, c, part, hidden)
    w.load_rows()
    masks = head_masks(heads, depth, c)
    ones = jnp.concatenate(masks, axis=0)

    def pick_bias():
        rel = rel_ref[...]
        rel = jnp.concatenate(
            [
                jnp.concatenate([rel[a + SHIFT : a + WIN], rel[a : a + SHIFT]], axis=0)
                for a in range(0, tokens, WIN)
            ],
            axis=0,
        )
        lane = lax.broadcasted_iota(jnp.int32, rel.shape, 1)
        rel = jnp.where(lane % WIN < SHIFT, pltpu.roll(rel, 128 - SHIFT, 1), pltpu.roll(rel, SHIFT, 1))
        rel = jnp.where(side == 0, pltpu.roll(rel[half:], half, 1), rel[:half])
        bias_ref[...] = w.bias(own_heads, entries - 128, rel)

    halo_ids = spread_message(halo_in, halo_ref)
    query_ids = spread_message(own_in, own_ref)
    key_ids = jnp.concatenate([query_ids, halo_ids] * 2, axis=0).T

    def first(i):
        slot = i % 2
        count = (chunks[i][1] - chunks[i][0]) * half

        def keep(target):
            def store(value):
                target[0:count] = value

            return store

        norm, rest = w.project_pieces(
            lambda: gather(halo_ref, chunks[i]),
            [(1 + m, None, keep(kv_ref.at[slot, m])) for m in range(2)],
        )
        return [norm, rest]

    def second(i):
        slot = i % 2
        base = chunks[i][0]

        def window(j):
            rows = slice((j - base) * half, (j - base + 1) * half)
            own = slice(j * half, (j + 1) * half)

            def read():
                k, v = (
                    jnp.concatenate([qkv_in[1 + m, own], kv_ref[slot, m, rows]], axis=0)
                    for m in range(2)
                )
                return qkv_in[0, own], k, v

            def allowed():
                same = jnp.broadcast_to(query_ids[:, j : j + 1], (half, 128)) == key_ids[j : j + 1, :]
                return jnp.concatenate([same, same], axis=1)

            def write(value):
                att_ref[slot, rows] = value.astype(BF)

            return window_pieces(read, lambda: bias_ref[...], allowed, write, masks, ones)

        return [skewed(grouped([window(j) for j in range(*chunks[i])], 99))]

    def third(i):
        base, stop = chunks[i]

        def store(out):
            for r in range(SHIFT):
                res_ref[r, base * WIN : stop * WIN, :] = jnp.concatenate(
                    [
                        out[n * half + r * WIN : n * half + (r + 1) * WIN]
                        for n in range(stop - base)
                    ],
                    axis=0,
                )
            begin = (base - 1) // 2 * 2 * WIN if i else 0
            end = (stop - 1) // 2 * 2 * WIN if i + 1 < len(chunks) else cols
            low = lax.broadcasted_iota(jnp.int32, (SHIFT, end - begin, c), 1) % WIN < SHIFT
            out_ref[:, begin:end, :] = jnp.where(
                low, res_ref[:, begin:end, :], res_ref[:, begin + WIN : end + WIN, :]
            ).astype(BF)
            if not near:
                copies.append(
                    pltpu.make_async_copy(
                        out_ref.at[:, begin:end],
                        out_hbm.at[pl.ds(side * SHIFT, SHIFT), begin:end],
                        sems.at[1 + i],
                    )
                )
                copies[-1].start()

        return w.finish_pieces(
            lambda: gather(own_ref, chunks[i]), lambda: att_ref[i % 2, 0 : (stop - base) * half], store
        )

    extra = {0: [w.load_qkv, pick_bias, w.load_rest]}
    pipeline(len(chunks), extra, first, second, third)
    for copy in copies:
        copy.wait()


def call(kernel, out_shapes, scratch, *args, **specs):
    return pl.pallas_call(
        kernel,
        out_shape=out_shapes,
        scratch_shapes=scratch,
        compiler_params=pltpu.CompilerParams(vmem_limit_bytes=48 * 1024 * 1024),
        **specs,
    )(*args)


def in_hbm(value):
    return pltpu.with_memory_space_constraint(value, pltpu.HBM)


def neighbours(axis, by):
    size = lax.axis_size(axis)
    return [(i, i + by) for i in range(size) if 0 <= i + by < size]


def both_blocks(*args):
    image_tokens, labels, _ = args[:3]
    qkv_weight, bias_table, fc1_weight = args[5], args[7], args[10]
    tile_cols, c = image_tokens.shape[1:]
    groups = lax.axis_size("ch")
    swap = [(i, (i + 1) % groups) for i in range(groups)]
    part = qkv_weight.shape[3]
    hidden = fc1_weight.shape[2]
    entries = bias_table.shape[1]
    own_heads = bias_table.shape[2]
    tokens = WIN * WIN

    def others(value):
        found = [value]
        for _ in range(groups - 1):
            found.append(lax.ppermute(found[-1], "ch", swap))
        return found

    rows = 4 * part + (hidden // 128) * c + hidden + 3 * SMALL
    pack = jax.ShapeDtypeStruct((rows, 128), BF)
    edge = jax.ShapeDtypeStruct((WIN + 1, WIN, c), BF)
    args = list(args)
    args[5] = qkv_weight.transpose(0, 1, 3, 2)
    args[6] = args[6].transpose(1, 0, 2)
    args[7] = bias_table.transpose(0, 2, 1)
    staged = [pltpu.VMEM((2, WIN, 2 * WIN, c), BF)] + [pltpu.VMEM(a.shape, a.dtype) for a in args[1:]]
    own0, own1, left_edge, right_edge, rel2 = call(
        lambda *refs: pack_kernel(*refs, count=len(args)),
        (pack, pack, edge, edge, jax.ShapeDtypeStruct((tokens, 2 * tokens), jnp.int32)),
        staged + [pltpu.VMEM((SMALL, 128), F32), pltpu.SemaphoreType.DMA((len(args) + 1,))],
        *(in_hbm(a) for a in args),
        in_specs=[pl.BlockSpec(memory_space=pltpu.HBM)] * len(args),
    )
    packs0 = others(own0)
    left = lax.ppermute(right_edge, "col", neighbours("col", 1))
    right = lax.ppermute(left_edge, "col", neighbours("col", -1))
    packs1 = others(own1)

    sizes = dict(groups=groups, own_heads=own_heads, entries=entries, part=part, hidden=hidden)
    weights_scratch = [
        pltpu.VMEM((c, 3 * c), BF),
        pltpu.VMEM((c, c), BF),
        pltpu.VMEM((c, groups * hidden), BF),
        pltpu.VMEM((groups * hidden, c), BF),
        pltpu.VMEM((8, groups * hidden), F32),
    ]
    strip = jax.ShapeDtypeStruct((SHIFT, tile_cols + 2 * WIN, c), BF)
    bias_scratch = pltpu.VMEM((tokens, own_heads * groups * tokens), F32)
    beside = pltpu.VMEM((SHIFT, 2 * WIN, c), BF)
    half_tile = jax.ShapeDtypeStruct((SHIFT, tile_cols, c), BF)
    bands = lax.axis_size(("row", "ch"))

    def swapped(value, first):
        pairs = [(m, m + 1) for m in range(first, bands - 1, 2)]
        return lax.ppermute(value, ("row", "ch"), pairs + [(j, i) for i, j in pairs])

    in_vmem = pl.BlockSpec(memory_space=pltpu.VMEM)
    normed, x_near, x_far, own_labels = call(
        lambda *refs: norm_kernel(*refs, part=part, hidden=hidden),
        (
            jax.ShapeDtypeStruct((tokens * (tile_cols // WIN), c), BF), half_tile, half_tile,
            jax.ShapeDtypeStruct(labels.shape, labels.dtype),
        ),
        [
            pltpu.VMEM(image_tokens.shape, BF), pltpu.VMEM((4, c), F32),
            pltpu.SemaphoreType.DMA((4,)),
        ],
        in_hbm(image_tokens), in_hbm(labels), own0,
        in_specs=[pl.BlockSpec(memory_space=pltpu.HBM)] * 2 + [in_vmem],
    )
    near, rest, ids = call(
        lambda *refs: regular_kernel(*refs, **sizes),
        (
            strip,
            jax.ShapeDtypeStruct((SHIFT * (tile_cols + 2 * WIN), c), BF),
            jax.ShapeDtypeStruct((WIN, WIN, 128), BF),
        ),
        [
            bias_scratch, beside,
            pltpu.VMEM((2, 3, 16 * tokens, c), BF), pltpu.VMEM((2, 8 * tokens, c), BF),
        ] + weights_scratch,
        x_near, own_labels, left, right, rel2, normed, *packs0,
    )
    near_halo = swapped(near, 0)
    chunks = even_split(tile_cols // WIN + 1, 17)
    own_qkv = jax.ShapeDtypeStruct((3, (tile_cols // WIN + 1) * SHIFT * WIN, c), BF)
    strip_wide = pltpu.VMEM((SHIFT, tile_cols + 2 * WIN, c), F32)
    far, near_qkv, far_qkv = call(
        lambda *refs: rest_kernel(*refs, chunks=chunks, **sizes),
        (strip, own_qkv, own_qkv),
        [beside, strip_wide, weights_scratch[0], weights_scratch[-1]] + weights_scratch,
        x_far, left, right, rest, ids, near, *packs0, *packs1,
    )
    far_halo = swapped(far, 1)
    most = max(stop - base for base, stop in chunks) * SHIFT * WIN
    scratch = [
        pltpu.VMEM((SHIFT * WIN, own_heads * groups * tokens), F32), strip_wide, strip_wide,
        pltpu.VMEM((SHIFT, tile_cols + WIN, c), F32),
        pltpu.VMEM((2, 2, most, c), BF), pltpu.VMEM((2, most, c), BF),
    ] + weights_scratch
    near_out = call(
        lambda *refs: shifted_kernel(*refs, chunks=chunks, near=True, **sizes),
        half_tile, scratch, near, near_halo, near_qkv, rel2, *packs1,
    )
    return call(
        lambda *refs: shifted_kernel(*refs, chunks=chunks, near=False, **sizes),
        jax.ShapeDtypeStruct(image_tokens.shape, BF),
        [pltpu.VMEM((SHIFT, tile_cols, c), BF), pltpu.SemaphoreType.DMA((1 + len(chunks),))] + scratch,
        far, far_halo, far_qkv, rel2, *packs1, near_out,
        out_specs=pl.BlockSpec(memory_space=pltpu.HBM),
    )


def solution(mesh):
    in_specs = (
        P(("row", "ch"), "col", None),
        P(("row", "ch"), "col"),
        P(),
        P(),
        P(),
        P(None, None, None, "ch"),
        P(None, None, "ch"),
        P(None, None, "ch"),
        P(None, "ch", None),
        P(),
        P(None, None, "ch"),
        P(None, "ch"),
        P(None, "ch", None),
        P(),
    )
    out_specs = P(("row", "ch"), "col", None)
    return jax.shard_map(
        both_blocks, mesh=mesh, in_specs=in_specs, out_specs=out_specs, check_vma=False
    )
```
